128 devices in a mesh: dp: 1, tp: 16 (over z, y), wg: 8 (over x, core).
Axes of the slice: x: 4, y: 4, z: 4, core: 2. Of those that a mesh axis runs over, the one named last changes fastest.
Arguments:
- tokens: bfloat16 [4096, 2560], P(('dp', 'wg'))
- gain_attn: float32 [2560], P('wg')
- gain_mlp: float32 [2560], P('wg')
- w_qkv: bfloat16 [2560, 3, 32, 80], P('wg', None, 'tp')
- w_rel: bfloat16 [2560, 32, 80], P('wg', 'tp')
- w_out: bfloat16 [32, 80, 2560], P('tp', None, 'wg')
- w_up: bfloat16 [2560, 10240], P('wg', 'tp')
- w_down: bfloat16 [10240, 2560], P('tp', 'wg')
- bias_u: float32 [32, 80], P('tp')
- bias_v: float32 [32, 80], P('tp')
- rel_table: bfloat16 [32, 2560], replicated
- k_cache: bfloat16 [4096, 32, 32, 80], P(('dp', 'wg'), 'tp')
- v_cache: bfloat16 [4096, 32, 32, 80], P(('dp', 'wg'), 'tp')
- positions: int32 [4096], P(('dp', 'wg'))
Outputs:
- output 1: bfloat16 [4096, 2560], P(('dp', 'wg'))
- output 2: bfloat16 [4096, 32, 80], P(('dp', 'wg'), 'tp')
- output 3: bfloat16 [4096, 32, 80], P(('dp', 'wg'), 'tp')
All inputs are finite; a program needn't handle non-finite values.
Results may differ from the reference program's by a relative error of at most 0.015003.
Values are sent between devices in bfloat16 or wider.
A program may use at most 1 GiB of HBM per device.

```python
import math
import jax
import jax.numpy as jnp
from jax import lax

D_MODEL = 2560
N_HEADS = 32
HEAD_DIM = 80
FF_DIM = 10240
CACHE_LEN = 32
SEQ_COUNT = 4096
SEQ_BLOCK = 8
NORM_EPS = 1e-6
SCORE_SCALE = 1.0 / math.sqrt(HEAD_DIM)
BLOCK_COUNT = SEQ_COUNT // SEQ_BLOCK


def setup_inputs(seed: int = 0, part: int = 0) -> dict:
    base_key = jax.random.key(seed)
    part_key = jax.random.fold_in(base_key, part)
    weight_keys = jax.random.split(base_key, 12)
    part_keys = jax.random.split(part_key, 4)
    head_width = N_HEADS * HEAD_DIM
    gain_attn = jax.random.uniform(weight_keys[0], (D_MODEL,), jnp.float32, 0.5, 1.5)
    gain_mlp = jax.random.uniform(weight_keys[1], (D_MODEL,), jnp.float32, 0.5, 1.5)
    w_qkv = (jax.random.normal(weight_keys[2], (D_MODEL, 3, N_HEADS, HEAD_DIM), jnp.float32) * D_MODEL ** -0.5).astype(jnp.bfloat16)
    w_rel = (jax.random.normal(weight_keys[3], (D_MODEL, N_HEADS, HEAD_DIM), jnp.float32) * (2.0 / D_MODEL) ** 0.5).astype(jnp.bfloat16)
    w_out = (jax.random.normal(weight_keys[4], (N_HEADS, HEAD_DIM, D_MODEL), jnp.float32) * 2.0 * head_width ** -0.5).astype(jnp.bfloat16)
    w_up = (jax.random.normal(weight_keys[5], (D_MODEL, FF_DIM), jnp.float32) * D_MODEL ** -0.5).astype(jnp.bfloat16)
    w_down = (jax.random.normal(weight_keys[6], (FF_DIM, D_MODEL), jnp.float32) * FF_DIM ** -0.5).astype(jnp.bfloat16)
    bias_u = jax.random.normal(weight_keys[7], (N_HEADS, HEAD_DIM), jnp.float32)
    bias_v = jax.random.normal(weight_keys[8], (N_HEADS, HEAD_DIM), jnp.float32)
    rel_freqs = jnp.exp(jax.random.uniform(weight_keys[9], (D_MODEL,), jnp.float32, math.log(0.01), math.log(3.0)))
    phases = jax.random.uniform(weight_keys[10], (D_MODEL,), jnp.float32, 0.0, 2.0 * math.pi)
    offsets = jnp.arange(CACHE_LEN, dtype=jnp.float32)
    rel_table = jnp.sin(offsets[:, None] * rel_freqs[None, :] + phases[None, :]).astype(jnp.bfloat16)
    tokens = jax.random.normal(part_keys[0], (SEQ_COUNT, D_MODEL), jnp.float32).astype(jnp.bfloat16)
    k_cache = jax.random.normal(part_keys[1], (SEQ_COUNT, N_HEADS, CACHE_LEN, HEAD_DIM), jnp.float32).astype(jnp.bfloat16)
    v_cache = jax.random.normal(part_keys[2], (SEQ_COUNT, N_HEADS, CACHE_LEN, HEAD_DIM), jnp.float32).astype(jnp.bfloat16)
    positions = jax.random.randint(part_keys[3], (SEQ_COUNT,), 0, CACHE_LEN, jnp.int32)
    positions = positions.at[0].set(CACHE_LEN - 1)
    return {"tokens": tokens, "gain_attn": gain_attn, "gain_mlp": gain_mlp, "w_qkv": w_qkv, "w_rel": w_rel, "w_out": w_out, "w_up": w_up, "w_down": w_down, "bias_u": bias_u, "bias_v": bias_v, "rel_table": rel_table, "k_cache": k_cache, "v_cache": v_cache, "positions": positions}


def rms_norm(row_vals, gain_vec):
    vals_f32 = row_vals.astype(jnp.float32)
    mean_sq = jnp.mean(vals_f32 * vals_f32, axis=-1, keepdims=True)
    return (vals_f32 * lax.rsqrt(mean_sq + NORM_EPS) * gain_vec).astype(jnp.bfloat16)


def attend_block(block_args, rel_f32):
    q_u, q_v, k_new, v_new, k_blk, v_blk, pos_blk = block_args
    key_steps = jnp.arange(CACHE_LEN)
    is_self = key_steps[None, :] == pos_blk[:, None]
    is_valid = key_steps[None, :] <= pos_blk[:, None]
    k_full = jnp.where(is_self[:, None, :, None], k_new[:, :, None, :], k_blk).astype(jnp.float32)
    v_full = jnp.where(is_self[:, None, :, None], v_new[:, :, None, :], v_blk).astype(jnp.float32)
    content = jnp.einsum("bhe,bhje->bhj", q_u.astype(jnp.float32), k_full)
    rel_all = jnp.einsum("bhe,rhe->bhr", q_v.astype(jnp.float32), rel_f32)
    rel_index = jnp.clip(pos_blk[:, None] - key_steps[None, :], 0, CACHE_LEN - 1)
    rel_scores = jnp.take_along_axis(rel_all, jnp.broadcast_to(rel_index[:, None, :], rel_all.shape), axis=2)
    scores = jnp.where(is_valid[:, None, :], (content + rel_scores) * SCORE_SCALE, -1e30)
    attn_probs = jax.nn.softmax(scores, axis=-1).astype(jnp.bfloat16)
    attn_out = jnp.einsum("bhj,bhje->bhe", attn_probs.astype(jnp.float32), v_full)
    return attn_out.astype(jnp.bfloat16)


def reference(tokens, gain_attn, gain_mlp, w_qkv, w_rel, w_out, w_up, w_down, bias_u, bias_v, rel_table, k_cache, v_cache, positions):
    head_width = N_HEADS * HEAD_DIM
    normed = rms_norm(tokens, gain_attn)
    qkv_heads = jnp.dot(normed, w_qkv.reshape(D_MODEL, 3 * head_width), preferred_element_type=jnp.float32).astype(jnp.bfloat16).reshape(SEQ_COUNT, 3, N_HEADS, HEAD_DIM)
    q_heads = qkv_heads[:, 0]
    k_new = qkv_heads[:, 1]
    v_new = qkv_heads[:, 2]
    rel_proj = jnp.dot(rel_table, w_rel.reshape(D_MODEL, head_width), preferred_element_type=jnp.float32).astype(jnp.bfloat16).reshape(CACHE_LEN, N_HEADS, HEAD_DIM)
    rel_f32 = rel_proj.astype(jnp.float32)
    q_u = (q_heads.astype(jnp.float32) + bias_u).astype(jnp.bfloat16)
    q_v = (q_heads.astype(jnp.float32) + bias_v).astype(jnp.bfloat16)

    def to_blocks(array_in):
        return array_in.reshape((BLOCK_COUNT, SEQ_BLOCK) + array_in.shape[1:])

    def run_block(block_args):
        return attend_block(block_args, rel_f32)

    blocked = tuple(to_blocks(array_in) for array_in in (q_u, q_v, k_new, v_new, k_cache, v_cache, positions))
    attn_out = lax.map(run_block, blocked)
    attn_flat = attn_out.reshape(SEQ_COUNT, head_width)
    attn_proj = jnp.dot(attn_flat, w_out.reshape(head_width, D_MODEL), preferred_element_type=jnp.float32)
    resid = tokens.astype(jnp.float32) + attn_proj
    normed_mlp = rms_norm(resid, gain_mlp)
    hidden = jax.nn.gelu(jnp.dot(normed_mlp, w_up, preferred_element_type=jnp.float32), approximate=True).astype(jnp.bfloat16)
    layer_out = (resid + jnp.dot(hidden, w_down, preferred_element_type=jnp.float32)).astype(jnp.bfloat16)
    return (layer_out, k_new, v_new)
```

```python
import jax
import jax.numpy as jnp
from jax import lax
from jax.sharding import PartitionSpec as P

NORM_EPS = 1e-6


def rms_norm(row_vals, gain_vec):
    vals_f32 = row_vals.astype(jnp.float32)
    mean_sq = jnp.mean(vals_f32 * vals_f32, axis=-1, keepdims=True)
    return (vals_f32 * lax.rsqrt(mean_sq + NORM_EPS) * gain_vec).astype(jnp.bfloat16)


def cache_attention(q_u, q_v, k_new, v_new, k_cache, v_cache, positions, rel_proj):
    cache_len = k_cache.shape[2]
    score_scale = q_u.shape[-1] ** -0.5
    key_steps = jnp.arange(cache_len)
    is_self = (key_steps[None, :] == positions[:, None])[:, None, :]
    is_valid = (key_steps[None, :] <= positions[:, None])[:, None, :]
    content = jnp.einsum("bhe,bhje->bhj", q_u, k_cache, preferred_element_type=jnp.float32)
    self_score = jnp.einsum("bhe,bhe->bh", q_u, k_new, preferred_element_type=jnp.float32)
    content = jnp.where(is_self, self_score[:, :, None], content)
    rel_all = jnp.einsum("bhe,rhe->bhr", q_v, rel_proj, preferred_element_type=jnp.float32)
    rel_index = jnp.clip(positions[:, None] - key_steps[None, :], 0, cache_len - 1)
    picked = rel_index[:, :, None] == key_steps[None, None, :]
    rel_scores = jnp.sum(jnp.where(picked[:, None], rel_all[:, :, None, :], 0.0), axis=3)
    scores = jnp.where(is_valid, (content + rel_scores) * score_scale, -1e30)
    attn_probs = jax.nn.softmax(scores, axis=-1).astype(jnp.bfloat16)
    zero_probs = jnp.zeros_like(attn_probs)
    self_prob = jnp.sum(jnp.where(is_self, attn_probs, zero_probs), axis=-1, dtype=jnp.float32)
    cache_probs = jnp.where(is_self, zero_probs, attn_probs)
    attn_out = jnp.einsum("bhj,bhje->bhe", cache_probs, v_cache, preferred_element_type=jnp.float32)
    attn_out = attn_out + self_prob[:, :, None] * v_new.astype(jnp.float32)
    return attn_out.astype(jnp.bfloat16)


def solution(mesh):
    tok_axes = ("dp", "wg")
    in_specs = (P(tok_axes, None), P("wg"), P("wg"), P("wg", None, "tp", None), P("wg", "tp", None), P("tp", None, "wg"), P("wg", "tp"), P("tp", "wg"), P("tp", None), P("tp", None), P(None, None), P(tok_axes, "tp", None, None), P(tok_axes, "tp", None, None), P(tok_axes))
    out_specs = (P(tok_axes, None), P(tok_axes, "tp", None), P(tok_axes, "tp", None))

    def device_step(tokens, gain_attn, gain_mlp, w_qkv, w_rel, w_out, w_up, w_down, bias_u, bias_v, rel_table, k_cache, v_cache, positions):
        gains = lax.all_gather(jnp.stack([gain_attn, gain_mlp]), "wg", axis=1, tiled=True)
        gain_attn_full, gain_mlp_full = gains[0], gains[1]
        qkv_full = lax.all_gather(w_qkv, "wg", axis=0, tiled=True)
        rel_full = lax.all_gather(w_rel, "wg", axis=0, tiled=True)
        out_full = lax.all_gather(w_out, "wg", axis=2, tiled=True)
        up_full = lax.all_gather(w_up, "wg", axis=0, tiled=True)
        down_full = lax.all_gather(w_down, "wg", axis=1, tiled=True)
        normed = rms_norm(tokens, gain_attn_full)
        qkv_heads = jnp.einsum("td,dshe->tshe", normed, qkv_full, preferred_element_type=jnp.float32).astype(jnp.bfloat16)
        q_heads = qkv_heads[:, 0]
        k_new = qkv_heads[:, 1]
        v_new = qkv_heads[:, 2]
        rel_proj = jnp.einsum("rd,dhe->rhe", rel_table, rel_full, preferred_element_type=jnp.float32).astype(jnp.bfloat16)
        q_u = (q_heads.astype(jnp.float32) + bias_u).astype(jnp.bfloat16)
        q_v = (q_heads.astype(jnp.float32) + bias_v).astype(jnp.bfloat16)
        attn_out = cache_attention(q_u, q_v, k_new, v_new, k_cache, v_cache, positions, rel_proj)
        attn_part = jnp.einsum("the,hed->td", attn_out, out_full, preferred_element_type=jnp.float32).astype(jnp.bfloat16)
        attn_sum = lax.psum(attn_part, "tp")
        resid = tokens.astype(jnp.float32) + attn_sum.astype(jnp.float32)
        normed_mlp = rms_norm(resid, gain_mlp_full)
        hidden = jax.nn.gelu(jnp.dot(normed_mlp, up_full, preferred_element_type=jnp.float32), approximate=True).astype(jnp.bfloat16)
        mlp_part = jnp.dot(hidden, down_full, preferred_element_type=jnp.float32).astype(jnp.bfloat16)
        mlp_sum = lax.psum(mlp_part, "tp")
        layer_out = (resid + mlp_sum.astype(jnp.float32)).astype(jnp.bfloat16)
        return layer_out, k_new, v_new

    return jax.shard_map(device_step, mesh=mesh, in_specs=in_specs, out_specs=out_specs, check_vma=False)
```

```python
import jax
import jax.numpy as jnp
from jax import lax
from jax.experimental import pallas as pl
from jax.experimental.pallas import tpu as pltpu
from jax.sharding import PartitionSpec as P

NORM_EPS = 1e-6
BF = jnp.bfloat16
F32 = jnp.float32
MESH = pl.DeviceIdType.MESH
ANY = pl.ANY
SEQ, DM, HALF, HD, CL, FF = 512, 2560, 1280, 80, 32, 640
NT = (((1,), (1,)), ((), ()))
NN = (((1,), (0,)), ((), ()))
TN = (((0,), (0,)), ((), ()))


def mm(a, b, dims):
    return lax.dot_general(a, b, dims, preferred_element_type=F32)


def layer_kernel(x_h, pos_h, bias_h, gain_h, wq_h, wo_h, wu_h, wd_h, rt_h, k_h, v_h,
                 y_h, kn_h, vn_h,
                 x_s, pos_s, bias_s, rt_s, wg_s, wq_s, wo_s, wu_s, wd_s, k_s, v_s,
                 rs_s, acc, qt_s, qu_s, sc_s, ot_s, o_s, wof_s, kn_s, vn_s, p_s,
                 rel1, rcv1, stg1, rel2, rcv2, stg2, s2_s, h_s, g_s, u_s, hid_s,
                 lsem, gsem_s, gsem_r, rsem_s, rsem_r, asem_s, asem_r):
    tp, wg = lax.axis_index("tp"), lax.axis_index("wg")
    z, y = tp // 4, tp % 4
    x, c = wg // 2, wg % 2

    def up1(i, d):
        return lax.rem(i + d, 4)

    def dev(dz=0, dy=0, dx=0, flip=False):
        cc = 1 - c if flip else c
        return (0, up1(z, dz) * 4 + up1(y, dy), up1(x, dx) * 2 + cc)

    xp, xm, sib = dev(dx=1), dev(dx=3), dev(flip=True)
    zp, zm, yp, ym = dev(dz=1), dev(dz=3), dev(dy=1), dev(dy=3)

    sends = []

    def send(src, dst, ssem, rsem, device):
        cp = pltpu.make_async_remote_copy(src, dst, ssem, rsem, device_id=device, device_id_type=MESH)
        cp.start()
        sends.append(cp)

    def arrived(dst, ssem, rsem, device):
        pltpu.make_async_remote_copy(dst, dst, ssem, rsem, device_id=device, device_id_type=MESH).wait_recv()

    n_local = [0]

    def local(src, dst):
        cp = pltpu.make_async_copy(src, dst, lsem.at[n_local[0]])
        n_local[0] += 1
        cp.start()
        return cp

    own = 2 * x + c
    l_g = local(gain_h, wg_s.at[own])
    l_q = local(wq_h, wq_s.at[own])
    l_x = local(x_h, x_s)
    l_rt = local(rt_h, rt_s)
    l_pos = local(pos_h, pos_s)
    l_bias = local(bias_h, bias_s)
    l_wo = local(wo_h, wo_s.at[own])
    l_wu = local(wu_h, wu_s.at[own])
    l_wd = local(wd_h, wd_s.at[own])
    l_k = local(k_h, k_s)
    l_v = local(v_h, v_s)

    barrier = pltpu.get_barrier_semaphore()
    for d in (xp, xm, sib, zp, zm, yp, ym):
        pl.semaphore_signal(barrier, inc=1, device_id=d, device_id_type=MESH)
    pl.semaphore_wait(barrier, 7)

    def slot(dx, flip=False):
        return 2 * up1(x, dx) + (1 - c if flip else c)

    class Gather:
        def __init__(self, ar, buf, rows, split=True):
            self.ar, self.buf, self.rows, self.split = ar, buf, rows, split

        def ref(self, s, part):
            if part is None:
                return self.buf.at[s]
            n = self.rows // 2
            return self.buf.at[s, pl.ds(part * n, n)]

        def sems(self, k):
            return gsem_s.at[self.ar, k], gsem_r.at[self.ar, k]

        def put(self, k, s, part, device):
            r = self.ref(s, part)
            send(r, r, *self.sems(k), device)

        def got(self, k, s, part, device):
            arrived(self.ref(s, part), *self.sems(k), device)

        def start(self):
            o = slot(0)
            if self.split:
                self.put(0, o, 0, xp)
                self.put(2, o, 1, xm)
                self.put(1, o, 1, xp)
                self.put(3, o, 0, xm)
            else:
                self.put(0, o, None, xp)
                self.put(2, o, None, xm)
            self.put(6, o, None, sib)

        def forward(self):
            if self.split:
                self.got(0, slot(3), 0, xm)
                self.put(4, slot(3), 0, xp)
                self.got(2, slot(1), 1, xp)
                self.put(5, slot(1), 1, xm)
                self.got(1, slot(3), 1, xm)
                self.got(3, slot(1), 0, xp)
            else:
                self.got(0, slot(3), None, xm)
                self.put(4, slot(3), None, xp)
                self.got(2, slot(1), None, xp)
            self.put(7, slot(3), None, sib)
            self.put(8, slot(1), None, sib)

        def last(self):
            if self.split:
                self.got(4, slot(2), 0, xm)
                self.got(5, slot(2), 1, xp)
            else:
                self.got(4, slot(2), None, xm)
            self.put(9, slot(2), None, sib)

        def sibling(self, k):
            self.got(k, slot({6: 0, 7: 3, 8: 1, 9: 2}[k], True), None, sib)

    g_g = Gather(0, wg_s, 8, split=False)
    g_q = Gather(1, wq_s, 640)
    g_o = Gather(2, wo_s, 160)
    g_u = Gather(3, wu_s, 320)
    g_d = Gather(4, wd_s, 320)

    l_g.wait()
    g_g.start()
    l_q.wait()
    g_q.start()

    l_x.wait()

    def stat_rows(r, carry):
        rows = pl.ds(pl.multiple_of(r * 32, 32), 32)
        v = x_s[rows, :].astype(F32)
        ms = jnp.sum(v * v, axis=1, keepdims=True) * (1.0 / DM)
        rs_s[rows, :] = jnp.broadcast_to(lax.rsqrt(ms + NORM_EPS), (32, 128))
        return carry

    lax.fori_loop(0, 16, stat_rows, 0)
    l_rt.wait()
    acc[...] = jnp.zeros_like(acc)
    qt_s[...] = jnp.zeros_like(qt_s)
    u_s[...] = jnp.zeros_like(u_s)

    def qkv_block(dx, flip):
        s = slot(dx, flip)
        xo, co = s // 2, s % 2
        cols = pl.ds(pl.multiple_of(xo * 640 + co * 256, 128), 384)
        n_win = (x_s[:, cols].astype(F32) * rs_s[:, 0:1] * wg_s[s, 0:1, :]).astype(BF)
        acc[...] += mm(wq_s[s, 0:480, :], n_win, NT)
        qt_s[...] += mm(wq_s[s, 480:640, :], rt_s[:, cols], NT)

    qkv_block(0, False)
    g_g.forward()
    g_g.last()
    for k in (6, 7, 8, 9):
        g_g.sibling(k)
    g_q.sibling(6)
    qkv_block(0, True)
    g_q.forward()
    l_wo.wait()
    g_o.start()
    l_wu.wait()
    g_u.start()
    l_wd.wait()
    g_d.start()
    qkv_block(3, False)
    qkv_block(1, False)
    g_q.sibling(7)
    qkv_block(3, True)
    g_q.sibling(8)
    qkv_block(1, True)
    g_q.last()
    qkv_block(2, False)
    g_q.sibling(9)
    qkv_block(2, True)

    kn_s[...] = acc[160:320, :].astype(BF)
    vn_s[...] = acc[320:480, :].astype(BF)
    l_kn = local(kn_s, kn_h)
    l_vn = local(vn_s, vn_h)
    l_pos.wait()
    l_bias.wait()

    flip_rows = (lax.broadcasted_iota(jnp.int32, (CL, CL), 0) + lax.broadcasted_iota(jnp.int32, (CL, CL), 1)) % CL == 0
    flip_mat = jnp.where(flip_rows, 1.0, 0.0).astype(BF)
    rel_rev = mm(qt_s[...].astype(BF), flip_mat, NN).astype(BF)
    pos = pos_s[...]
    steps = lax.broadcasted_iota(jnp.int32, (CL, SEQ), 0)
    is_self = steps == pos
    l_k.wait()
    l_v.wait()
    g_o.forward()

    for h in range(2):
        hr = slice(h * HD, h * HD + HD)
        q = acc[hr, :].astype(BF).astype(F32)
        q_u = (q + bias_s[hr, 0:1]).astype(BF).astype(F32)
        q_v = (q + bias_s[hr, 1:2]).astype(BF)
        qu_s[...] = q_u
        rel = mm(rel_rev[hr, :], q_v, TN)
        for b in range(5):
            rel = jnp.where((pos >> b) & 1 == 1, pltpu.roll(rel, 1 << b, 0), rel)
        self_score = jnp.sum(q_u * kn_s[hr, :].astype(F32), axis=0, keepdims=True)
        for lc in range(4):
            ln = slice(lc * 128, lc * 128 + 128)
            quc = qu_s[:, ln]

            def content(g, carry, h=h, ln=ln, quc=quc):
                rows = [jnp.sum(k_s[h, g * 8 + j, :, ln].astype(F32) * quc, axis=0, keepdims=True) for j in range(8)]
                sc_s[pl.ds(pl.multiple_of(g * 8, 8), 8), ln] = jnp.concatenate(rows, axis=0)
                return carry

            lax.fori_loop(0, CL // 8, content, 0)
        scores = jnp.where(is_self, self_score, sc_s[...])
        scores = jnp.where(steps <= pos, (scores + rel) * (HD ** -0.5), -1e30)
        e = jnp.exp(scores - jnp.max(scores, axis=0, keepdims=True))
        prob = (e / jnp.sum(e, axis=0, keepdims=True)).astype(BF).astype(F32)
        self_prob = jnp.sum(jnp.where(is_self, prob, 0.0), axis=0, keepdims=True)
        sc_s[...] = jnp.where(is_self, 0.0, prob)
        for lc in range(4):
            ln = slice(lc * 128, lc * 128 + 128)

            def mix(g, o, h=h, ln=ln):
                pr = sc_s[pl.ds(pl.multiple_of(g * 8, 8), 8), ln]
                for j in range(8):
                    o = o + pr[j:j + 1, :] * v_s[h, g * 8 + j, :, ln].astype(F32)
                return o

            start = self_prob[:, ln] * vn_s[hr, ln].astype(F32)
            ot_s[hr, ln] = lax.fori_loop(0, CL // 8, mix, start)

    o_s[...] = jnp.transpose(ot_s[...]).astype(BF).reshape(4, 4, 32, 160)
    g_o.last()
    for k in (6, 7, 8, 9):
        g_o.sibling(k)
    for xo in range(4):
        even, odd = wo_s[2 * xo], wo_s[2 * xo + 1]
        base = 640 * xo
        wof_s[:, base:base + 256] = even[:, 0:256]
        wof_s[:, base + 256:base + 384] = even[:, 256:384] + odd[:, 0:128]
        wof_s[:, base + 384:base + 640] = odd[:, 128:384]

    place = ((z, y, zp, zm, yp, ym), (y, z, yp, ym, zp, zm))

    def reduce_scatter(ps, chunk, between):
        for hf in range(2):
            a, b, ap, am, _, _ = place[hf]
            ss, rr = rsem_s.at[ps, hf, 0], rsem_r.at[ps, hf, 0]
            chunk(hf, up1(a, 2))
            send(p_s.at[ps, hf, up1(a, 2), pl.ds(0, 2)], rel1.at[ps, hf, 0], ss.at[0], rr.at[0], ap)
            send(p_s.at[ps, hf, up1(a, 2), pl.ds(2, 2)], rel1.at[ps, hf, 1], ss.at[1], rr.at[1], am)
        for hf in range(2):
            a, b, ap, am, _, _ = place[hf]
            ss, rr = rsem_s.at[ps, hf, 0], rsem_r.at[ps, hf, 0]
            chunk(hf, up1(a, 1))
            send(p_s.at[ps, hf, up1(a, 1), pl.ds(2, 2)], rcv1.at[ps, hf, 0, pl.ds(2, 2)], ss.at[2], rr.at[2], ap)
            chunk(hf, up1(a, 3))
            send(p_s.at[ps, hf, up1(a, 3), pl.ds(0, 2)], rcv1.at[ps, hf, 1, pl.ds(0, 2)], ss.at[3], rr.at[3], am)
        for hf in range(2):
            chunk(hf, place[hf][0])
        for hf in range(2):
            a, b, ap, am, _, _ = place[hf]
            ss, rr = rsem_s.at[ps, hf, 0], rsem_r.at[ps, hf, 0]
            arrived(rel1.at[ps, hf, 0], ss.at[0], rr.at[0], am)
            stg1[ps, hf, 0] = (p_s[ps, hf, up1(a, 1), 0:2].astype(F32) + rel1[ps, hf, 0].astype(F32)).astype(BF)
            send(stg1.at[ps, hf, 0], rcv1.at[ps, hf, 0, pl.ds(0, 2)], ss.at[4], rr.at[4], ap)
            arrived(rel1.at[ps, hf, 1], ss.at[1], rr.at[1], ap)
            stg1[ps, hf, 1] = (p_s[ps, hf, up1(a, 3), 2:4].astype(F32) + rel1[ps, hf, 1].astype(F32)).astype(BF)
            send(stg1.at[ps, hf, 1], rcv1.at[ps, hf, 1, pl.ds(2, 2)], ss.at[5], rr.at[5], am)
        between(0)
        for hf in range(2):
            a, b, ap, am, bp, bm = place[hf]
            ss, rr = rsem_s.at[ps, hf, 0], rsem_r.at[ps, hf, 0]
            arrived(rcv1.at[ps, hf, 0, pl.ds(2, 2)], ss.at[2], rr.at[2], am)
            arrived(rcv1.at[ps, hf, 1, pl.ds(0, 2)], ss.at[3], rr.at[3], ap)
            arrived(rcv1.at[ps, hf, 0, pl.ds(0, 2)], ss.at[4], rr.at[4], am)
            arrived(rcv1.at[ps, hf, 1, pl.ds(2, 2)], ss.at[5], rr.at[5], ap)
            for j in (2, 1, 3, 0):
                bj = up1(b, j)
                s2_s[ps, hf, bj] = (p_s[ps, hf, a, bj].astype(F32) + rcv1[ps, hf, 0, bj].astype(F32)
                                    + rcv1[ps, hf, 1, bj].astype(F32)).astype(BF)
                ss, rr = rsem_s.at[ps, hf, 1], rsem_r.at[ps, hf, 1]
                if j == 2:
                    send(s2_s.at[ps, hf, bj, pl.ds(0, 16)], rel2.at[ps, hf, 0], ss.at[0], rr.at[0], bp)
                    send(s2_s.at[ps, hf, bj, pl.ds(16, 16)], rel2.at[ps, hf, 1], ss.at[1], rr.at[1], bm)
                elif j == 1:
                    send(s2_s.at[ps, hf, bj, pl.ds(16, 16)], rcv2.at[ps, hf, 0, pl.ds(16, 16)], ss.at[2], rr.at[2], bp)
                elif j == 3:
                    send(s2_s.at[ps, hf, bj, pl.ds(0, 16)], rcv2.at[ps, hf, 1, pl.ds(0, 16)], ss.at[3], rr.at[3], bm)
        for hf in range(2):
            a, b, ap, am, bp, bm = place[hf]
            ss, rr = rsem_s.at[ps, hf, 1], rsem_r.at[ps, hf, 1]
            arrived(rel2.at[ps, hf, 0], ss.at[0], rr.at[0], bm)
            stg2[ps, hf, 0] = (s2_s[ps, hf, up1(b, 1), 0:16].astype(F32) + rel2[ps, hf, 0].astype(F32)).astype(BF)
            send(stg2.at[ps, hf, 0], rcv2.at[ps, hf, 0, pl.ds(0, 16)], ss.at[4], rr.at[4], bp)
            arrived(rel2.at[ps, hf, 1], ss.at[1], rr.at[1], bp)
            stg2[ps, hf, 1] = (s2_s[ps, hf, up1(b, 3), 16:32].astype(F32) + rel2[ps, hf, 1].astype(F32)).astype(BF)
            send(stg2.at[ps, hf, 1], rcv2.at[ps, hf, 1, pl.ds(16, 16)], ss.at[5], rr.at[5], bm)
        between(1)
        out = []
        for hf in range(2):
            a, b, ap, am, bp, bm = place[hf]
            ss, rr = rsem_s.at[ps, hf, 1], rsem_r.at[ps, hf, 1]
            arrived(rcv2.at[ps, hf, 0, pl.ds(16, 16)], ss.at[2], rr.at[2], bm)
            arrived(rcv2.at[ps, hf, 1, pl.ds(0, 16)], ss.at[3], rr.at[3], bp)
            arrived(rcv2.at[ps, hf, 0, pl.ds(0, 16)], ss.at[4], rr.at[4], bm)
            arrived(rcv2.at[ps, hf, 1, pl.ds(16, 16)], ss.at[5], rr.at[5], bp)
            out.append(s2_s[ps, hf, b].astype(F32) + rcv2[ps, hf, 0].astype(F32) + rcv2[ps, hf, 1].astype(F32))
        return out

    class Ring:
        def __init__(self, ps, ph, hf):
            a, b, ap, am, bp, bm = place[hf]
            self.ps, self.ph, self.hf, self.a = ps, ph, hf, a
            self.i, self.fwd, self.bwd = (b, bp, bm) if ph == 0 else (a, ap, am)

        def ref(self, d, part):
            i = up1(self.i, d)
            if self.ph == 0:
                return g_s.at[self.ps, self.hf, self.a, i, pl.ds(part * 16, 16)]
            return g_s.at[self.ps, self.hf, i, pl.ds(part * 2, 2)]

        def sems(self, k):
            return asem_s.at[self.ps, self.hf, self.ph, k], asem_r.at[self.ps, self.hf, self.ph, k]

        def put(self, k, d, part, device):
            r = self.ref(d, part)
            send(r, r, *self.sems(k), device)

        def got(self, k):
            d, part, device = {0: (3, 0, self.bwd), 1: (1, 1, self.fwd), 2: (3, 1, self.bwd),
                               3: (1, 0, self.fwd), 4: (2, 0, self.bwd), 5: (2, 1, self.fwd)}[k]
            arrived(self.ref(d, part), *self.sems(k), device)

        def start(self):
            self.put(0, 0, 0, self.fwd)
            self.put(1, 0, 1, self.bwd)
            self.put(2, 0, 1, self.fwd)
            self.put(3, 0, 0, self.bwd)

        def forward(self):
            self.got(0)
            self.put(4, 3, 0, self.fwd)
            self.got(1)
            self.put(5, 1, 1, self.bwd)

    def all_gather(ps, consume):
        inner = [Ring(ps, 0, hf) for hf in range(2)]
        outer = [Ring(ps, 1, hf) for hf in range(2)]
        for r in inner:
            r.start()
        for r in inner:
            r.forward()
        for hf in range(2):
            for k in (2, 3, 4, 5):
                inner[hf].got(k)
            outer[hf].start()
        for hf in range(2):
            consume(hf, outer[hf].i)
        for r in outer:
            r.forward()
        for k, d in ((2, 3), (3, 1)):
            for hf in range(2):
                outer[hf].got(k)
                consume(hf, up1(outer[hf].i, d))
        for hf in range(2):
            outer[hf].got(4)
            outer[hf].got(5)
            consume(hf, up1(outer[hf].i, 2))

    def out_chunk(hf, i):
        rows = (o_s[i] if hf == 0 else o_s[:, i]).reshape(128, 160)
        part = mm(rows, wof_s[:, hf * HALF:hf * HALF + HALF], NN)
        p_s[0, hf, i] = part.astype(BF).reshape(4, 32, HALF)

    def attn_between(step):
        if step == 0:
            g_u.forward()
        else:
            g_u.last()

    part = reduce_scatter(0, out_chunk, attn_between)
    mine = pl.ds(pl.multiple_of(tp * 32, 32), 32)
    for hf in range(2):
        cols = slice(hf * HALF, hf * HALF + HALF)
        h_s[:, cols] = x_s[mine, cols].astype(F32) + part[hf]
    resid = h_s[...]
    inv = lax.rsqrt(jnp.sum(resid * resid, axis=1, keepdims=True) * (1.0 / DM) + NORM_EPS)
    gains = []
    for xo in range(4):
        even, odd = wg_s[2 * xo, 1:2, :], wg_s[2 * xo + 1, 1:2, :]
        gains += [even[:, 0:256], even[:, 256:384] + odd[:, 0:128], odd[:, 128:384]]
    normed = (resid * inv * jnp.concatenate(gains, axis=1)).astype(BF)
    g_s[0, 0, z, y] = normed[:, 0:HALF]
    g_s[0, 1, y, z] = normed[:, HALF:DM]

    first = [True]

    def up_part(hf, i):
        if first[0]:
            first[0] = False
            for k in (6, 7, 8, 9):
                g_u.sibling(k)
        w = wu_s[4 * hf:4 * hf + 4].reshape(HALF, FF)
        prod = mm(g_s[0, hf, i].reshape(128, HALF), w, NN).reshape(4, 32, FF)
        if hf == 0:
            u_s[i] += prod
        else:
            u_s[:, i] += prod

    all_gather(0, up_part)
    g_d.forward()
    g_d.last()
    for k in (6, 7, 8, 9):
        g_d.sibling(k)
    for i in range(4):
        hid_s[i] = jax.nn.gelu(u_s[i], approximate=True).astype(BF)

    def down_chunk(hf, i):
        rows = (hid_s[i] if hf == 0 else hid_s[:, i]).reshape(128, FF)
        w = wd_s[4 * hf:4 * hf + 4].reshape(HALF, FF)
        p_s[1, hf, i] = mm(rows, w, NT).astype(BF).reshape(4, 32, HALF)

    part = reduce_scatter(1, down_chunk, lambda step: None)
    g_s[1, 0, z, y] = (h_s[:, 0:HALF] + part[0]).astype(BF)
    g_s[1, 1, y, z] = (h_s[:, HALF:DM] + part[1]).astype(BF)
    outs = [l_kn, l_vn]

    def write_out(hf, i):
        if hf == 0:
            outs.append(local(g_s.at[1, 0, i], y_h.at[i, :, :, pl.ds(0, HALF)]))
        else:
            outs.append(local(g_s.at[1, 1, i], y_h.at[:, i, :, pl.ds(HALF, HALF)]))

    all_gather(1, write_out)
    for cp in outs:
        cp.wait()
    for cp in sends:
        cp.wait_send()


def solution(mesh):
    tok_axes = ("dp", "wg")
    in_specs = (P(tok_axes, None), P("wg"), P("wg"), P("wg", None, "tp", None), P("wg", "tp", None), P("tp", None, "wg"), P("wg", "tp"), P("tp", "wg"), P("tp", None), P("tp", None), P(None, None), P(tok_axes, "tp", None, None), P(tok_axes, "tp", None, None), P(tok_axes))
    out_specs = (P(tok_axes, None), P(tok_axes, "tp", None), P(tok_axes, "tp", None))

    def vm(shape, dtype=BF):
        return pltpu.VMEM(shape, dtype)

    scratch = [
        vm((SEQ, DM)), vm((1, SEQ), jnp.int32), vm((160, 128), F32), vm((CL, DM)),
        vm((8, 8, 384), F32), vm((8, 640, 384)), vm((8, 160, 384)), vm((8, 320, FF)), vm((8, 320, FF)),
        vm((2, CL, HD, SEQ)), vm((2, CL, HD, SEQ)),
        vm((SEQ, 128), F32), vm((480, SEQ), F32), vm((160, CL), F32), vm((HD, SEQ), F32), vm((CL, SEQ), F32),
        vm((160, SEQ), F32), vm((4, 4, 32, 160)), vm((160, DM)), vm((160, SEQ)), vm((160, SEQ)),
        vm((2, 2, 4, 4, 32, HALF)),
        vm((2, 2, 2, 2, 32, HALF)), vm((2, 2, 2, 4, 32, HALF)), vm((2, 2, 2, 2, 32, HALF)),
        vm((2, 2, 2, 16, HALF)), vm((2, 2, 2, 32, HALF)), vm((2, 2, 2, 16, HALF)),
        vm((2, 2, 4, 32, HALF)), vm((32, DM), F32), vm((2, 2, 4, 4, 32, HALF)),
        vm((4, 4, 32, FF), F32), vm((4, 4, 32, FF)),
        pltpu.SemaphoreType.DMA((24,)),
        pltpu.SemaphoreType.DMA((5, 10)), pltpu.SemaphoreType.DMA((5, 10)),
        pltpu.SemaphoreType.DMA((2, 2, 2, 6)), pltpu.SemaphoreType.DMA((2, 2, 2, 6)),
        pltpu.SemaphoreType.DMA((2, 2, 2, 6)), pltpu.SemaphoreType.DMA((2, 2, 2, 6)),
    ]
    call = pl.pallas_call(
        layer_kernel,
        out_shape=(jax.ShapeDtypeStruct((4, 4, 32, DM), BF), jax.ShapeDtypeStruct((160, SEQ), BF), jax.ShapeDtypeStruct((160, SEQ), BF)),
        in_specs=[pl.BlockSpec(memory_space=ANY)] * 11,
        out_specs=[pl.BlockSpec(memory_space=ANY)] * 3,
        scratch_shapes=scratch,
        compiler_params=pltpu.CompilerParams(collective_id=0, has_side_effects=True, vmem_limit_bytes=62 * 1024 * 1024),
        name="layer",
    )

    def device_step(tokens, gain_attn, gain_mlp, w_qkv, w_rel, w_out, w_up, w_down, bias_u, bias_v, rel_table, k_cache, v_cache, positions):
        odd = lax.axis_index("wg") % 2 == 1

        def window(w):
            return jnp.where(odd, jnp.pad(w, ((0, 0), (64, 0))), jnp.pad(w, ((0, 0), (0, 64))))

        wq = window(jnp.concatenate([w_qkv.transpose(1, 2, 3, 0).reshape(480, 320), w_rel.transpose(1, 2, 0).reshape(160, 320)]))
        wo = window(w_out.reshape(160, 320))
        gains = window(jnp.pad(jnp.stack([gain_attn, gain_mlp]), ((0, 6), (0, 0))))
        bias = jnp.pad(jnp.stack([bias_u.reshape(160), bias_v.reshape(160)], axis=1), ((0, 0), (0, 126)))
        out, k_new, v_new = call(
            tokens, positions.reshape(1, SEQ), bias, gains, wq, wo, w_up, w_down.T, rel_table,
            k_cache.transpose(1, 2, 3, 0), v_cache.transpose(1, 2, 3, 0))
        return (out.reshape(SEQ, DM), k_new.reshape(2, HD, SEQ).transpose(2, 0, 1), v_new.reshape(2, HD, SEQ).transpose(2, 0, 1))

    return jax.shard_map(device_step, mesh=mesh, in_specs=in_specs, out_specs=out_specs, check_vma=False)
```

```python
import jax
import jax.numpy as jnp
from jax import lax
from jax.experimental import pallas as pl
from jax.experimental.pallas import tpu as pltpu
from jax.sharding import PartitionSpec as P

NORM_EPS = 1e-6
BF = jnp.bfloat16
F32 = jnp.float32
MESH = pl.DeviceIdType.MESH
ANY = pl.ANY
SEQ, DM, HALF, HD, CL, FF = 512, 2560, 1280, 80, 32, 640
NT = (((1,), (1,)), ((), ()))
NN = (((1,), (0,)), ((), ()))
TN = (((0,), (0,)), ((), ()))


def mm(a, b, dims):
    return lax.dot_general(a, b, dims, preferred_element_type=F32)


def layer_kernel(x_h, pos_h, bu_h, bv_h, gain_h, wq_h, wr_h, wo_h, wu_h, wd_h, rt_h, k_h, v_h,
                 y_v, kn_s, vn_s,
                 x_s, pos_s, bu_s, bv_s, rt_s, wr_s, wg_s, wq_s, qp_s, wo_s, wu_s, wd_s, k_s, v_s,
                 rs_s, acc, qu_s, sc_s, ot_s, o_s, wof_s, p_s,
                 rel1, rcv1, stg1, rel2, rcv2, stg2, s2_s, h_s, g_s, u_s, hid_s,
                 lsem, gsem_s, gsem_r, rsem_s, rsem_r, asem_s, asem_r):
    tp, wg = lax.axis_index("tp"), lax.axis_index("wg")
    z, y = tp // 4, tp % 4
    x, c = wg // 2, wg % 2

    def up1(i, d):
        return lax.rem(i + d, 4)

    def dev(dz=0, dy=0, dx=0, flip=False):
        cc = 1 - c if flip else c
        return (0, up1(z, dz) * 4 + up1(y, dy), up1(x, dx) * 2 + cc)

    xp, xm, sib = dev(dx=1), dev(dx=3), dev(flip=True)
    zp, zm, yp, ym = dev(dz=1), dev(dz=3), dev(dy=1), dev(dy=3)

    sends = []

    def send(src, dst, ssem, rsem, device):
        cp = pltpu.make_async_remote_copy(src, dst, ssem, rsem, device_id=device, device_id_type=MESH)
        cp.start()
        sends.append(cp)

    def arrived(dst, ssem, rsem, device):
        pltpu.make_async_remote_copy(dst, dst, ssem, rsem, device_id=device, device_id_type=MESH).wait_recv()

    n_local = [0]

    def local(src, dst):
        cp = pltpu.make_async_copy(src, dst, lsem.at[n_local[0]])
        n_local[0] += 1
        cp.start()
        return cp

    own = 2 * x + c
    l_g = local(gain_h, wg_s.at[own])
    l_q = local(wq_h, wq_s.at[own])
    l_x = local(x_h, x_s)
    l_rt = local(rt_h, rt_s)
    l_pos = local(pos_h, pos_s)
    l_bu = local(bu_h, bu_s)
    l_bv = local(bv_h, bv_s)
    l_wr = local(wr_h, wr_s)
    l_wo = local(wo_h, wo_s.at[own])
    l_wu = local(wu_h, wu_s.at[own])
    l_wd = local(wd_h, wd_s.at[own])
    l_k = local(k_h, k_s)
    l_v = local(v_h, v_s)

    barrier = pltpu.get_barrier_semaphore()
    for d in (xp, xm, sib, zp, zm, yp, ym):
        pl.semaphore_signal(barrier, inc=1, device_id=d, device_id_type=MESH)
    pl.semaphore_wait(barrier, 7)

    def slot(dx, flip=False):
        return 2 * up1(x, dx) + (1 - c if flip else c)

    class Gather:
        def __init__(self, ar, buf, rows, split=True):
            self.ar, self.buf, self.rows, self.split = ar, buf, rows, split

        def ref(self, s, part):
            if part is None:
                return self.buf.at[s]
            n = self.rows // 2
            return self.buf.at[s, pl.ds(part * n, n)]

        def sems(self, k):
            return gsem_s.at[self.ar, k], gsem_r.at[self.ar, k]

        def put(self, k, s, part, device):
            r = self.ref(s, part)
            send(r, r, *self.sems(k), device)

        def got(self, k, s, part, device):
            arrived(self.ref(s, part), *self.sems(k), device)

        def start(self):
            o = slot(0)
            if self.split:
                self.put(0, o, 0, xp)
                self.put(2, o, 1, xm)
                self.put(1, o, 1, xp)
                self.put(3, o, 0, xm)
            else:
                self.put(0, o, None, xp)
                self.put(2, o, None, xm)
            self.put(6, o, None, sib)

        def forward(self):
            if self.split:
                self.got(0, slot(3), 0, xm)
                self.put(4, slot(3), 0, xp)
                self.got(2, slot(1), 1, xp)
                self.put(5, slot(1), 1, xm)
                self.got(1, slot(3), 1, xm)
                self.got(3, slot(1), 0, xp)
            else:
                self.got(0, slot(3), None, xm)
                self.put(4, slot(3), None, xp)
                self.got(2, slot(1), None, xp)
            self.put(7, slot(3), None, sib)
            self.put(8, slot(1), None, sib)

        def last(self):
            if self.split:
                self.got(4, slot(2), 0, xm)
                self.got(5, slot(2), 1, xp)
            else:
                self.got(4, slot(2), None, xm)
            self.put(9, slot(2), None, sib)

        def sibling(self, k):
            self.got(k, slot({6: 0, 7: 3, 8: 1, 9: 2}[k], True), None, sib)

    g_g = Gather(0, wg_s, 8, split=False)
    g_q = Gather(1, wq_s, 480)
    g_o = Gather(2, wo_s, 160)
    g_u = Gather(3, wu_s, 320)
    g_d = Gather(4, wd_s, 320)
    g_r = Gather(5, qp_s, 32)

    l_g.wait()
    g_g.start()
    l_q.wait()
    g_q.start()

    l_x.wait()

    def stat_rows(r, carry):
        rows = pl.ds(pl.multiple_of(r * 32, 32), 32)
        v = x_s[rows, :].astype(F32)
        ms = jnp.sum(v * v, axis=1, keepdims=True) * (1.0 / DM)
        rs_s[rows, :] = jnp.broadcast_to(lax.rsqrt(ms + NORM_EPS), (32, 128))
        return carry

    lax.fori_loop(0, 16, stat_rows, 0)
    l_rt.wait()
    l_wr.wait()
    base = pl.multiple_of(640 * x, 128)
    q_even = mm(rt_s[:, pl.ds(base, 384)][:, 0:320], wr_s[...], NT)
    q_odd = mm(rt_s[:, pl.ds(pl.multiple_of(base + 256, 128), 384)][:, 64:384], wr_s[...], NT)
    qp_s[own] = jnp.where(c == 1, q_odd, q_even)
    g_r.start()
    acc[...] = jnp.zeros_like(acc)
    u_s[...] = jnp.zeros_like(u_s)

    def qkv_pair(dx):
        xo = up1(x, dx)
        cols = pl.ds(pl.multiple_of(xo * 640, 128), 640)
        gain = jnp.concatenate([wg_s[2 * xo, 0:1, :], wg_s[2 * xo + 1, 0:1, :]], axis=1)
        n_win = (x_s[:, cols].astype(F32) * rs_s[:, 0:1] * gain).astype(BF)
        w = jnp.concatenate([wq_s[2 * xo], wq_s[2 * xo + 1]], axis=1)
        acc[...] += mm(w, n_win, NT)

    g_g.forward()
    g_g.last()
    for k in (6, 7, 8, 9):
        g_g.sibling(k)
    g_q.sibling(6)
    qkv_pair(0)
    g_q.forward()
    g_r.forward()
    l_wo.wait()
    g_o.start()
    g_q.sibling(7)
    qkv_pair(3)
    g_q.sibling(8)
    qkv_pair(1)
    g_q.last()
    g_r.last()
    g_q.sibling(9)
    qkv_pair(2)

    kn_s[...] = acc[160:320, :].astype(BF)
    vn_s[...] = acc[320:480, :].astype(BF)
    l_pos.wait()
    l_bu.wait()
    l_bv.wait()
    for k in (6, 7, 8, 9):
        g_r.sibling(k)

    flip_rows = (lax.broadcasted_iota(jnp.int32, (CL, CL), 0) + lax.broadcasted_iota(jnp.int32, (CL, CL), 1)) % CL == 0
    flip_mat = jnp.where(flip_rows, 1.0, 0.0).astype(BF)
    q_rel = qp_s[0]
    for i in range(1, 8):
        q_rel = q_rel + qp_s[i]
    rel_rev = mm(flip_mat, q_rel.astype(BF), NN).astype(BF)
    diag = lax.broadcasted_iota(jnp.int32, (HD, HD), 0) == lax.broadcasted_iota(jnp.int32, (HD, HD), 1)

    def column(row):
        return jnp.sum(jnp.where(diag, row, 0.0), axis=1, keepdims=True)

    pos = pos_s[...]
    steps = lax.broadcasted_iota(jnp.int32, (CL, SEQ), 0)
    is_self = steps == pos
    l_k.wait()
    l_v.wait()

    for h in range(2):
        hr = slice(h * HD, h * HD + HD)
        q = acc[hr, :].astype(BF).astype(F32)
        q_u = (q + column(bu_s[h:h + 1, :])).astype(BF).astype(F32)
        q_v = (q + column(bv_s[h:h + 1, :])).astype(BF)
        qu_s[...] = q_u
        rel = mm(rel_rev[:, hr], q_v, NN)
        for b in range(5):
            rel = jnp.where((pos >> b) & 1 == 1, pltpu.roll(rel, 1 << b, 0), rel)
        self_score = jnp.sum(q_u * kn_s[hr, :].astype(F32), axis=0, keepdims=True)
        for lc in range(4):
            ln = slice(lc * 128, lc * 128 + 128)
            quc = qu_s[:, ln]

            def content(g, carry, h=h, ln=ln, quc=quc):
                rows = [jnp.sum(k_s[h, g * 8 + j, :, ln].astype(F32) * quc, axis=0, keepdims=True) for j in range(8)]
                sc_s[pl.ds(pl.multiple_of(g * 8, 8), 8), ln] = jnp.concatenate(rows, axis=0)
                return carry

            lax.fori_loop(0, CL // 8, content, 0)
        scores = jnp.where(is_self, self_score, sc_s[...])
        scores = jnp.where(steps <= pos, (scores + rel) * (HD ** -0.5), -1e30)
        e = jnp.exp(scores - jnp.max(scores, axis=0, keepdims=True))
        prob = (e / jnp.sum(e, axis=0, keepdims=True)).astype(BF).astype(F32)
        self_prob = jnp.sum(jnp.where(is_self, prob, 0.0), axis=0, keepdims=True)
        sc_s[...] = jnp.where(is_self, 0.0, prob)
        for lc in range(4):
            ln = slice(lc * 128, lc * 128 + 128)

            def mix(g, o, h=h, ln=ln):
                pr = sc_s[pl.ds(pl.multiple_of(g * 8, 8), 8), ln]
                for j in range(8):
                    o = o + pr[j:j + 1, :] * v_s[h, g * 8 + j, :, ln].astype(F32)
                return o

            start = self_prob[:, ln] * vn_s[hr, ln].astype(F32)
            ot_s[hr, ln] = lax.fori_loop(0, CL // 8, mix, start)
        if h == 0:
            g_o.forward()
            l_wu.wait()
            g_u.start()
            l_wd.wait()
            g_d.start()

    o_s[...] = jnp.transpose(ot_s[...]).astype(BF).reshape(4, 4, 32, 160)
    g_o.last()
    for k in (6, 7, 8, 9):
        g_o.sibling(k)
    for xo in range(4):
        wof_s[:, 640 * xo:640 * xo + 640] = jnp.concatenate([wo_s[2 * xo], wo_s[2 * xo + 1]], axis=1)

    place = ((z, y, zp, zm, yp, ym), (y, z, yp, ym, zp, zm))

    def reduce_scatter(ps, chunk, between):
        for hf in range(2):
            a, b, ap, am, _, _ = place[hf]
            ss, rr = rsem_s.at[ps, hf, 0], rsem_r.at[ps, hf, 0]
            chunk(hf, up1(a, 2))
            send(p_s.at[ps, hf, up1(a, 2), pl.ds(0, 2)], rel1.at[ps, hf, 0], ss.at[0], rr.at[0], ap)
            send(p_s.at[ps, hf, up1(a, 2), pl.ds(2, 2)], rel1.at[ps, hf, 1], ss.at[1], rr.at[1], am)
        for hf in range(2):
            a, b, ap, am, _, _ = place[hf]
            ss, rr = rsem_s.at[ps, hf, 0], rsem_r.at[ps, hf, 0]
            chunk(hf, up1(a, 1))
            send(p_s.at[ps, hf, up1(a, 1), pl.ds(2, 2)], rcv1.at[ps, hf, 0, pl.ds(2, 2)], ss.at[2], rr.at[2], ap)
            chunk(hf, up1(a, 3))
            send(p_s.at[ps, hf, up1(a, 3), pl.ds(0, 2)], rcv1.at[ps, hf, 1, pl.ds(0, 2)], ss.at[3], rr.at[3], am)
        for hf in range(2):
            chunk(hf, place[hf][0])
        for hf in range(2):
            a, b, ap, am, _, _ = place[hf]
            ss, rr = rsem_s.at[ps, hf, 0], rsem_r.at[ps, hf, 0]
            arrived(rel1.at[ps, hf, 0], ss.at[0], rr.at[0], am)
            stg1[ps, hf, 0] = (p_s[ps, hf, up1(a, 1), 0:2].astype(F32) + rel1[ps, hf, 0].astype(F32)).astype(BF)
            send(stg1.at[ps, hf, 0], rcv1.at[ps, hf, 0, pl.ds(0, 2)], ss.at[4], rr.at[4], ap)
            arrived(rel1.at[ps, hf, 1], ss.at[1], rr.at[1], ap)
            stg1[ps, hf, 1] = (p_s[ps, hf, up1(a, 3), 2:4].astype(F32) + rel1[ps, hf, 1].astype(F32)).astype(BF)
            send(stg1.at[ps, hf, 1], rcv1.at[ps, hf, 1, pl.ds(2, 2)], ss.at[5], rr.at[5], am)
        between(0)
        for hf in range(2):
            a, b, ap, am, bp, bm = place[hf]
            ss, rr = rsem_s.at[ps, hf, 0], rsem_r.at[ps, hf, 0]
            arrived(rcv1.at[ps, hf, 0, pl.ds(2, 2)], ss.at[2], rr.at[2], am)
            arrived(rcv1.at[ps, hf, 1, pl.ds(0, 2)], ss.at[3], rr.at[3], ap)
            arrived(rcv1.at[ps, hf, 0, pl.ds(0, 2)], ss.at[4], rr.at[4], am)
            arrived(rcv1.at[ps, hf, 1, pl.ds(2, 2)], ss.at[5], rr.at[5], ap)
            for j in (2, 1, 3, 0):
                bj = up1(b, j)
                s2_s[ps, hf, bj] = (p_s[ps, hf, a, bj].astype(F32) + rcv1[ps, hf, 0, bj].astype(F32)
                                    + rcv1[ps, hf, 1, bj].astype(F32)).astype(BF)
                ss, rr = rsem_s.at[ps, hf, 1], rsem_r.at[ps, hf, 1]
                if j == 2:
                    send(s2_s.at[ps, hf, bj, pl.ds(0, 16)], rel2.at[ps, hf, 0], ss.at[0], rr.at[0], bp)
                    send(s2_s.at[ps, hf, bj, pl.ds(16, 16)], rel2.at[ps, hf, 1], ss.at[1], rr.at[1], bm)
                elif j == 1:
                    send(s2_s.at[ps, hf, bj, pl.ds(16, 16)], rcv2.at[ps, hf, 0, pl.ds(16, 16)], ss.at[2], rr.at[2], bp)
                elif j == 3:
                    send(s2_s.at[ps, hf, bj, pl.ds(0, 16)], rcv2.at[ps, hf, 1, pl.ds(0, 16)], ss.at[3], rr.at[3], bm)
        for hf in range(2):
            a, b, ap, am, bp, bm = place[hf]
            ss, rr = rsem_s.at[ps, hf, 1], rsem_r.at[ps, hf, 1]
            arrived(rel2.at[ps, hf, 0], ss.at[0], rr.at[0], bm)
            stg2[ps, hf, 0] = (s2_s[ps, hf, up1(b, 1), 0:16].astype(F32) + rel2[ps, hf, 0].astype(F32)).astype(BF)
            send(stg2.at[ps, hf, 0], rcv2.at[ps, hf, 0, pl.ds(0, 16)], ss.at[4], rr.at[4], bp)
            arrived(rel2.at[ps, hf, 1], ss.at[1], rr.at[1], bp)
            stg2[ps, hf, 1] = (s2_s[ps, hf, up1(b, 3), 16:32].astype(F32) + rel2[ps, hf, 1].astype(F32)).astype(BF)
            send(stg2.at[ps, hf, 1], rcv2.at[ps, hf, 1, pl.ds(16, 16)], ss.at[5], rr.at[5], bm)
        between(1)
        out = []
        for hf in range(2):
            a, b, ap, am, bp, bm = place[hf]
            ss, rr = rsem_s.at[ps, hf, 1], rsem_r.at[ps, hf, 1]
            arrived(rcv2.at[ps, hf, 0, pl.ds(16, 16)], ss.at[2], rr.at[2], bm)
            arrived(rcv2.at[ps, hf, 1, pl.ds(0, 16)], ss.at[3], rr.at[3], bp)
            arrived(rcv2.at[ps, hf, 0, pl.ds(0, 16)], ss.at[4], rr.at[4], bm)
            arrived(rcv2.at[ps, hf, 1, pl.ds(16, 16)], ss.at[5], rr.at[5], bp)
            out.append(s2_s[ps, hf, b].astype(F32) + rcv2[ps, hf, 0].astype(F32) + rcv2[ps, hf, 1].astype(F32))
        return out

    class Ring:
        def __init__(self, ps, ph, hf):
            a, b, ap, am, bp, bm = place[hf]
            self.ps, self.ph, self.hf, self.a = ps, ph, hf, a
            self.i, self.fwd, self.bwd = (b, bp, bm) if ph == 0 else (a, ap, am)

        def ref(self, d, part):
            i = up1(self.i, d)
            buf, cols = (g_s, y_v)[self.ps], pl.ds(self.hf * HALF, HALF)
            rows = pl.ds(part * 16, 16) if self.ph == 0 else pl.ds(part * 2, 2)
            if self.ph == 0:
                return buf.at[z, i, rows, cols] if self.hf == 0 else buf.at[i, y, rows, cols]
            return buf.at[i, rows, :, cols] if self.hf == 0 else buf.at[rows, i, :, cols]

        def sems(self, k):
            return asem_s.at[self.ps, self.hf, self.ph, k], asem_r.at[self.ps, self.hf, self.ph, k]

        def put(self, k, d, part, device):
            r = self.ref(d, part)
            send(r, r, *self.sems(k), device)

        def got(self, k):
            d, part, device = {0: (3, 0, self.bwd), 1: (1, 1, self.fwd), 2: (3, 1, self.bwd),
                               3: (1, 0, self.fwd), 4: (2, 0, self.bwd), 5: (2, 1, self.fwd)}[k]
            arrived(self.ref(d, part), *self.sems(k), device)

        def start(self):
            self.put(0, 0, 0, self.fwd)
            self.put(1, 0, 1, self.bwd)
            self.put(2, 0, 1, self.fwd)
            self.put(3, 0, 0, self.bwd)

        def forward(self):
            self.got(0)
            self.put(4, 3, 0, self.fwd)
            self.got(1)
            self.put(5, 1, 1, self.bwd)

    def all_gather(ps, consume):
        inner = [Ring(ps, 0, hf) for hf in range(2)]
        outer = [Ring(ps, 1, hf) for hf in range(2)]
        for r in inner:
            r.start()
        for r in inner:
            r.forward()
        for hf in range(2):
            for k in (2, 3, 4, 5):
                inner[hf].got(k)
            outer[hf].start()
        for hf in range(2):
            consume(hf, outer[hf].i)
        for r in outer:
            r.forward()
        for k, d in ((2, 3), (3, 1)):
            for hf in range(2):
                outer[hf].got(k)
                consume(hf, up1(outer[hf].i, d))
        for hf in range(2):
            outer[hf].got(4)
            outer[hf].got(5)
            consume(hf, up1(outer[hf].i, 2))

    def out_chunk(hf, i):
        rows = (o_s[i] if hf == 0 else o_s[:, i]).reshape(128, 160)
        part = mm(rows, wof_s[:, hf * HALF:hf * HALF + HALF], NN)
        p_s[0, hf, i] = part.astype(BF).reshape(4, 32, HALF)

    def attn_between(step):
        if step == 1:
            g_u.forward()

    part = reduce_scatter(0, out_chunk, attn_between)
    mine = pl.ds(pl.multiple_of(tp * 32, 32), 32)
    for hf in range(2):
        cols = slice(hf * HALF, hf * HALF + HALF)
        h_s[:, cols] = x_s[mine, cols].astype(F32) + part[hf]
    resid = h_s[...]
    inv = lax.rsqrt(jnp.sum(resid * resid, axis=1, keepdims=True) * (1.0 / DM) + NORM_EPS)
    gain = jnp.concatenate([wg_s[i, 1:2, :] for i in range(8)], axis=1)
    g_s[z, y] = (resid * inv * gain).astype(BF)

    first = [True]

    def up_part(hf, i):
        if first[0]:
            first[0] = False
            g_u.last()
            g_d.forward()
            for k in (6, 7, 8, 9):
                g_u.sibling(k)
        w = wu_s[4 * hf:4 * hf + 4].reshape(HALF, FF)
        cols = slice(hf * HALF, hf * HALF + HALF)
        rows = (g_s[i, :, :, cols] if hf == 0 else g_s[:, i, :, cols]).reshape(128, HALF)
        prod = mm(rows, w, NN).reshape(4, 32, FF)
        if hf == 0:
            u_s[i] += prod
        else:
            u_s[:, i] += prod

    all_gather(0, up_part)
    g_d.last()
    for k in (6, 7, 8, 9):
        g_d.sibling(k)
    for i in range(4):
        hid_s[i] = jax.nn.gelu(u_s[i], approximate=True).astype(BF)

    def down_chunk(hf, i):
        rows = (hid_s[i] if hf == 0 else hid_s[:, i]).reshape(128, FF)
        w = wd_s[4 * hf:4 * hf + 4].reshape(HALF, FF)
        p_s[1, hf, i] = mm(rows, w, NT).astype(BF).reshape(4, 32, HALF)

    part = reduce_scatter(1, down_chunk, lambda step: None)
    y_v[z, y] = jnp.concatenate([h_s[:, 0:HALF] + part[0], h_s[:, HALF:DM] + part[1]], axis=1).astype(BF)
    all_gather(1, lambda hf, i: None)
    for cp in sends:
        cp.wait_send()


def solution(mesh):
    tok_axes = ("dp", "wg")
    in_specs = (P(tok_axes, None), P("wg"), P("wg"), P("wg", None, "tp", None), P("wg", "tp", None), P("tp", None, "wg"), P("wg", "tp"), P("tp", "wg"), P("tp", None), P("tp", None), P(None, None), P(tok_axes, "tp", None, None), P(tok_axes, "tp", None, None), P(tok_axes))
    out_specs = (P(tok_axes, None), P(tok_axes, "tp", None), P(tok_axes, "tp", None))

    def vm(shape, dtype=BF):
        return pltpu.VMEM(shape, dtype)

    scratch = [
        vm((SEQ, DM)), vm((1, SEQ), jnp.int32), vm((2, HD), F32), vm((2, HD), F32), vm((CL, DM)), vm((160, 320)),
        vm((8, 2, 320), F32), vm((8, 480, 320)), vm((8, CL, 160), F32), vm((8, 160, 320)), vm((8, 320, FF)), vm((8, 320, FF)),
        vm((2, CL, HD, SEQ)), vm((2, CL, HD, SEQ)),
        vm((SEQ, 128), F32), vm((480, SEQ), F32), vm((HD, SEQ), F32), vm((CL, SEQ), F32),
        vm((160, SEQ), F32), vm((4, 4, 32, 160)), vm((160, DM)),
        vm((2, 2, 4, 4, 32, HALF)),
        vm((2, 2, 2, 2, 32, HALF)), vm((2, 2, 2, 4, 32, HALF)), vm((2, 2, 2, 2, 32, HALF)),
        vm((2, 2, 2, 16, HALF)), vm((2, 2, 2, 32, HALF)), vm((2, 2, 2, 16, HALF)),
        vm((2, 2, 4, 32, HALF)), vm((32, DM), F32), vm((4, 4, 32, DM)),
        vm((4, 4, 32, FF), F32), vm((4, 4, 32, FF)),
        pltpu.SemaphoreType.DMA((24,)),
        pltpu.SemaphoreType.DMA((6, 10)), pltpu.SemaphoreType.DMA((6, 10)),
        pltpu.SemaphoreType.DMA((2, 2, 2, 6)), pltpu.SemaphoreType.DMA((2, 2, 2, 6)),
        pltpu.SemaphoreType.DMA((2, 2, 2, 6)), pltpu.SemaphoreType.DMA((2, 2, 2, 6)),
    ]
    call = pl.pallas_call(
        layer_kernel,
        out_shape=(pltpu.VMEM((4, 4, 32, DM), BF), pltpu.VMEM((160, SEQ), BF), pltpu.VMEM((160, SEQ), BF)),
        in_specs=[pl.BlockSpec(memory_space=ANY)] * 13,
        out_specs=[pl.BlockSpec(memory_space=pltpu.VMEM)] * 3,
        scratch_shapes=scratch,
        compiler_params=pltpu.CompilerParams(collective_id=0, has_side_effects=True, vmem_limit_bytes=56 * 1024 * 1024),
        name="layer",
    )

    def device_step(tokens, gain_attn, gain_mlp, w_qkv, w_rel, w_out, w_up, w_down, bias_u, bias_v, rel_table, k_cache, v_cache, positions):
        out, k_new, v_new = call(
            tokens, positions.reshape(1, SEQ), bias_u, bias_v, jnp.stack([gain_attn, gain_mlp]),
            w_qkv.transpose(1, 2, 3, 0).reshape(480, 320), w_rel.transpose(1, 2, 0).reshape(160, 320),
            w_out.reshape(160, 320), w_up, w_down.T, rel_table,
            k_cache.transpose(1, 2, 3, 0), v_cache.transpose(1, 2, 3, 0))
        return (out.reshape(SEQ, DM), k_new.reshape(2, HD, SEQ).transpose(2, 0, 1), v_new.reshape(2, HD, SEQ).transpose(2, 0, 1))

    return jax.shard_map(device_step, mesh=mesh, in_specs=in_specs, out_specs=out_specs, check_vma=False)
```

```python
import jax
import jax.numpy as jnp
from jax import lax
from jax.experimental import pallas as pl
from jax.experimental.pallas import tpu as pltpu
from jax.sharding import PartitionSpec as P

NORM_EPS = 1e-6
BF = jnp.bfloat16
F32 = jnp.float32
MESH = pl.DeviceIdType.MESH
ANY = pl.ANY
SEQ, DM, HALF, HD, CL, FF = 512, 2560, 1280, 80, 32, 640
SLICE, HW = 320, 160
ME, NEXT, FAR, PREV, TAIL = range(5)
LO, HI, WHOLE = 0, 1, None
ORDER = (FAR, NEXT, PREV, ME)
NT = (((1,), (1,)), ((), ()))
NN = (((1,), (0,)), ((), ()))
TN = (((0,), (0,)), ((), ()))


def mm(a, b, dims):
    return lax.dot_general(a, b, dims, preferred_element_type=F32)


def layer_kernel(x_h, pos_h, bu_h, bv_h, ga_h, gm_h, wq_h, wr_h, wo_h, wu_h, wd_h, rt_h, k_h, v_h,
                 y_v, kn_s, vn_s,
                 x_s, pos_s, bu_s, bv_s, rt_s, wr_s, wg_s, wq_s, qp_s, wo_s, wu_s, wd_s, k_s, v_s,
                 rs_s, acc, qu_s, sc_s, ot_s, o_s, wof_s, p_s, rel_s, rcv_s, stg_s, s2_s, h_s, g_s, u_s, hid_s,
                 lsem, gsem_s, gsem_r, msem_s, rsem, asem):
    tp, wg = lax.axis_index("tp"), lax.axis_index("wg")
    z, y = tp // 4, tp % 4
    x, c = wg // 2, wg % 2

    def up1(i, d):
        return lax.rem(i + d, 4)

    def dev(dz=0, dy=0, dx=0, flip=False):
        cc = 1 - c if flip else c
        return (0, up1(z, dz) * 4 + up1(y, dy), up1(x, dx) * 2 + cc)

    xp, xm, sib = dev(dx=1), dev(dx=3), dev(flip=True)
    zp, zm, yp, ym = dev(dz=1), dev(dz=3), dev(dy=1), dev(dy=3)

    def send(src, dst, ssem, rsem, device):
        pltpu.make_async_remote_copy(src, dst, ssem, rsem, device_id=device, device_id_type=MESH).start()

    def sent(ref, ssem, rsem):
        pltpu.make_async_remote_copy(ref, ref, ssem, rsem, device_id=sib, device_id_type=MESH).wait_send()

    def arrived(dst, rsem):
        pltpu.make_async_remote_copy(dst, dst, gsem_s.at[0], rsem, device_id=sib, device_id_type=MESH).wait_recv()

    n_local = [0]

    def local(src, dst):
        cp = pltpu.make_async_copy(src, dst, lsem.at[n_local[0]])
        n_local[0] += 1
        cp.start()
        return cp

    own = 2 * x + c
    l_g = [local(ga_h, wg_s.at[own, 0, 0]), local(gm_h, wg_s.at[own, 1, 0])]
    l_q = local(wq_h, wq_s.at[own])
    l_x = local(x_h, x_s)
    l_rt = local(rt_h, rt_s)
    l_pos = local(pos_h, pos_s)
    l_bu = local(bu_h, bu_s)
    l_bv = local(bv_h, bv_s)
    l_wr = local(wr_h, wr_s)
    l_wo = local(wo_h, wo_s.at[own])
    l_wu = local(wu_h, wu_s.at[own])
    l_wd = local(wd_h, wd_s.at[own])
    l_k = local(k_h, k_s)
    l_v = local(v_h, v_s)

    barrier = pltpu.get_barrier_semaphore()
    for d in (xp, xm, sib, zp, zm, yp, ym):
        pl.semaphore_signal(barrier, inc=1, device_id=d, device_id_type=MESH)
    pl.semaphore_wait(barrier, 7)

    def slot(dx, flip=False):
        return 2 * up1(x, dx) + (1 - c if flip else c)

    class Gather:
        def __init__(self, ar, buf, rows):
            self.ar, self.buf, self.rows = ar, buf, rows

        def ref(self, s, part):
            n = self.rows // 2
            return self.buf.at[s] if part is WHOLE else self.buf.at[s, pl.ds(part * n, n)]

        def put(self, k, s, part, device):
            r = self.ref(s, part)
            send(r, r, gsem_s.at[self.ar], gsem_r.at[self.ar, k], device)

        def got(self, k, s, part):
            arrived(self.ref(s, part), gsem_r.at[self.ar, k])

        def start(self):
            o = slot(ME)
            self.put(0, o, LO, xp)
            self.put(1, o, HI, xm)
            self.put(2, o, HI, xp)
            self.put(3, o, LO, xm)
            self.put(6, o, WHOLE, sib)

        def forward(self):
            self.got(0, slot(PREV), LO)
            self.put(4, slot(PREV), LO, xp)
            self.got(1, slot(NEXT), HI)
            self.put(5, slot(NEXT), HI, xm)

        def share(self):
            self.got(2, slot(PREV), HI)
            self.put(7, slot(PREV), WHOLE, sib)
            self.got(3, slot(NEXT), LO)
            self.put(8, slot(NEXT), WHOLE, sib)

        def last(self):
            self.got(4, slot(FAR), LO)
            self.got(5, slot(FAR), HI)
            self.put(9, slot(FAR), WHOLE, sib)

        def sibling(self, dx):
            self.got({ME: 6, PREV: 7, NEXT: 8, FAR: 9}[dx], slot(dx, True), WHOLE)

        def siblings(self):
            for dx in (ME, PREV, NEXT, FAR):
                self.sibling(dx)

        def all_sent(self):
            sent(self.buf.at[pl.ds(0, 7)], gsem_s.at[self.ar], gsem_r.at[self.ar, 0])

    g_g, g_q, g_o, g_u, g_d, g_r = gathers = [Gather(i, b, r) for i, (b, r) in enumerate((
        (wg_s, 2), (wq_s, 480), (wo_s, 160), (wu_s, 320), (wd_s, 320), (qp_s, CL)))]

    for cp in l_g:
        cp.wait()
    g_g.start()
    l_q.wait()
    g_q.start()

    l_x.wait()

    def stat_rows(r, carry):
        rows = pl.ds(pl.multiple_of(r * 32, 32), 32)
        v = x_s[rows, :].astype(F32)
        ms = jnp.sum(v * v, axis=1, keepdims=True) * (1.0 / DM)
        rs_s[rows, :] = jnp.broadcast_to(lax.rsqrt(ms + NORM_EPS), (32, 128))
        return carry

    lax.fori_loop(0, 16, stat_rows, 0)
    l_rt.wait()
    l_wr.wait()
    base = pl.multiple_of(640 * x, 128)
    q_even = mm(rt_s[:, pl.ds(base, 384)][:, 0:320], wr_s[...], NT)
    q_odd = mm(rt_s[:, pl.ds(pl.multiple_of(base + 256, 128), 384)][:, 64:384], wr_s[...], NT)
    qp_s[own] = jnp.where(c == 1, q_odd, q_even)
    g_r.start()
    acc[...] = jnp.zeros_like(acc)
    u_s[...] = jnp.zeros_like(u_s)

    def qkv_pair(dx):
        xo = up1(x, dx)
        cols = pl.ds(pl.multiple_of(xo * 640, 128), 640)
        gain = jnp.concatenate([wg_s[2 * xo, 0], wg_s[2 * xo + 1, 0]], axis=1)
        n_win = (x_s[:, cols].astype(F32) * rs_s[:, 0:1] * gain).astype(BF)
        w = jnp.concatenate([wq_s[2 * xo], wq_s[2 * xo + 1]], axis=1)
        acc[...] += mm(w, n_win, NT)

    g_g.sibling(ME)
    g_q.sibling(ME)
    qkv_pair(ME)
    g_g.forward()
    g_q.forward()
    g_g.share()
    g_q.share()
    g_r.forward()
    g_r.share()
    l_wo.wait()
    g_o.start()
    g_g.last()
    for dx in (PREV, NEXT, FAR):
        g_g.sibling(dx)
        g_q.sibling(dx)
        qkv_pair(dx)
        if dx == PREV:
            g_q.last()
            g_r.last()

    kn_s[...] = acc[160:320, :].astype(BF)
    vn_s[...] = acc[320:480, :].astype(BF)
    l_pos.wait()
    l_bu.wait()
    l_bv.wait()
    g_r.siblings()
    g_o.forward()
    g_o.share()
    l_wu.wait()
    g_u.start()
    l_wd.wait()
    g_d.start()

    flip_rows = (lax.broadcasted_iota(jnp.int32, (CL, CL), 0) + lax.broadcasted_iota(jnp.int32, (CL, CL), 1)) % CL == 0
    flip_mat = jnp.where(flip_rows, 1.0, 0.0).astype(BF)
    q_rel = qp_s[0]
    for i in range(1, 8):
        q_rel = q_rel + qp_s[i]
    rel_rev = mm(flip_mat, q_rel.astype(BF), NN).astype(BF)
    diag = lax.broadcasted_iota(jnp.int32, (HD, HD), 0) == lax.broadcasted_iota(jnp.int32, (HD, HD), 1)

    def column(row):
        return jnp.sum(jnp.where(diag, row, 0.0), axis=1, keepdims=True)

    pos = pos_s[...]
    steps = lax.broadcasted_iota(jnp.int32, (CL, SEQ), 0)
    is_self = steps == pos
    l_k.wait()
    l_v.wait()

    for h in range(2):
        hr = slice(h * HD, h * HD + HD)
        q = acc[hr, :].astype(BF).astype(F32)
        q_u = (q + column(bu_s[h:h + 1, :])).astype(BF).astype(F32)
        q_v = (q + column(bv_s[h:h + 1, :])).astype(BF)
        qu_s[...] = q_u
        rel = mm(rel_rev[:, hr], q_v, NN)
        for b in range(5):
            rel = jnp.where((pos >> b) & 1 == 1, pltpu.roll(rel, 1 << b, 0), rel)
        self_score = jnp.sum(q_u * kn_s[hr, :].astype(F32), axis=0, keepdims=True)
        for lc in range(4):
            ln = slice(lc * 128, lc * 128 + 128)
            quc = qu_s[:, ln]

            def content(g, carry, h=h, ln=ln, quc=quc):
                rows = [jnp.sum(k_s[h, g * 8 + j, :, ln].astype(F32) * quc, axis=0, keepdims=True) for j in range(8)]
                sc_s[pl.ds(pl.multiple_of(g * 8, 8), 8), ln] = jnp.concatenate(rows, axis=0)
                return carry

            lax.fori_loop(0, CL // 8, content, 0)
        if h == 1:
            g_o.last()
        scores = jnp.where(is_self, self_score, sc_s[...])
        scores = jnp.where(steps <= pos, (scores + rel) * (HD ** -0.5), -1e30)
        e = jnp.exp(scores - jnp.max(scores, axis=0, keepdims=True))
        prob = (e / jnp.sum(e, axis=0, keepdims=True)).astype(BF).astype(F32)
        self_prob = jnp.sum(jnp.where(is_self, prob, 0.0), axis=0, keepdims=True)
        sc_s[...] = jnp.where(is_self, 0.0, prob)
        for lc in range(4):
            ln = slice(lc * 128, lc * 128 + 128)

            def mix(g, o, h=h, ln=ln):
                pr = sc_s[pl.ds(pl.multiple_of(g * 8, 8), 8), ln]
                for j in range(8):
                    o = o + pr[j:j + 1, :] * v_s[h, g * 8 + j, :, ln].astype(F32)
                return o

            start = self_prob[:, ln] * vn_s[hr, ln].astype(F32)
            ot_s[hr, ln] = lax.fori_loop(0, CL // 8, mix, start)

    o_s[...] = jnp.transpose(ot_s[...]).astype(BF).reshape(4, 4, 32, 160)
    g_o.siblings()
    for xo in range(4):
        wof_s[:, 640 * xo:640 * xo + 640] = jnp.concatenate([wo_s[2 * xo], wo_s[2 * xo + 1]], axis=1)

    place = ((z, y, zp, zm, yp, ym), (y, z, yp, ym, zp, zm))

    lo, hi = pl.ds(0, 16), pl.ds(16, 16)

    class Exchange:
        def __init__(self, ps, hf, e, src, fwd, bwd):
            self.src, self.fwd, self.bwd, self.sem = src, fwd, bwd, rsem.at[hf, e]
            self.ssem = msem_s.at[ps, 0, 0 if e == TAIL else 1]
            self.rel, self.rcv, self.stg = rel_s.at[ps, hf, e], rcv_s.at[ps, hf, e], stg_s.at[ps, hf, e]

        def relay(self):
            send(self.src(FAR).at[lo], self.rel.at[LO], self.ssem, self.sem.at[0], self.fwd)
            send(self.src(FAR).at[hi], self.rel.at[HI], self.ssem, self.sem.at[1], self.bwd)

        def direct(self, d):
            if d == NEXT:
                send(self.src(NEXT).at[hi], self.rcv.at[0, hi], self.ssem, self.sem.at[2], self.fwd)
            else:
                send(self.src(PREV).at[lo], self.rcv.at[1, lo], self.ssem, self.sem.at[3], self.bwd)

        def join(self):
            for part, rows, d, device in ((LO, lo, NEXT, self.fwd), (HI, hi, PREV, self.bwd)):
                arrived(self.rel.at[part], self.sem.at[part])
                both = self.src(d).at[rows][...].astype(F32) + self.rel.at[part][...].astype(F32)
                self.stg.at[part][...] = both.astype(BF)
                send(self.stg.at[part], self.rcv.at[part, rows], self.ssem, self.sem.at[4 + part], device)

        def received(self):
            for k, way, rows in ((2, 0, hi), (3, 1, lo), (4, 0, lo), (5, 1, hi)):
                arrived(self.rcv.at[way, rows], self.sem.at[k])
            return self.rcv.at[0][...].astype(F32) + self.rcv.at[1][...].astype(F32)

        def total(self):
            return self.received() + self.src(ME)[...].astype(F32)

    def reduce_scatter(ps, chunk, between):
        first, second = [], []
        for hf in range(2):
            a, b, ap, am, bp, bm = place[hf]
            first.append([Exchange(ps, hf, j, lambda d, hf=hf, a=a, b=b, j=j: p_s.at[ps, hf, up1(a, d), up1(b, j)], ap, am)
                          for j in range(4)])
            second.append(Exchange(ps, hf, TAIL, lambda d, hf=hf: s2_s.at[ps, hf, d], bp, bm))

        def directs(hf, j):
            first[hf][j].direct(NEXT)
            first[hf][j].direct(PREV)

        for hf in range(2):
            chunk(hf, up1(place[hf][0], FAR))
            for j in ORDER:
                first[hf][j].relay()
        for hf in range(2):
            chunk(hf, up1(place[hf][0], NEXT))
            chunk(hf, up1(place[hf][0], PREV))
            directs(hf, ORDER[0])
            directs(hf, ORDER[1])
        for hf in range(2):
            chunk(hf, place[hf][0])
        for t, j in enumerate(ORDER):
            for hf in range(2):
                first[hf][j].join()
                if t < 2:
                    directs(hf, ORDER[t + 2])
        between(0)
        for j in ORDER[:3]:
            for hf in range(2):
                s2_s[ps, hf, j] = first[hf][j].total().astype(BF)
                if j == FAR:
                    second[hf].relay()
                else:
                    second[hf].direct(j)
        for hf in range(2):
            second[hf].join()
        between(1)
        own_sum = [first[hf][ME].total() for hf in range(2)]
        return [own_sum[hf] + second[hf].received() for hf in range(2)]

    class Ring:
        def __init__(self, ps, hf, e, blk, fwd, bwd):
            self.blk, self.fwd, self.bwd, self.sem = blk, fwd, bwd, asem.at[hf, e]
            self.ssem = msem_s.at[ps, 1, 0 if e == TAIL else 1]

        def put(self, k, d, rows, device):
            r = self.blk(d, rows)
            send(r, r, self.ssem, self.sem.at[k], device)

        def start(self):
            self.put(0, ME, lo, self.fwd)
            self.put(1, ME, hi, self.bwd)
            self.put(2, ME, hi, self.fwd)
            self.put(3, ME, lo, self.bwd)

        def forward(self):
            arrived(self.blk(PREV, lo), self.sem.at[0])
            self.put(4, PREV, lo, self.fwd)
            arrived(self.blk(NEXT, hi), self.sem.at[1])
            self.put(5, NEXT, hi, self.bwd)

        def got(self, d):
            for k, rows in {PREV: ((2, hi),), NEXT: ((3, lo),), FAR: ((4, lo), (5, hi))}[d]:
                arrived(self.blk(d, rows), self.sem.at[k])

    def all_gather(ps, buf, consume, hook):
        inner, outer = [], []
        for hf in range(2):
            a, b, ap, am, bp, bm = place[hf]

            def block(ia, ib, rows, hf=hf):
                cols = pl.ds(hf * HALF, HALF)
                return buf.at[ia, ib, rows, cols] if hf == 0 else buf.at[ib, ia, rows, cols]

            inner.append(Ring(ps, hf, TAIL, lambda d, rows, a=a, b=b, block=block: block(a, up1(b, d), rows), bp, bm))
            outer.append([Ring(ps, hf, j, lambda d, rows, a=a, b=b, j=j, block=block: block(up1(a, d), up1(b, j), rows), ap, am)
                          for j in range(4)])
        for hf in range(2):
            inner[hf].start()
        for hf in range(2):
            outer[hf][ME].start()
        for hf in range(2):
            inner[hf].forward()
        for d in (PREV, NEXT):
            for hf in range(2):
                inner[hf].got(d)
                outer[hf][d].start()
        for hf in range(2):
            outer[hf][ME].forward()
        for hf in range(2):
            inner[hf].got(FAR)
            outer[hf][FAR].start()
        for d in (PREV, NEXT):
            for hf in range(2):
                outer[hf][d].forward()
        hook(0)
        for hf in range(2):
            consume(hf, place[hf][0])
        for hf in range(2):
            outer[hf][FAR].forward()
        for d in (PREV, NEXT, FAR):
            for hf in range(2):
                for r in outer[hf]:
                    r.got(d)
                consume(hf, up1(place[hf][0], d))
            if d == NEXT:
                hook(1)

    def out_chunk(hf, i):
        rows = (o_s[i] if hf == 0 else o_s[:, i]).reshape(128, 160)
        part = mm(rows, wof_s[:, hf * HALF:hf * HALF + HALF], NN)
        p_s[0, hf, i] = part.astype(BF).reshape(4, 32, HALF)

    def attn_between(step):
        if step == 1:
            g_u.forward()
            g_u.share()

    part = reduce_scatter(0, out_chunk, attn_between)
    mine = pl.ds(pl.multiple_of(tp * 32, 32), 32)
    for hf in range(2):
        cols = slice(hf * HALF, hf * HALF + HALF)
        h_s[:, cols] = x_s[mine, cols].astype(F32) + part[hf]
    resid = h_s[...]
    inv = lax.rsqrt(jnp.sum(resid * resid, axis=1, keepdims=True) * (1.0 / DM) + NORM_EPS)
    gain = jnp.concatenate([wg_s[i, 1] for i in range(8)], axis=1)
    g_s[z, y] = (resid * inv * gain).astype(BF)

    def mlp_hook(step):
        if step == 0:
            g_u.last()
            g_d.forward()
            g_u.siblings()
        else:
            g_d.share()
            g_d.last()

    def up_part(hf, i):
        w = wu_s[4 * hf:4 * hf + 4].reshape(HALF, FF)
        cols = slice(hf * HALF, hf * HALF + HALF)
        rows = (g_s[i, :, :, cols] if hf == 0 else g_s[:, i, :, cols]).reshape(128, HALF)
        prod = mm(rows, w, NN).reshape(4, 32, FF)
        if hf == 0:
            u_s[i] += prod
        else:
            u_s[:, i] += prod

    all_gather(0, g_s, up_part, mlp_hook)
    g_d.siblings()
    for i in range(4):
        hid_s[i] = jax.nn.gelu(u_s[i], approximate=True).astype(BF)

    def down_chunk(hf, i):
        rows = (hid_s[i] if hf == 0 else hid_s[:, i]).reshape(128, FF)
        w = wd_s[4 * hf:4 * hf + 4].reshape(HALF, FF)
        p_s[1, hf, i] = mm(rows, w, NT).astype(BF).reshape(4, 32, HALF)

    part = reduce_scatter(1, down_chunk, lambda step: None)
    y_v[z, y] = jnp.concatenate([h_s[:, 0:HALF] + part[0], h_s[:, HALF:DM] + part[1]], axis=1).astype(BF)
    all_gather(1, y_v, lambda hf, i: None, lambda step: None)
    for g in gathers:
        g.all_sent()
    for ps in range(2):
        for kind in range(2):
            sent(g_s.at[0, pl.ds(0, 3)], msem_s.at[ps, kind, 0], rsem.at[0, 0, 0])
            sent(g_s.at[pl.ds(0, 3)], msem_s.at[ps, kind, 1], rsem.at[0, 0, 0])


def solution(mesh):
    tok_axes = ("dp", "wg")
    in_specs = (P(tok_axes, None), P("wg"), P("wg"), P("wg", None, "tp", None), P("wg", "tp", None), P("tp", None, "wg"), P("wg", "tp"), P("tp", "wg"), P("tp", None), P("tp", None), P(None, None), P(tok_axes, "tp", None, None), P(tok_axes, "tp", None, None), P(tok_axes))
    out_specs = (P(tok_axes, None), P(tok_axes, "tp", None), P(tok_axes, "tp", None))

    def vm(shape, dtype=BF):
        return pltpu.VMEM(shape, dtype)

    def dma(*shape):
        return pltpu.SemaphoreType.DMA(shape)

    blocks = (2, 2, 5, 2)
    scratch = [
        vm((SEQ, DM)), vm((1, SEQ), jnp.int32), vm((2, HD), F32), vm((2, HD), F32), vm((CL, DM)), vm((HW, SLICE)),
        vm((8, 2, 1, SLICE), F32), vm((8, 3 * HW, SLICE)), vm((8, CL, HW), F32), vm((8, HW, SLICE)),
        vm((8, SLICE, FF)), vm((8, SLICE, FF)), vm((2, CL, HD, SEQ)), vm((2, CL, HD, SEQ)),
        vm((SEQ, 128), F32), vm((3 * HW, SEQ), F32), vm((HD, SEQ), F32), vm((CL, SEQ), F32),
        vm((HW, SEQ), F32), vm((4, 4, 32, HW)), vm((HW, DM)), vm((2, 2, 4, 4, 32, HALF)),
        vm(blocks + (16, HALF)), vm(blocks + (32, HALF)), vm(blocks + (16, HALF)), vm((2, 2, 4, 32, HALF)),
        vm((32, DM), F32), vm((4, 4, 32, DM)), vm((4, 4, 32, FF), F32), vm((4, 4, 32, FF)),
        dma(14), dma(6), dma(6, 10), dma(2, 2, 2), dma(2, 5, 6), dma(2, 5, 6),
    ]
    call = pl.pallas_call(
        layer_kernel,
        out_shape=(pltpu.VMEM((4, 4, 32, DM), BF), pltpu.VMEM((160, SEQ), BF), pltpu.VMEM((160, SEQ), BF)),
        in_specs=[pl.BlockSpec(memory_space=ANY)] * 14,
        out_specs=[pl.BlockSpec(memory_space=pltpu.VMEM)] * 3,
        scratch_shapes=scratch,
        compiler_params=pltpu.CompilerParams(collective_id=0, has_side_effects=True, vmem_limit_bytes=56 * 1024 * 1024),
        name="layer",
    )

    def device_step(tokens, gain_attn, gain_mlp, w_qkv, w_rel, w_out, w_up, w_down, bias_u, bias_v, rel_table, k_cache, v_cache, positions):
        out, k_new, v_new = call(
            tokens, positions.reshape(1, SEQ), bias_u, bias_v, gain_attn, gain_mlp,
            w_qkv.transpose(1, 2, 3, 0).reshape(480, 320), w_rel.transpose(1, 2, 0).reshape(160, 320),
            w_out.reshape(160, 320), w_up, w_down.T, rel_table,
            k_cache.transpose(1, 2, 3, 0), v_cache.transpose(1, 2, 3, 0))
        return (out.reshape(SEQ, DM), k_new.reshape(2, HD, SEQ).transpose(2, 0, 1), v_new.reshape(2, HD, SEQ).transpose(2, 0, 1))

    return jax.shard_map(device_step, mesh=mesh, in_specs=in_specs, out_specs=out_specs, check_vma=False)
```

```python
import jax
import jax.numpy as jnp
from jax import lax
from jax.experimental import pallas as pl
from jax.experimental.pallas import tpu as pltpu
from jax.sharding import PartitionSpec as P

NORM_EPS = 1e-6
BF = jnp.bfloat16
F32 = jnp.float32
MESH = pl.DeviceIdType.MESH
ANY = pl.ANY
SEQ, DM, HALF, HD, CL, FF = 512, 2560, 1280, 80, 32, 640
SLICE, HW = 320, 160
ME, NEXT, FAR, PREV, TAIL = range(5)
LO, HI, WHOLE = 0, 1, None
ORDER = (FAR, NEXT, PREV, ME)
NT = (((1,), (1,)), ((), ()))
NN = (((1,), (0,)), ((), ()))
TN = (((0,), (0,)), ((), ()))


def mm(a, b, dims):
    return lax.dot_general(a, b, dims, preferred_element_type=F32)


def layer_kernel(x_h, pos_h, bu_h, bv_h, ga_h, gm_h, wq_h, wr_h, wo_h, wu_h, wd_h, rt_h, k_h, v_h,
                 y_v, kn_s, vn_s,
                 x_s, pos_s, bu_s, bv_s, rt_s, wr_s, wqt_s, wot_s, wg_s, wq_s, qp_s, wo_s, wu_s, wd_s, k_s, v_s,
                 rs_s, acc, qu_s, sc_s, ot_s, o_s, wof_s, p_s, rel_s, rcv_s, stg_s, s2_s, t_s, h_s, g_s, u_s, hid_s,
                 lsem, gsem_s, gsem_r, msem_s, rsem, asem):
    tp, wg = lax.axis_index("tp"), lax.axis_index("wg")
    z, y = tp // 4, tp % 4
    x, c = wg // 2, wg % 2

    def up1(i, d):
        return lax.rem(i + d, 4)

    def dev(dz=0, dy=0, dx=0, flip=False):
        cc = 1 - c if flip else c
        return (0, up1(z, dz) * 4 + up1(y, dy), up1(x, dx) * 2 + cc)

    xp, xm, sib = dev(dx=1), dev(dx=3), dev(flip=True)
    zp, zm, yp, ym = dev(dz=1), dev(dz=3), dev(dy=1), dev(dy=3)
    xf, zf, yf = dev(dx=2), dev(dz=2), dev(dy=2)

    def send(src, dst, ssem, rsem, device):
        pltpu.make_async_remote_copy(src, dst, ssem, rsem, device_id=device, device_id_type=MESH).start()

    def sent(ref, ssem, rsem):
        pltpu.make_async_remote_copy(ref, ref, ssem, rsem, device_id=sib, device_id_type=MESH).wait_send()

    def arrived(dst, rsem):
        pltpu.make_async_remote_copy(dst, dst, gsem_s.at[0], rsem, device_id=sib, device_id_type=MESH).wait_recv()

    n_local = [0]

    def local(src, dst):
        cp = pltpu.make_async_copy(src, dst, lsem.at[n_local[0]])
        n_local[0] += 1
        cp.start()
        return cp

    barrier = pltpu.get_barrier_semaphore()
    peers = (xp, xm, xf, sib, zp, zm, zf, yp, ym, yf)
    for d in peers:
        pl.semaphore_signal(barrier, inc=1, device_id=d, device_id_type=MESH)

    own = 2 * x + c
    l_g = [local(ga_h, wg_s.at[own, 0, 0]), local(gm_h, wg_s.at[own, 1, 0])]
    l_q = local(wq_h, wqt_s)
    l_x = local(x_h, x_s)
    l_rt = local(rt_h, rt_s)
    l_pos = local(pos_h, pos_s)
    l_bu = local(bu_h, bu_s)
    l_bv = local(bv_h, bv_s)
    l_wr = local(wr_h, wr_s)
    l_wo = local(wo_h, wot_s)
    l_wu = local(wu_h, wu_s.at[own])
    l_wd = local(wd_h, wd_s.at[own])
    l_k = local(k_h, k_s)
    l_v = local(v_h, v_s)

    def slot(dx, flip=False):
        return 2 * up1(x, dx) + (1 - c if flip else c)

    class Gather:
        def __init__(self, ar, buf, rows, low):
            self.ar, self.buf, self.rows, self.low, self.relay = ar, buf, rows, low, True

        def ref(self, s, part):
            if part is WHOLE:
                return self.buf.at[s]
            return self.buf.at[s, pl.ds(0, self.low) if part == LO else pl.ds(self.low, self.rows - self.low)]

        def put(self, k, s, part, device):
            r = self.ref(s, part)
            send(r, r, gsem_s.at[self.ar], gsem_r.at[self.ar, k], device)

        def got(self, k, s, part):
            arrived(self.ref(s, part), gsem_r.at[self.ar, k])

        def start(self):
            o = slot(ME)
            if not self.relay:
                self.put(4, o, LO, xf)
                self.put(5, o, HI, xf)
            self.put(0, o, LO, xp)
            self.put(1, o, HI, xm)
            self.put(2, o, HI, xp)
            self.put(3, o, LO, xm)
            self.put(6, o, WHOLE, sib)

        def forward(self):
            self.got(0, slot(PREV), LO)
            if self.relay:
                self.put(4, slot(PREV), LO, xp)
            self.got(1, slot(NEXT), HI)
            if self.relay:
                self.put(5, slot(NEXT), HI, xm)

        def share(self):
            self.got(2, slot(PREV), HI)
            self.put(7, slot(PREV), WHOLE, sib)
            self.got(3, slot(NEXT), LO)
            self.put(8, slot(NEXT), WHOLE, sib)

        def last(self):
            self.got(4, slot(FAR), LO)
            self.got(5, slot(FAR), HI)
            self.put(9, slot(FAR), WHOLE, sib)

        def sibling(self, dx):
            self.got({ME: 6, PREV: 7, NEXT: 8, FAR: 9}[dx], slot(dx, True), WHOLE)

        def siblings(self):
            for dx in (ME, PREV, NEXT, FAR):
                self.sibling(dx)

        def all_sent(self):
            sent(self.buf.at[pl.ds(0, 7)], gsem_s.at[self.ar], gsem_r.at[self.ar, 0])

    g_g, g_q, g_o, g_u, g_d, g_r = gathers = [Gather(i, *spec) for i, spec in enumerate((
        (wg_s, 2, 1), (wq_s, 240, 128), (wo_s, 80, 48), (wu_s, SLICE, HW), (wd_s, SLICE, HW), (qp_s, CL, 16)))]
    g_o.relay = False

    l_q.wait()
    wq_s[own] = jnp.concatenate([wqt_s[0:240, :], wqt_s[240:480, :]], axis=1)
    l_wo.wait()
    wo_s[own] = jnp.concatenate([wot_s[0:80, :], wot_s[80:160, :]], axis=1)
    l_x.wait()

    def stat_rows(r, carry):
        rows = pl.ds(pl.multiple_of(r * 32, 32), 32)
        v = x_s[rows, :].astype(F32)
        ms = jnp.sum(v * v, axis=1, keepdims=True) * (1.0 / DM)
        rs_s[rows, :] = jnp.broadcast_to(lax.rsqrt(ms + NORM_EPS), (32, 128))
        return carry

    lax.fori_loop(0, 16, stat_rows, 0)
    l_rt.wait()
    l_wr.wait()
    base = pl.multiple_of(640 * x, 128)
    q_even = mm(rt_s[:, pl.ds(base, 384)][:, 0:320], wr_s[...], NT)
    q_odd = mm(rt_s[:, pl.ds(pl.multiple_of(base + 256, 128), 384)][:, 64:384], wr_s[...], NT)
    qp_s[own] = jnp.where(c == 1, q_odd, q_even)
    for cp in l_g:
        cp.wait()
    pl.semaphore_wait(barrier, len(peers))
    g_g.start()
    g_q.start()
    g_r.start()
    acc[...] = jnp.zeros_like(acc)
    u_s[...] = jnp.zeros_like(u_s)

    def unpack(even, odd):
        halves = [jnp.concatenate([even[:, cut], odd[:, cut]], axis=1) for cut in (slice(0, SLICE), slice(SLICE, FF))]
        return jnp.concatenate(halves, axis=0)

    def qkv_pair(dx):
        xo = up1(x, dx)
        cols = pl.ds(pl.multiple_of(xo * 640, 128), 640)
        gain = jnp.concatenate([wg_s[2 * xo, 0], wg_s[2 * xo + 1, 0]], axis=1)
        n_win = (x_s[:, cols].astype(F32) * rs_s[:, 0:1] * gain).astype(BF)
        acc[...] += mm(unpack(wq_s[2 * xo], wq_s[2 * xo + 1]), n_win, NT)

    g_g.sibling(ME)
    g_q.sibling(ME)
    qkv_pair(ME)
    g_g.forward()
    g_q.forward()
    g_g.share()
    g_q.share()
    g_r.forward()
    g_r.share()
    g_o.start()
    g_g.last()
    for dx in (PREV, NEXT, FAR):
        g_g.sibling(dx)
        g_q.sibling(dx)
        qkv_pair(dx)
        if dx == PREV:
            g_q.last()
            g_r.last()

    kn_s[...] = acc[160:320, :].astype(BF)
    vn_s[...] = acc[320:480, :].astype(BF)
    l_pos.wait()
    l_bu.wait()
    l_bv.wait()
    g_r.siblings()
    g_o.forward()
    g_o.share()
    l_wu.wait()
    g_u.start()
    l_wd.wait()
    g_d.start()

    flip_rows = (lax.broadcasted_iota(jnp.int32, (CL, CL), 0) + lax.broadcasted_iota(jnp.int32, (CL, CL), 1)) % CL == 0
    flip_mat = jnp.where(flip_rows, 1.0, 0.0).astype(BF)
    q_rel = qp_s[0]
    for i in range(1, 8):
        q_rel = q_rel + qp_s[i]
    rel_rev = mm(flip_mat, q_rel.astype(BF), NN).astype(BF)
    diag = lax.broadcasted_iota(jnp.int32, (HD, HD), 0) == lax.broadcasted_iota(jnp.int32, (HD, HD), 1)

    def column(row):
        return jnp.sum(jnp.where(diag, row, 0.0), axis=1, keepdims=True)

    pos = pos_s[...]
    steps = lax.broadcasted_iota(jnp.int32, (CL, SEQ), 0)
    is_self = steps == pos
    l_k.wait()
    l_v.wait()

    for h in range(2):
        hr = slice(h * HD, h * HD + HD)
        q = acc[hr, :].astype(BF).astype(F32)
        q_u = (q + column(bu_s[h:h + 1, :])).astype(BF).astype(F32)
        q_v = (q + column(bv_s[h:h + 1, :])).astype(BF)
        qu_s[...] = q_u
        rel = mm(rel_rev[:, hr], q_v, NN)
        for b in range(5):
            rel = jnp.where((pos >> b) & 1 == 1, pltpu.roll(rel, 1 << b, 0), rel)
        self_score = jnp.sum(q_u * kn_s[hr, :].astype(F32), axis=0, keepdims=True)
        for lc in range(4):
            ln = slice(lc * 128, lc * 128 + 128)
            quc = qu_s[:, ln]

            def content(g, carry, h=h, ln=ln, quc=quc):
                rows = [jnp.sum(k_s[h, g * 8 + j, :, ln].astype(F32) * quc, axis=0, keepdims=True) for j in range(8)]
                sc_s[pl.ds(pl.multiple_of(g * 8, 8), 8), ln] = jnp.concatenate(rows, axis=0)
                return carry

            lax.fori_loop(0, CL // 8, content, 0)
        if h == 1:
            g_o.last()
        scores = jnp.where(is_self, self_score, sc_s[...])
        scores = jnp.where(steps <= pos, (scores + rel) * (HD ** -0.5), -1e30)
        e = jnp.exp(scores - jnp.max(scores, axis=0, keepdims=True))
        prob = (e / jnp.sum(e, axis=0, keepdims=True)).astype(BF).astype(F32)
        self_prob = jnp.sum(jnp.where(is_self, prob, 0.0), axis=0, keepdims=True)
        sc_s[...] = jnp.where(is_self, 0.0, prob)
        for lc in range(4):
            ln = slice(lc * 128, lc * 128 + 128)

            def mix(g, o, h=h, ln=ln):
                pr = sc_s[pl.ds(pl.multiple_of(g * 8, 8), 8), ln]
                for j in range(8):
                    o = o + pr[j:j + 1, :] * v_s[h, g * 8 + j, :, ln].astype(F32)
                return o

            start = self_prob[:, ln] * vn_s[hr, ln].astype(F32)
            ot_s[hr, ln] = lax.fori_loop(0, CL // 8, mix, start)

    o_s[...] = jnp.transpose(ot_s[...]).astype(BF).reshape(4, 4, 32, 160)
    g_o.siblings()
    for xo in range(4):
        wof_s[:, 640 * xo:640 * xo + 640] = unpack(wo_s[2 * xo], wo_s[2 * xo + 1])

    place = ((z, y, zp, zm, yp, ym, yf), (y, z, yp, ym, zp, zm, zf))

    lo, hi = pl.ds(0, 16), pl.ds(16, 16)

    class Exchange:
        def __init__(self, ps, hf, e, src, fwd, bwd):
            self.src, self.fwd, self.bwd, self.sem = src, fwd, bwd, rsem.at[hf, e]
            self.ssem = msem_s.at[ps, 0, 1]
            self.rel, self.rcv, self.stg = rel_s.at[ps, hf, e], rcv_s.at[ps, hf, e], stg_s.at[ps, hf, e]

        def relay(self):
            send(self.src(FAR).at[lo], self.rel.at[LO], self.ssem, self.sem.at[0], self.fwd)
            send(self.src(FAR).at[hi], self.rel.at[HI], self.ssem, self.sem.at[1], self.bwd)

        def direct(self, d):
            if d == NEXT:
                send(self.src(NEXT).at[hi], self.rcv.at[0, hi], self.ssem, self.sem.at[2], self.fwd)
            else:
                send(self.src(PREV).at[lo], self.rcv.at[1, lo], self.ssem, self.sem.at[3], self.bwd)

        def join(self):
            for part, rows, d, device in ((LO, lo, NEXT, self.fwd), (HI, hi, PREV, self.bwd)):
                arrived(self.rel.at[part], self.sem.at[part])
                both = self.src(d).at[rows][...].astype(F32) + self.rel.at[part][...].astype(F32)
                self.stg.at[part][...] = both.astype(BF)
                send(self.stg.at[part], self.rcv.at[part, rows], self.ssem, self.sem.at[4 + part], device)

        def received(self):
            for k, way, rows in ((2, 0, hi), (3, 1, lo), (4, 0, lo), (5, 1, hi)):
                arrived(self.rcv.at[way, rows], self.sem.at[k])
            return self.rcv.at[0][...].astype(F32) + self.rcv.at[1][...].astype(F32)

        def total(self):
            return self.received() + self.src(ME)[...].astype(F32)

    class Spread:
        def __init__(self, ps, hf, devices):
            self.src, self.rcv, self.devices = s2_s.at[ps, hf], t_s.at[ps, hf], devices
            self.sem, self.ssem = rsem.at[hf, TAIL], msem_s.at[ps, 0, 0]

        def put(self, j):
            send(self.src.at[j], self.rcv.at[j], self.ssem, self.sem.at[j], self.devices[j])

        def received(self):
            for j in ORDER[:3]:
                arrived(self.rcv.at[j], self.sem.at[j])
            return sum(self.rcv.at[j][...].astype(F32) for j in ORDER[:3])

    def reduce_scatter(ps, chunk, between):
        first, second = [], []
        for hf in range(2):
            a, b, ap, am, bp, bm, bf = place[hf]
            first.append([Exchange(ps, hf, j, lambda d, hf=hf, a=a, b=b, j=j: p_s.at[ps, hf, up1(a, d), up1(b, j)], ap, am)
                          for j in range(4)])
            second.append(Spread(ps, hf, {NEXT: bp, FAR: bf, PREV: bm}))

        def directs(hf, j):
            first[hf][j].direct(NEXT)
            first[hf][j].direct(PREV)

        for hf in range(2):
            chunk(hf, up1(place[hf][0], FAR))
            for j in ORDER:
                first[hf][j].relay()
        for hf in range(2):
            chunk(hf, up1(place[hf][0], NEXT))
            chunk(hf, up1(place[hf][0], PREV))
            directs(hf, ORDER[0])
            directs(hf, ORDER[1])
        for hf in range(2):
            chunk(hf, place[hf][0])
        for t, j in enumerate(ORDER):
            for hf in range(2):
                first[hf][j].join()
                if t < 2:
                    directs(hf, ORDER[t + 2])
        between(0)
        for j in ORDER[:3]:
            for hf in range(2):
                s2_s[ps, hf, j] = first[hf][j].total().astype(BF)
                second[hf].put(j)
        between(1)
        own_sum = [first[hf][ME].total() for hf in range(2)]
        return [own_sum[hf] + second[hf].received() for hf in range(2)]

    class Ring:
        def __init__(self, ps, hf, e, blk, fwd, bwd):
            self.blk, self.fwd, self.bwd, self.sem = blk, fwd, bwd, asem.at[hf, e]
            self.ssem = msem_s.at[ps, 1, 0 if e == TAIL else 1]

        def put(self, k, d, rows, device):
            r = self.blk(d, rows)
            send(r, r, self.ssem, self.sem.at[k], device)

        def start(self):
            self.put(0, ME, lo, self.fwd)
            self.put(1, ME, hi, self.bwd)
            self.put(2, ME, hi, self.fwd)
            self.put(3, ME, lo, self.bwd)

        def forward(self):
            arrived(self.blk(PREV, lo), self.sem.at[0])
            self.put(4, PREV, lo, self.fwd)
            arrived(self.blk(NEXT, hi), self.sem.at[1])
            self.put(5, NEXT, hi, self.bwd)

        def got(self, d):
            for k, rows in {PREV: ((2, hi),), NEXT: ((3, lo),), FAR: ((4, lo), (5, hi))}[d]:
                arrived(self.blk(d, rows), self.sem.at[k])

    def all_gather(ps, buf, consume, hook):
        inner, outer = [], []
        for hf in range(2):
            a, b, ap, am, bp, bm, _ = place[hf]

            def block(ia, ib, rows, hf=hf):
                cols = pl.ds(hf * HALF, HALF)
                return buf.at[ia, ib, rows, cols] if hf == 0 else buf.at[ib, ia, rows, cols]

            inner.append(Ring(ps, hf, TAIL, lambda d, rows, a=a, b=b, block=block: block(a, up1(b, d), rows), bp, bm))
            outer.append([Ring(ps, hf, j, lambda d, rows, a=a, b=b, j=j, block=block: block(up1(a, d), up1(b, j), rows), ap, am)
                          for j in range(4)])
        for hf in range(2):
            inner[hf].start()
        for hf in range(2):
            outer[hf][ME].start()
        for hf in range(2):
            inner[hf].forward()
        for d in (PREV, NEXT):
            for hf in range(2):
                inner[hf].got(d)
                outer[hf][d].start()
        for hf in range(2):
            outer[hf][ME].forward()
        for hf in range(2):
            inner[hf].got(FAR)
            outer[hf][FAR].start()
        for d in (PREV, NEXT):
            for hf in range(2):
                outer[hf][d].forward()
        hook(0)
        for hf in range(2):
            consume(hf, place[hf][0])
        for hf in range(2):
            outer[hf][FAR].forward()
        for d in (PREV, NEXT, FAR):
            for hf in range(2):
                for r in outer[hf]:
                    r.got(d)
                consume(hf, up1(place[hf][0], d))
            if d == NEXT:
                hook(1)

    def out_chunk(hf, i):
        rows = (o_s[i] if hf == 0 else o_s[:, i]).reshape(128, 160)
        part = mm(rows, wof_s[:, hf * HALF:hf * HALF + HALF], NN)
        p_s[0, hf, i] = part.astype(BF).reshape(4, 32, HALF)

    def attn_between(step):
        if step == 1:
            g_u.forward()
            g_u.share()

    part = reduce_scatter(0, out_chunk, attn_between)
    mine = pl.ds(pl.multiple_of(tp * 32, 32), 32)
    for hf in range(2):
        cols = slice(hf * HALF, hf * HALF + HALF)
        h_s[:, cols] = x_s[mine, cols].astype(F32) + part[hf]
    resid = h_s[...]
    inv = lax.rsqrt(jnp.sum(resid * resid, axis=1, keepdims=True) * (1.0 / DM) + NORM_EPS)
    gain = jnp.concatenate([wg_s[i, 1] for i in range(8)], axis=1)
    g_s[z, y] = (resid * inv * gain).astype(BF)

    def mlp_hook(step):
        if step == 0:
            g_u.last()
            g_d.forward()
            g_u.siblings()
        else:
            g_d.share()
            g_d.last()

    def up_part(hf, i):
        w = wu_s[4 * hf:4 * hf + 4].reshape(HALF, FF)
        cols = slice(hf * HALF, hf * HALF + HALF)
        rows = (g_s[i, :, :, cols] if hf == 0 else g_s[:, i, :, cols]).reshape(128, HALF)
        prod = mm(rows, w, NN).reshape(4, 32, FF)
        if hf == 0:
            u_s[i] += prod
        else:
            u_s[:, i] += prod

    all_gather(0, g_s, up_part, mlp_hook)
    g_d.siblings()
    def down_chunk(hf, i):
        rows = (hid_s[i] if hf == 0 else hid_s[:, i]).reshape(128, FF)
        w = wd_s[4 * hf:4 * hf + 4].reshape(HALF, FF)
        p_s[1, hf, i] = mm(rows, w, NT).astype(BF).reshape(4, 32, HALF)

    for d in ORDER:
        i = up1(z, d)
        hid_s[i] = jax.nn.gelu(u_s[i], approximate=True).astype(BF)
    part = reduce_scatter(1, down_chunk, lambda step: None)
    y_v[z, y] = jnp.concatenate([h_s[:, 0:HALF] + part[0], h_s[:, HALF:DM] + part[1]], axis=1).astype(BF)
    all_gather(1, y_v, lambda hf, i: None, lambda step: None)
    for g in gathers:
        g.all_sent()
    for ps in range(2):
        for kind in range(2):
            sent(g_s.at[0, pl.ds(0, 3)], msem_s.at[ps, kind, 0], rsem.at[0, 0, 0])
            sent(g_s.at[pl.ds(0, 3)], msem_s.at[ps, kind, 1], rsem.at[0, 0, 0])


def solution(mesh):
    tok_axes = ("dp", "wg")
    in_specs = (P(tok_axes, None), P("wg"), P("wg"), P("wg", None, "tp", None), P("wg", "tp", None), P("tp", None, "wg"), P("wg", "tp"), P("tp", "wg"), P("tp", None), P("tp", None), P(None, None), P(tok_axes, "tp", None, None), P(tok_axes, "tp", None, None), P(tok_axes))
    out_specs = (P(tok_axes, None), P(tok_axes, "tp", None), P(tok_axes, "tp", None))

    def vm(shape, dtype=BF):
        return pltpu.VMEM(shape, dtype)

    def dma(*shape):
        return pltpu.SemaphoreType.DMA(shape)

    blocks = (2, 2, 4, 2)
    scratch = [
        vm((SEQ, DM)), vm((1, SEQ), jnp.int32), vm((2, HD), F32), vm((2, HD), F32), vm((CL, DM)), vm((HW, SLICE)),
        vm((3 * HW, SLICE)), vm((HW, SLICE)), vm((8, 2, 1, SLICE), F32), vm((8, 240, FF)), vm((8, CL, HW), F32), vm((8, 80, FF)),
        vm((8, SLICE, FF)), vm((8, SLICE, FF)), vm((2, CL, HD, SEQ)), vm((2, CL, HD, SEQ)),
        vm((SEQ, 128), F32), vm((3 * HW, SEQ), F32), vm((HD, SEQ), F32), vm((CL, SEQ), F32),
        vm((HW, SEQ), F32), vm((4, 4, 32, HW)), vm((HW, DM)), vm((2, 2, 4, 4, 32, HALF)),
        vm(blocks + (16, HALF)), vm(blocks + (32, HALF)), vm(blocks + (16, HALF)), vm((2, 2, 4, 32, HALF)), vm((2, 2, 4, 32, HALF)),
        vm((32, DM), F32), vm((4, 4, 32, DM)), vm((4, 4, 32, FF), F32), vm((4, 4, 32, FF)),
        dma(14), dma(6), dma(6, 10), dma(2, 2, 2), dma(2, 5, 6), dma(2, 5, 6),
    ]
    call = pl.pallas_call(
        layer_kernel,
        out_shape=(pltpu.VMEM((4, 4, 32, DM), BF), pltpu.VMEM((160, SEQ), BF), pltpu.VMEM((160, SEQ), BF)),
        in_specs=[pl.BlockSpec(memory_space=ANY)] * 14,
        out_specs=[pl.BlockSpec(memory_space=pltpu.VMEM)] * 3,
        scratch_shapes=scratch,
        compiler_params=pltpu.CompilerParams(collective_id=0, has_side_effects=True, vmem_limit_bytes=56 * 1024 * 1024),
        name="layer",
    )

    def device_step(tokens, gain_attn, gain_mlp, w_qkv, w_rel, w_out, w_up, w_down, bias_u, bias_v, rel_table, k_cache, v_cache, positions):
        out, k_new, v_new = call(
            tokens, positions.reshape(1, SEQ), bias_u, bias_v, gain_attn, gain_mlp,
            w_qkv.transpose(1, 2, 3, 0).reshape(480, 320), w_rel.transpose(1, 2, 0).reshape(160, 320),
            w_out.reshape(160, 320), w_up, w_down.T, rel_table,
            k_cache.transpose(1, 2, 3, 0), v_cache.transpose(1, 2, 3, 0))
        return (out.reshape(SEQ, DM), k_new.reshape(2, HD, SEQ).transpose(2, 0, 1), v_new.reshape(2, HD, SEQ).transpose(2, 0, 1))

    return jax.shard_map(device_step, mesh=mesh, in_specs=in_specs, out_specs=out_specs, check_vma=False)
```

```python
import jax
import jax.numpy as jnp
from jax import lax
from jax.experimental import pallas as pl
from jax.experimental.pallas import tpu as pltpu
from jax.sharding import PartitionSpec as P

NORM_EPS = 1e-6
BF = jnp.bfloat16
F32 = jnp.float32
MESH = pl.DeviceIdType.MESH
ANY = pl.ANY
SEQ, DM, HALF, HD, CL, FF = 512, 2560, 1280, 80, 32, 640
SLICE, HW = 320, 160
ME, NEXT, FAR, PREV, TAIL = range(5)
LO, HI, WHOLE = 0, 1, None
ORDER = (FAR, NEXT, PREV, ME)
NT = (((1,), (1,)), ((), ()))
NN = (((1,), (0,)), ((), ()))
TN = (((0,), (0,)), ((), ()))


def mm(a, b, dims):
    return lax.dot_general(a, b, dims, preferred_element_type=F32)


def layer_kernel(x_h, pos_h, bu_h, bv_h, ga_h, gm_h, wq_h, wr_h, wo_h, wu_h, wd_h, rt_h, k_h, v_h,
                 y_v, kn_s, vn_s,
                 x_s, pos_s, bu_s, bv_s, rt_s, wr_s, wqt_s, wot_s, wg_s, wq_s, qp_s, wo_s, wu_s, wd_s, k_s, v_s,
                 rs_s, acc, qu_s, sc_s, ot_s, o_s, wof_s, p_s, rel_s, rcv_s, stg_s, s2_s, t_s, h_s, g_s, u_s, hid_s, n_s,
                 lsem, gsem_s, gsem_r, msem_s, rsem, asem):
    tp, wg = lax.axis_index("tp"), lax.axis_index("wg")
    z, y = tp // 4, tp % 4
    x, c = wg // 2, wg % 2

    def up1(i, d):
        return lax.rem(i + d, 4)

    def dev(dz=0, dy=0, dx=0, flip=False):
        cc = 1 - c if flip else c
        return (0, up1(z, dz) * 4 + up1(y, dy), up1(x, dx) * 2 + cc)

    xp, xm, sib = dev(dx=1), dev(dx=3), dev(flip=True)
    zp, zm, yp, ym = dev(dz=1), dev(dz=3), dev(dy=1), dev(dy=3)
    xf, zf, yf = dev(dx=2), dev(dz=2), dev(dy=2)

    def send(src, dst, ssem, rsem, device):
        pltpu.make_async_remote_copy(src, dst, ssem, rsem, device_id=device, device_id_type=MESH).start()

    def sent(ref, ssem, rsem):
        pltpu.make_async_remote_copy(ref, ref, ssem, rsem, device_id=sib, device_id_type=MESH).wait_send()

    def arrived(dst, rsem):
        pltpu.make_async_remote_copy(dst, dst, gsem_s.at[0], rsem, device_id=sib, device_id_type=MESH).wait_recv()

    n_local = [0]

    def local(src, dst):
        cp = pltpu.make_async_copy(src, dst, lsem.at[n_local[0]])
        n_local[0] += 1
        cp.start()
        return cp

    barrier = pltpu.get_barrier_semaphore()
    peers = (xp, xm, xf, sib, zp, zm, zf, yp, ym, yf)
    for d in peers:
        pl.semaphore_signal(barrier, inc=1, device_id=d, device_id_type=MESH)

    own = 2 * x + c
    l_g = [local(ga_h, wg_s.at[own, 0, 0]), local(gm_h, wg_s.at[own, 1, 0])]
    l_q = local(wq_h, wqt_s)
    l_x = local(x_h, x_s)
    l_rt = local(rt_h, rt_s)
    l_pos = local(pos_h, pos_s)
    l_bu = local(bu_h, bu_s)
    l_bv = local(bv_h, bv_s)
    l_wr = local(wr_h, wr_s)
    l_wo = local(wo_h, wot_s)
    l_wu = local(wu_h, wu_s.at[own])
    l_wd = local(wd_h, wd_s.at[own])
    l_k = local(k_h, k_s)
    l_v = local(v_h, v_s)

    def slot(dx, flip=False):
        return 2 * up1(x, dx) + (1 - c if flip else c)

    class Gather:
        def __init__(self, ar, buf, rows, low):
            self.ar, self.buf, self.rows, self.low, self.relay = ar, buf, rows, low, True

        def ref(self, s, part):
            if part is WHOLE:
                return self.buf.at[s]
            return self.buf.at[s, pl.ds(0, self.low) if part == LO else pl.ds(self.low, self.rows - self.low)]

        def put(self, k, s, part, device):
            r = self.ref(s, part)
            send(r, r, gsem_s.at[self.ar], gsem_r.at[self.ar, k], device)

        def got(self, k, s, part):
            arrived(self.ref(s, part), gsem_r.at[self.ar, k])

        def start(self):
            o = slot(ME)
            if not self.relay:
                self.put(4, o, LO, xf)
                self.put(5, o, HI, xf)
            self.put(0, o, LO, xp)
            self.put(1, o, HI, xm)
            self.put(2, o, HI, xp)
            self.put(3, o, LO, xm)
            self.put(6, o, WHOLE, sib)

        def forward(self):
            self.got(0, slot(PREV), LO)
            if self.relay:
                self.put(4, slot(PREV), LO, xp)
            self.got(1, slot(NEXT), HI)
            if self.relay:
                self.put(5, slot(NEXT), HI, xm)

        def share(self):
            self.got(2, slot(PREV), HI)
            self.put(7, slot(PREV), WHOLE, sib)
            self.got(3, slot(NEXT), LO)
            self.put(8, slot(NEXT), WHOLE, sib)

        def last(self):
            self.got(4, slot(FAR), LO)
            self.got(5, slot(FAR), HI)
            self.put(9, slot(FAR), WHOLE, sib)

        def sibling(self, dx):
            self.got({ME: 6, PREV: 7, NEXT: 8, FAR: 9}[dx], slot(dx, True), WHOLE)

        def siblings(self):
            for dx in (ME, PREV, NEXT, FAR):
                self.sibling(dx)

        def all_sent(self):
            sent(self.buf.at[pl.ds(0, 7)], gsem_s.at[self.ar], gsem_r.at[self.ar, 0])

    g_g, g_q, g_o, g_u, g_d, g_r = gathers = [Gather(i, *spec) for i, spec in enumerate((
        (wg_s, 2, 1), (wq_s, 240, 128), (wo_s, 80, 48), (wu_s, SLICE, HW), (wd_s, SLICE, HW), (qp_s, CL, 16)))]
    g_o.relay = False

    l_q.wait()
    wq_s[own] = jnp.concatenate([wqt_s[0:240, :], wqt_s[240:480, :]], axis=1)
    l_wo.wait()
    wo_s[own] = jnp.concatenate([wot_s[0:80, :], wot_s[80:160, :]], axis=1)
    l_x.wait()

    def stat_rows(r, carry):
        rows = pl.ds(pl.multiple_of(r * 32, 32), 32)
        v = x_s[rows, :].astype(F32)
        ms = jnp.sum(v * v, axis=1, keepdims=True) * (1.0 / DM)
        rs_s[rows, :] = jnp.broadcast_to(lax.rsqrt(ms + NORM_EPS), (32, 128))
        return carry

    lax.fori_loop(0, 16, stat_rows, 0)
    l_rt.wait()
    l_wr.wait()
    base = pl.multiple_of(640 * x, 128)
    q_even = mm(rt_s[:, pl.ds(base, 384)][:, 0:320], wr_s[...], NT)
    q_odd = mm(rt_s[:, pl.ds(pl.multiple_of(base + 256, 128), 384)][:, 64:384], wr_s[...], NT)
    qp_s[own] = jnp.where(c == 1, q_odd, q_even)
    for cp in l_g:
        cp.wait()
    pl.semaphore_wait(barrier, len(peers))
    g_g.start()
    g_q.start()
    g_r.start()
    acc[...] = jnp.zeros_like(acc)
    u_s[...] = jnp.zeros_like(u_s)

    def unpack(even, odd):
        halves = [jnp.concatenate([even[:, cut], odd[:, cut]], axis=1) for cut in (slice(0, SLICE), slice(SLICE, FF))]
        return jnp.concatenate(halves, axis=0)

    def qkv_pair(dx):
        xo = up1(x, dx)
        cols = pl.ds(pl.multiple_of(xo * 640, 128), 640)
        g_g.sibling(dx)
        gain = jnp.concatenate([wg_s[2 * xo, 0], wg_s[2 * xo + 1, 0]], axis=1)
        n_s[...] = (x_s[:, cols].astype(F32) * rs_s[:, 0:1] * gain).astype(BF)
        g_q.sibling(dx)
        acc[...] += mm(unpack(wq_s[2 * xo], wq_s[2 * xo + 1]), n_s[...], NT)

    qkv_pair(ME)
    g_g.forward()
    g_q.forward()
    g_g.share()
    g_q.share()
    g_r.forward()
    g_r.share()
    g_o.start()
    g_g.last()
    for dx in (PREV, NEXT, FAR):
        qkv_pair(dx)
        if dx == PREV:
            g_q.last()
            g_r.last()

    kn_s[...] = acc[160:320, :].astype(BF)
    vn_s[...] = acc[320:480, :].astype(BF)
    l_pos.wait()
    l_bu.wait()
    l_bv.wait()
    g_r.siblings()
    g_o.forward()
    g_o.share()
    l_wu.wait()
    g_u.start()
    l_wd.wait()
    g_d.start()

    flip_rows = (lax.broadcasted_iota(jnp.int32, (CL, CL), 0) + lax.broadcasted_iota(jnp.int32, (CL, CL), 1)) % CL == 0
    flip_mat = jnp.where(flip_rows, 1.0, 0.0).astype(BF)
    q_rel = qp_s[0]
    for i in range(1, 8):
        q_rel = q_rel + qp_s[i]
    rel_rev = mm(flip_mat, q_rel.astype(BF), NN).astype(BF)
    diag = lax.broadcasted_iota(jnp.int32, (HD, HD), 0) == lax.broadcasted_iota(jnp.int32, (HD, HD), 1)

    def column(row):
        return jnp.sum(jnp.where(diag, row, 0.0), axis=1, keepdims=True)

    pos = pos_s[...]
    steps = lax.broadcasted_iota(jnp.int32, (CL, SEQ), 0)
    is_self = steps == pos
    l_k.wait()
    l_v.wait()

    for h in range(2):
        hr = slice(h * HD, h * HD + HD)
        q = acc[hr, :].astype(BF).astype(F32)
        q_u = (q + column(bu_s[h:h + 1, :])).astype(BF).astype(F32)
        q_v = (q + column(bv_s[h:h + 1, :])).astype(BF)
        qu_s[...] = q_u
        rel = mm(rel_rev[:, hr], q_v, NN)
        for b in range(5):
            rel = jnp.where((pos >> b) & 1 == 1, pltpu.roll(rel, 1 << b, 0), rel)
        self_score = jnp.sum(q_u * kn_s[hr, :].astype(F32), axis=0, keepdims=True)
        for lc in range(4):
            ln = slice(lc * 128, lc * 128 + 128)
            quc = qu_s[:, ln]

            def content(g, carry, h=h, ln=ln, quc=quc):
                rows = [jnp.sum(k_s[h, g * 8 + j, :, ln].astype(F32) * quc, axis=0, keepdims=True) for j in range(8)]
                sc_s[pl.ds(pl.multiple_of(g * 8, 8), 8), ln] = jnp.concatenate(rows, axis=0)
                return carry

            lax.fori_loop(0, CL // 8, content, 0)
        if h == 1:
            g_o.last()
        scores = jnp.where(is_self, self_score, sc_s[...])
        scores = jnp.where(steps <= pos, (scores + rel) * (HD ** -0.5), -1e30)
        e = jnp.exp(scores - jnp.max(scores, axis=0, keepdims=True))
        prob = (e / jnp.sum(e, axis=0, keepdims=True)).astype(BF).astype(F32)
        self_prob = jnp.sum(jnp.where(is_self, prob, 0.0), axis=0, keepdims=True)
        sc_s[...] = jnp.where(is_self, 0.0, prob)
        for lc in range(4):
            ln = slice(lc * 128, lc * 128 + 128)

            def mix(g, o, h=h, ln=ln):
                pr = sc_s[pl.ds(pl.multiple_of(g * 8, 8), 8), ln]
                for j in range(8):
                    o = o + pr[j:j + 1, :] * v_s[h, g * 8 + j, :, ln].astype(F32)
                return o

            start = self_prob[:, ln] * vn_s[hr, ln].astype(F32)
            ot_s[hr, ln] = lax.fori_loop(0, CL // 8, mix, start)

    o_s[...] = jnp.transpose(ot_s[...]).astype(BF).reshape(4, 4, 32, 160)
    g_o.siblings()
    for xo in range(4):
        wof_s[:, 640 * xo:640 * xo + 640] = unpack(wo_s[2 * xo], wo_s[2 * xo + 1])

    place = ((z, y, zp, zm, yp, ym, yf), (y, z, yp, ym, zp, zm, zf))

    lo, hi = pl.ds(0, 16), pl.ds(16, 16)

    class Exchange:
        def __init__(self, ps, hf, e, src, fwd, bwd):
            self.src, self.fwd, self.bwd, self.sem = src, fwd, bwd, rsem.at[hf, e]
            self.ssem = msem_s.at[ps, 0, 1]
            self.rel, self.rcv, self.stg = rel_s.at[ps, hf, e], rcv_s.at[ps, hf, e], stg_s.at[ps, hf, e]

        def relay(self):
            send(self.src(FAR).at[lo], self.rel.at[LO], self.ssem, self.sem.at[0], self.fwd)
            send(self.src(FAR).at[hi], self.rel.at[HI], self.ssem, self.sem.at[1], self.bwd)

        def direct(self, d):
            if d == NEXT:
                send(self.src(NEXT).at[hi], self.rcv.at[0, hi], self.ssem, self.sem.at[2], self.fwd)
            else:
                send(self.src(PREV).at[lo], self.rcv.at[1, lo], self.ssem, self.sem.at[3], self.bwd)

        def join(self):
            for part, rows, d, device in ((LO, lo, NEXT, self.fwd), (HI, hi, PREV, self.bwd)):
                arrived(self.rel.at[part], self.sem.at[part])
                both = self.src(d).at[rows][...].astype(F32) + self.rel.at[part][...].astype(F32)
                self.stg.at[part][...] = both.astype(BF)
                send(self.stg.at[part], self.rcv.at[part, rows], self.ssem, self.sem.at[4 + part], device)

        def received(self):
            for k, way, rows in ((2, 0, hi), (3, 1, lo), (4, 0, lo), (5, 1, hi)):
                arrived(self.rcv.at[way, rows], self.sem.at[k])
            return self.rcv.at[0][...].astype(F32) + self.rcv.at[1][...].astype(F32)

        def total(self):
            return self.received() + self.src(ME)[...].astype(F32)

    class Spread:
        def __init__(self, ps, hf, devices):
            self.src, self.rcv, self.devices = s2_s.at[ps, hf], t_s.at[ps, hf], devices
            self.sem, self.ssem = rsem.at[hf, TAIL], msem_s.at[ps, 0, 0]

        def put(self, j):
            send(self.src.at[j], self.rcv.at[j], self.ssem, self.sem.at[j], self.devices[j])

        def received(self):
            for j in ORDER[:3]:
                arrived(self.rcv.at[j], self.sem.at[j])
            return sum(self.rcv.at[j][...].astype(F32) for j in ORDER[:3])

    def reduce_scatter(ps, chunk, between):
        first, second = [], []
        for hf in range(2):
            a, b, ap, am, bp, bm, bf = place[hf]
            first.append([Exchange(ps, hf, j, lambda d, hf=hf, a=a, b=b, j=j: p_s.at[ps, hf, up1(a, d), up1(b, j)], ap, am)
                          for j in range(4)])
            second.append(Spread(ps, hf, {NEXT: bp, FAR: bf, PREV: bm}))

        def directs(hf, j):
            first[hf][j].direct(NEXT)
            first[hf][j].direct(PREV)

        for hf in range(2):
            chunk(hf, up1(place[hf][0], FAR))
            for j in ORDER:
                first[hf][j].relay()
        for hf in range(2):
            chunk(hf, up1(place[hf][0], NEXT))
            chunk(hf, up1(place[hf][0], PREV))
            directs(hf, ORDER[0])
            directs(hf, ORDER[1])
        for hf in range(2):
            chunk(hf, place[hf][0])
        for t, j in enumerate(ORDER):
            for hf in range(2):
                first[hf][j].join()
                if t < 2:
                    directs(hf, ORDER[t + 2])
        for j in ORDER[:3]:
            for hf in range(2):
                s2_s[ps, hf, j] = first[hf][j].total().astype(BF)
                second[hf].put(j)
            if j == FAR:
                between()
        own_sum = [first[hf][ME].total() for hf in range(2)]
        return [own_sum[hf] + second[hf].received() for hf in range(2)]

    class Ring:
        def __init__(self, ps, hf, e, blk, fwd, bwd):
            self.blk, self.fwd, self.bwd, self.sem = blk, fwd, bwd, asem.at[hf, e]
            self.ssem = msem_s.at[ps, 1, 0 if e == TAIL else 1]

        def put(self, k, d, rows, device):
            r = self.blk(d, rows)
            send(r, r, self.ssem, self.sem.at[k], device)

        def start(self):
            self.put(0, ME, lo, self.fwd)
            self.put(1, ME, hi, self.bwd)
            self.put(2, ME, hi, self.fwd)
            self.put(3, ME, lo, self.bwd)

        def forward(self):
            arrived(self.blk(PREV, lo), self.sem.at[0])
            self.put(4, PREV, lo, self.fwd)
            arrived(self.blk(NEXT, hi), self.sem.at[1])
            self.put(5, NEXT, hi, self.bwd)

        def got(self, d):
            for k, rows in {PREV: ((2, hi),), NEXT: ((3, lo),), FAR: ((4, lo), (5, hi))}[d]:
                arrived(self.blk(d, rows), self.sem.at[k])

    def all_gather(ps, buf, consume, hook):
        inner, outer = [], []
        for hf in range(2):
            a, b, ap, am, bp, bm, _ = place[hf]

            def block(ia, ib, rows, hf=hf):
                cols = pl.ds(hf * HALF, HALF)
                return buf.at[ia, ib, rows, cols] if hf == 0 else buf.at[ib, ia, rows, cols]

            inner.append(Ring(ps, hf, TAIL, lambda d, rows, a=a, b=b, block=block: block(a, up1(b, d), rows), bp, bm))
            outer.append([Ring(ps, hf, j, lambda d, rows, a=a, b=b, j=j, block=block: block(up1(a, d), up1(b, j), rows), ap, am)
                          for j in range(4)])
        for hf in range(2):
            inner[hf].start()
        for hf in range(2):
            outer[hf][ME].start()
        for hf in range(2):
            inner[hf].forward()
        for d in (PREV, NEXT):
            for hf in range(2):
                inner[hf].got(d)
                outer[hf][d].start()
        hook(0)
        for hf in range(2):
            outer[hf][ME].forward()
        for hf in range(2):
            inner[hf].got(FAR)
            outer[hf][FAR].start()
        for d in (PREV, NEXT):
            for hf in range(2):
                outer[hf][d].forward()
        hook(1)
        for hf in range(2):
            consume(hf, place[hf][0])
        for hf in range(2):
            outer[hf][FAR].forward()
        for d in (PREV, NEXT, FAR):
            for hf in range(2):
                for r in outer[hf]:
                    r.got(d)
                consume(hf, up1(place[hf][0], d))
            if d == NEXT:
                hook(2)

    def out_chunk(hf, i):
        rows = (o_s[i] if hf == 0 else o_s[:, i]).reshape(128, 160)
        part = mm(rows, wof_s[:, hf * HALF:hf * HALF + HALF], NN)
        p_s[0, hf, i] = part.astype(BF).reshape(4, 32, HALF)

    def attn_between():
        g_u.forward()
        g_u.share()

    part = reduce_scatter(0, out_chunk, attn_between)
    mine = pl.ds(pl.multiple_of(tp * 32, 32), 32)
    for hf in range(2):
        cols = slice(hf * HALF, hf * HALF + HALF)
        h_s[:, cols] = x_s[mine, cols].astype(F32) + part[hf]
    resid = h_s[...]
    inv = lax.rsqrt(jnp.sum(resid * resid, axis=1, keepdims=True) * (1.0 / DM) + NORM_EPS)
    gain = jnp.concatenate([wg_s[i, 1] for i in range(8)], axis=1)
    g_s[z, y] = (resid * inv * gain).astype(BF)

    def mlp_hook(step):
        if step == 0:
            g_u.last()
            g_d.forward()
        elif step == 1:
            g_d.share()
            g_u.siblings()
        else:
            g_d.last()

    def up_part(hf, i):
        w = wu_s[4 * hf:4 * hf + 4].reshape(HALF, FF)
        cols = slice(hf * HALF, hf * HALF + HALF)
        rows = (g_s[i, :, :, cols] if hf == 0 else g_s[:, i, :, cols]).reshape(128, HALF)
        prod = mm(rows, w, NN).reshape(4, 32, FF)
        if hf == 0:
            u_s[i] += prod
        else:
            u_s[:, i] += prod

    all_gather(0, g_s, up_part, mlp_hook)
    g_d.siblings()
    todo = [FAR], [NEXT, PREV, ME], [], [], [], [], [], []
    calls = iter(todo)

    def down_chunk(hf, i):
        for d in next(calls):
            k = up1(z, d)
            hid_s[k] = jax.nn.gelu(u_s[k], approximate=True).astype(BF)
        rows = (hid_s[i] if hf == 0 else hid_s[:, i]).reshape(128, FF)
        w = wd_s[4 * hf:4 * hf + 4].reshape(HALF, FF)
        p_s[1, hf, i] = mm(rows, w, NT).astype(BF).reshape(4, 32, HALF)

    part = reduce_scatter(1, down_chunk, lambda: None)
    y_v[z, y] = jnp.concatenate([h_s[:, 0:HALF] + part[0], h_s[:, HALF:DM] + part[1]], axis=1).astype(BF)
    all_gather(1, y_v, lambda hf, i: None, lambda step: None)
    for g in gathers:
        g.all_sent()
    for ps in range(2):
        for kind in range(2):
            sent(g_s.at[0, pl.ds(0, 3)], msem_s.at[ps, kind, 0], rsem.at[0, 0, 0])
            sent(g_s.at[pl.ds(0, 3)], msem_s.at[ps, kind, 1], rsem.at[0, 0, 0])


def result_kernel(y_v, k_v, v_v, y_h, k_h, v_h, sem):
    copies = [pltpu.make_async_copy(src, dst, sem.at[i]) for i, (src, dst) in enumerate(((y_v, y_h), (k_v, k_h), (v_v, v_h)))]
    for cp in copies:
        cp.start()
    for cp in copies:
        cp.wait()


def solution(mesh):
    tok_axes = ("dp", "wg")
    in_specs = (P(tok_axes, None), P("wg"), P("wg"), P("wg", None, "tp", None), P("wg", "tp", None), P("tp", None, "wg"), P("wg", "tp"), P("tp", "wg"), P("tp", None), P("tp", None), P(None, None), P(tok_axes, "tp", None, None), P(tok_axes, "tp", None, None), P(tok_axes))
    out_specs = (P(tok_axes, None), P(tok_axes, "tp", None), P(tok_axes, "tp", None))

    def vm(shape, dtype=BF):
        return pltpu.VMEM(shape, dtype)

    def dma(*shape):
        return pltpu.SemaphoreType.DMA(shape)

    blocks = (2, 2, 4, 2)
    scratch = [
        vm((SEQ, DM)), vm((1, SEQ), jnp.int32), vm((2, HD), F32), vm((2, HD), F32), vm((CL, DM)), vm((HW, SLICE)),
        vm((3 * HW, SLICE)), vm((HW, SLICE)), vm((8, 2, 1, SLICE), F32), vm((8, 240, FF)), vm((8, CL, HW), F32), vm((8, 80, FF)),
        vm((8, SLICE, FF)), vm((8, SLICE, FF)), vm((2, CL, HD, SEQ)), vm((2, CL, HD, SEQ)),
        vm((SEQ, 128), F32), vm((3 * HW, SEQ), F32), vm((HD, SEQ), F32), vm((CL, SEQ), F32),
        vm((HW, SEQ), F32), vm((4, 4, 32, HW)), vm((HW, DM)), vm((2, 2, 4, 4, 32, HALF)),
        vm(blocks + (16, HALF)), vm(blocks + (32, HALF)), vm(blocks + (16, HALF)), vm((2, 2, 4, 32, HALF)), vm((2, 2, 4, 32, HALF)),
        vm((32, DM), F32), vm((4, 4, 32, DM)), vm((4, 4, 32, FF), F32), vm((4, 4, 32, FF)), vm((SEQ, FF)),
        dma(14), dma(6), dma(6, 10), dma(2, 2, 2), dma(2, 5, 6), dma(2, 5, 6),
    ]
    call = pl.pallas_call(
        layer_kernel,
        out_shape=[vm((4, 4, 32, DM)), vm((HW, SEQ)), vm((HW, SEQ))],
        in_specs=[pl.BlockSpec(memory_space=ANY)] * 14,
        out_specs=[pl.BlockSpec(memory_space=pltpu.VMEM)] * 3,
        scratch_shapes=scratch,
        compiler_params=pltpu.CompilerParams(collective_id=0, has_side_effects=True, vmem_limit_bytes=56 * 1024 * 1024),
        name="layer",
    )

    shapes = ((4, 4, 32, DM), (HW, SEQ), (HW, SEQ))
    write = pl.pallas_call(
        result_kernel,
        out_shape=[jax.ShapeDtypeStruct(shape, BF) for shape in shapes],
        in_specs=[pl.BlockSpec(memory_space=pltpu.VMEM)] * 3,
        out_specs=[pl.BlockSpec(memory_space=ANY)] * 3,
        scratch_shapes=[dma(3)],
        compiler_params=pltpu.CompilerParams(vmem_limit_bytes=1 << 20),
        name="results",
    )

    def device_step(tokens, gain_attn, gain_mlp, w_qkv, w_rel, w_out, w_up, w_down, bias_u, bias_v, rel_table, k_cache, v_cache, positions):
        out, k_new, v_new = write(*call(
            tokens, positions.reshape(1, SEQ), bias_u, bias_v, gain_attn, gain_mlp,
            w_qkv.transpose(1, 2, 3, 0).reshape(480, 320), w_rel.transpose(1, 2, 0).reshape(160, 320),
            w_out.reshape(160, 320), w_up, w_down.T, rel_table,
            k_cache.transpose(1, 2, 3, 0), v_cache.transpose(1, 2, 3, 0)))
        return (out.reshape(SEQ, DM), k_new.reshape(2, HD, SEQ).transpose(2, 0, 1), v_new.reshape(2, HD, SEQ).transpose(2, 0, 1))

    return jax.shard_map(device_step, mesh=mesh, in_specs=in_specs, out_specs=out_specs, check_vma=False)
```

```python
import jax
import jax.numpy as jnp
from jax import lax
from jax.experimental import pallas as pl
from jax.experimental.pallas import tpu as pltpu
from jax.sharding import PartitionSpec as P

NORM_EPS = 1e-6
BF = jnp.bfloat16
F32 = jnp.float32
MESH = pl.DeviceIdType.MESH
ANY = pl.ANY
SEQ, DM, HALF, HD, CL, FF = 512, 2560, 1280, 80, 32, 640
SLICE, HW, QK = 320, 160, 320
ME, NEXT, FAR, PREV, TAIL = range(5)
LO, HI, WHOLE = 0, 1, None
BOTH = range(2)
ORDER = (FAR, NEXT, PREV, ME)
NT = (((1,), (1,)), ((), ()))
NN = (((1,), (0,)), ((), ()))
TN = (((0,), (0,)), ((), ()))


def mm(a, b, dims):
    return lax.dot_general(a, b, dims, preferred_element_type=F32)


def layer_kernel(x_h, pos_h, bu_h, bv_h, ga_h, gm_h, wq_h, wr_h, wo_h, wu_h, wd_h, rt_h, k_h, v_h,
                 y_v, kn_s, vn_s,
                 x_s, pos_s, bu_s, bv_s, rt_s, wr_s, wqt_s, wot_s, wg_s, wk_s, wv_s, qp_s, wo_s, wu_s, wd_s, k_s, v_s,
                 rs_s, acc, qu_s, sc_s, sp_s, ot_s, o_s, wof_s, p_s, rel_s, rcv_s, stg_s, s2_s, t_s, h_s, g_s, u_s, hid_s, n_s,
                 lsem, gsem_s, gsem_r, msem_s, rsem, asem):
    tp, wg = lax.axis_index("tp"), lax.axis_index("wg")
    z, y = tp // 4, tp % 4
    x, c = wg // 2, wg % 2

    def up1(i, d):
        return lax.rem(i + d, 4)

    def dev(dz=0, dy=0, dx=0, flip=False):
        cc = 1 - c if flip else c
        return (0, up1(z, dz) * 4 + up1(y, dy), up1(x, dx) * 2 + cc)

    xp, xm, sib = dev(dx=1), dev(dx=3), dev(flip=True)
    zp, zm, yp, ym = dev(dz=1), dev(dz=3), dev(dy=1), dev(dy=3)
    xf, zf, yf = dev(dx=2), dev(dz=2), dev(dy=2)

    def send(src, dst, ssem, rsem, device):
        pltpu.make_async_remote_copy(src, dst, ssem, rsem, device_id=device, device_id_type=MESH).start()

    def sent(ref, ssem, rsem):
        pltpu.make_async_remote_copy(ref, ref, ssem, rsem, device_id=sib, device_id_type=MESH).wait_send()

    def arrived(dst, rsem):
        pltpu.make_async_remote_copy(dst, dst, gsem_s.at[0], rsem, device_id=sib, device_id_type=MESH).wait_recv()

    n_local = [0]

    def local(src, dst):
        cp = pltpu.make_async_copy(src, dst, lsem.at[n_local[0]])
        n_local[0] += 1
        cp.start()
        return cp

    barrier = pltpu.get_barrier_semaphore()
    peers = (xp, xm, xf, sib, zp, zm, zf, yp, ym, yf)
    for d in peers:
        pl.semaphore_signal(barrier, inc=1, device_id=d, device_id_type=MESH)

    own = 2 * x + c
    l_g = [local(ga_h, wg_s.at[own, 0, 0]), local(gm_h, wg_s.at[own, 1, 0])]
    l_q = local(wq_h, wqt_s)
    l_x = local(x_h, x_s)
    l_rt = local(rt_h, rt_s)
    l_pos = local(pos_h, pos_s)
    l_bu = local(bu_h, bu_s)
    l_bv = local(bv_h, bv_s)
    l_wr = local(wr_h, wr_s)
    l_wo = local(wo_h, wot_s)
    l_wu = local(wu_h, wu_s.at[own])
    l_wd = local(wd_h, wd_s.at[own])
    l_k = local(k_h, k_s)
    l_v = local(v_h, v_s)

    def slot(dx, flip=False):
        return 2 * up1(x, dx) + (1 - c if flip else c)

    class Gather:
        def __init__(self, ar, buf, rows, low):
            self.ar, self.buf, self.rows, self.low, self.relay = ar, buf, rows, low, True

        def ref(self, s, part):
            if part is WHOLE:
                return self.buf.at[s]
            return self.buf.at[s, pl.ds(0, self.low) if part == LO else pl.ds(self.low, self.rows - self.low)]

        def put(self, k, s, part, device):
            r = self.ref(s, part)
            send(r, r, gsem_s.at[self.ar], gsem_r.at[self.ar, k], device)

        def got(self, k, s, part):
            arrived(self.ref(s, part), gsem_r.at[self.ar, k])

        def start(self):
            o = slot(ME)
            if not self.relay:
                self.put(4, o, LO, xf)
                self.put(5, o, HI, xf)
            self.put(0, o, LO, xp)
            self.put(1, o, HI, xm)
            self.put(2, o, HI, xp)
            self.put(3, o, LO, xm)
            self.put(6, o, WHOLE, sib)

        def forward(self):
            self.got(0, slot(PREV), LO)
            if self.relay:
                self.put(4, slot(PREV), LO, xp)
            self.got(1, slot(NEXT), HI)
            if self.relay:
                self.put(5, slot(NEXT), HI, xm)

        def share(self):
            self.got(2, slot(PREV), HI)
            self.put(7, slot(PREV), WHOLE, sib)
            self.got(3, slot(NEXT), LO)
            self.put(8, slot(NEXT), WHOLE, sib)

        def last(self):
            self.got(4, slot(FAR), LO)
            self.got(5, slot(FAR), HI)
            self.put(9, slot(FAR), WHOLE, sib)

        def sibling(self, dx):
            self.got({ME: 6, PREV: 7, NEXT: 8, FAR: 9}[dx], slot(dx, True), WHOLE)

        def siblings(self):
            for dx in (ME, PREV, NEXT, FAR):
                self.sibling(dx)

        def all_sent(self):
            sent(self.buf.at[pl.ds(0, 7)], gsem_s.at[self.ar], gsem_r.at[self.ar, 0])

    g_g, g_k, g_v, g_o, g_u, g_d, g_r = gathers = [Gather(i, *spec) for i, spec in enumerate((
        (wg_s, 2, 1), (wk_s, HW, 80), (wv_s, 80, 48), (wo_s, 80, 48), (wu_s, SLICE, HW), (wd_s, SLICE, HW), (qp_s, CL, 16)))]
    g_v.relay = g_o.relay = False

    l_q.wait()
    wk_s[own] = jnp.concatenate([wqt_s[0:HW, :], wqt_s[HW:QK, :]], axis=1)
    wv_s[own] = jnp.concatenate([wqt_s[QK:400, :], wqt_s[400:480, :]], axis=1)
    l_wo.wait()
    wo_s[own] = jnp.concatenate([wot_s[0:80, :], wot_s[80:160, :]], axis=1)
    l_x.wait()

    def stat_rows(r, carry):
        rows = pl.ds(pl.multiple_of(r * 32, 32), 32)
        v = x_s[rows, :].astype(F32)
        ms = jnp.sum(v * v, axis=1, keepdims=True) * (1.0 / DM)
        rs_s[rows, :] = jnp.broadcast_to(lax.rsqrt(ms + NORM_EPS), (32, 128))
        return carry

    lax.fori_loop(0, 16, stat_rows, 0)
    l_rt.wait()
    l_wr.wait()
    base = pl.multiple_of(640 * x, 128)
    q_even = mm(rt_s[:, pl.ds(base, 384)][:, 0:320], wr_s[...], NT)
    q_odd = mm(rt_s[:, pl.ds(pl.multiple_of(base + 256, 128), 384)][:, 64:384], wr_s[...], NT)
    qp_s[own] = jnp.where(c == 1, q_odd, q_even)
    for cp in l_g:
        cp.wait()
    pl.semaphore_wait(barrier, len(peers))
    g_g.start()
    g_k.start()
    g_r.start()
    acc[...] = jnp.zeros_like(acc)
    u_s[...] = jnp.zeros_like(u_s)

    def unpack(even, odd):
        halves = [jnp.concatenate([even[:, cut], odd[:, cut]], axis=1) for cut in (slice(0, SLICE), slice(SLICE, FF))]
        return jnp.concatenate(halves, axis=0)

    def norm_cols(dx):
        xo = up1(x, dx)
        cols = pl.ds(pl.multiple_of(xo * 640, 128), 640)
        g_g.sibling(dx)
        gain = jnp.concatenate([wg_s[2 * xo, 0], wg_s[2 * xo + 1, 0]], axis=1)
        n_s[dx] = (x_s[:, cols].astype(F32) * rs_s[:, 0:1] * gain).astype(BF)

    def pair(g, buf, rows, dx):
        xo = up1(x, dx)
        g.sibling(dx)
        acc[rows, :] += mm(unpack(buf[2 * xo], buf[2 * xo + 1]), n_s[dx], NT)

    qk_rows, v_rows = slice(0, QK), slice(QK, None)
    norm_cols(ME)
    pair(g_k, wk_s, qk_rows, ME)
    g_g.forward()
    g_k.forward()
    g_r.forward()
    g_v.start()
    g_o.start()
    g_g.share()
    g_k.share()
    g_r.share()
    l_wu.wait()
    g_u.start()
    l_wd.wait()
    g_d.start()
    g_g.last()
    for dx in (PREV, NEXT, FAR):
        norm_cols(dx)
    pair(g_k, wk_s, qk_rows, PREV)
    g_k.last()
    g_r.last()
    pair(g_k, wk_s, qk_rows, NEXT)
    pair(g_v, wv_s, v_rows, ME)
    pair(g_k, wk_s, qk_rows, FAR)

    kn_s[...] = acc[HW:QK, :].astype(BF)
    l_pos.wait()
    l_bu.wait()
    l_bv.wait()
    g_r.siblings()

    flip_rows = (lax.broadcasted_iota(jnp.int32, (CL, CL), 0) + lax.broadcasted_iota(jnp.int32, (CL, CL), 1)) % CL == 0
    flip_mat = jnp.where(flip_rows, 1.0, 0.0).astype(BF)
    q_rel = qp_s[0]
    for i in range(1, 8):
        q_rel = q_rel + qp_s[i]
    rel_rev = mm(flip_mat, q_rel.astype(BF), NN).astype(BF)
    diag = lax.broadcasted_iota(jnp.int32, (HD, HD), 0) == lax.broadcasted_iota(jnp.int32, (HD, HD), 1)

    def column(row):
        return jnp.sum(jnp.where(diag, row, 0.0), axis=1, keepdims=True)

    lanes = [slice(first, first + 128) for first in range(0, SEQ, 128)]
    pos = pos_s[...]
    steps = lax.broadcasted_iota(jnp.int32, (CL, SEQ), 0)
    is_self = steps == pos
    l_k.wait()

    for h in BOTH:
        hr = slice(h * HD, h * HD + HD)
        q = acc[hr, :].astype(BF).astype(F32)
        q_u = (q + column(bu_s[h:h + 1, :])).astype(BF).astype(F32)
        q_v = (q + column(bv_s[h:h + 1, :])).astype(BF)
        qu_s[...] = q_u
        rel = mm(rel_rev[:, hr], q_v, NN)
        for b in range(5):
            rel = jnp.where((pos >> b) & 1 == 1, pltpu.roll(rel, 1 << b, 0), rel)
        self_score = jnp.sum(q_u * kn_s[hr, :].astype(F32), axis=0, keepdims=True)
        for ln in lanes:
            quc = qu_s[:, ln]

            def content(g, carry, h=h, ln=ln, quc=quc):
                rows = [jnp.sum(k_s[h, g * 8 + j, :, ln].astype(F32) * quc, axis=0, keepdims=True) for j in range(8)]
                sc_s[h, pl.ds(pl.multiple_of(g * 8, 8), 8), ln] = jnp.concatenate(rows, axis=0)
                return carry

            lax.fori_loop(0, CL // 8, content, 0)
        scores = jnp.where(is_self, self_score, sc_s[h])
        scores = jnp.where(steps <= pos, (scores + rel) * (HD ** -0.5), -1e30)
        e = jnp.exp(scores - jnp.max(scores, axis=0, keepdims=True))
        prob = (e / jnp.sum(e, axis=0, keepdims=True)).astype(BF).astype(F32)
        sp_s[h] = jnp.sum(jnp.where(is_self, prob, 0.0), axis=0, keepdims=True)
        sc_s[h] = jnp.where(is_self, 0.0, prob)
        if h == 0:
            g_v.forward()
            g_v.share()
            g_v.last()

    for dx in (PREV, NEXT, FAR):
        pair(g_v, wv_s, v_rows, dx)
    vn_s[...] = acc[v_rows, :].astype(BF)
    l_v.wait()
    for h in BOTH:
        hr = slice(h * HD, h * HD + HD)
        for ln in lanes:

            def mix(g, o, h=h, ln=ln):
                pr = sc_s[h, pl.ds(pl.multiple_of(g * 8, 8), 8), ln]
                for j in range(8):
                    o = o + pr[j:j + 1, :] * v_s[h, g * 8 + j, :, ln].astype(F32)
                return o

            start = sp_s[h, :, ln] * vn_s[hr, ln].astype(F32)
            ot_s[hr, ln] = lax.fori_loop(0, CL // 8, mix, start)

    o_s[...] = jnp.transpose(ot_s[...]).astype(BF).reshape(4, 4, 32, 160)
    g_o.forward()
    g_o.share()
    g_o.last()
    g_o.siblings()
    for xo in range(4):
        wof_s[:, 640 * xo:640 * xo + 640] = unpack(wo_s[2 * xo], wo_s[2 * xo + 1])

    place = ((z, y, zp, zm, yp, ym, yf), (y, z, yp, ym, zp, zm, zf))

    lo, hi = pl.ds(0, 16), pl.ds(16, 16)

    class Exchange:
        def __init__(self, ps, hf, e, src, fwd, bwd):
            self.src, self.fwd, self.bwd, self.sem = src, fwd, bwd, rsem.at[hf, e]
            self.ssem = msem_s.at[ps, 0, 1]
            self.rel, self.rcv, self.stg = rel_s.at[ps, hf, e], rcv_s.at[ps, hf, e], stg_s.at[ps, hf, e]

        def relay(self):
            send(self.src(FAR).at[lo], self.rel.at[LO], self.ssem, self.sem.at[0], self.fwd)
            send(self.src(FAR).at[hi], self.rel.at[HI], self.ssem, self.sem.at[1], self.bwd)

        def direct(self, d):
            if d == NEXT:
                send(self.src(NEXT).at[hi], self.rcv.at[0, hi], self.ssem, self.sem.at[2], self.fwd)
            else:
                send(self.src(PREV).at[lo], self.rcv.at[1, lo], self.ssem, self.sem.at[3], self.bwd)

        def join(self):
            for part, rows, d, device in ((LO, lo, NEXT, self.fwd), (HI, hi, PREV, self.bwd)):
                arrived(self.rel.at[part], self.sem.at[part])
                both = self.src(d).at[rows][...].astype(F32) + self.rel.at[part][...].astype(F32)
                self.stg.at[part][...] = both.astype(BF)
                send(self.stg.at[part], self.rcv.at[part, rows], self.ssem, self.sem.at[4 + part], device)

        def received(self):
            for k, way, rows in ((2, 0, hi), (3, 1, lo), (4, 0, lo), (5, 1, hi)):
                arrived(self.rcv.at[way, rows], self.sem.at[k])
            return self.rcv.at[0][...].astype(F32) + self.rcv.at[1][...].astype(F32)

        def total(self):
            return self.received() + self.src(ME)[...].astype(F32)

    class Spread:
        def __init__(self, ps, hf, devices):
            self.src, self.rcv, self.devices = s2_s.at[ps, hf], t_s.at[ps, hf], devices
            self.sem, self.ssem = rsem.at[hf, TAIL], msem_s.at[ps, 0, 0]

        def put(self, j):
            send(self.src.at[j], self.rcv.at[j], self.ssem, self.sem.at[j], self.devices[j])

        def received(self):
            for j in ORDER[:3]:
                arrived(self.rcv.at[j], self.sem.at[j])
            return sum(self.rcv.at[j][...].astype(F32) for j in ORDER[:3])

    def reduce_scatter(ps, chunk, between):
        first, second = [], []
        for hf in BOTH:
            a, b, ap, am, bp, bm, bf = place[hf]
            first.append([Exchange(ps, hf, j, lambda d, hf=hf, a=a, b=b, j=j: p_s.at[ps, hf, up1(a, d), up1(b, j)], ap, am)
                          for j in range(4)])
            second.append(Spread(ps, hf, {NEXT: bp, FAR: bf, PREV: bm}))

        def directs(hf, j):
            first[hf][j].direct(NEXT)
            first[hf][j].direct(PREV)

        for hf in BOTH:
            chunk(hf, up1(place[hf][0], FAR))
            for j in ORDER:
                first[hf][j].relay()
        for hf in BOTH:
            chunk(hf, up1(place[hf][0], NEXT))
            chunk(hf, up1(place[hf][0], PREV))
            directs(hf, ORDER[0])
            directs(hf, ORDER[1])
        for hf in BOTH:
            chunk(hf, place[hf][0])
        for t, j in enumerate(ORDER):
            for hf in BOTH:
                first[hf][j].join()
                if t < 2:
                    directs(hf, ORDER[t + 2])
        for j in ORDER[:3]:
            for hf in BOTH:
                s2_s[ps, hf, j] = first[hf][j].total().astype(BF)
                second[hf].put(j)
            if j == FAR:
                between()
        own_sum = [first[hf][ME].total() for hf in BOTH]
        return [own_sum[hf] + second[hf].received() for hf in BOTH]

    class Ring:
        def __init__(self, ps, hf, e, blk, fwd, bwd):
            self.blk, self.fwd, self.bwd, self.sem = blk, fwd, bwd, asem.at[hf, e]
            self.ssem = msem_s.at[ps, 1, 0 if e == TAIL else 1]

        def put(self, k, d, rows, device):
            r = self.blk(d, rows)
            send(r, r, self.ssem, self.sem.at[k], device)

        def start(self):
            self.put(0, ME, lo, self.fwd)
            self.put(1, ME, hi, self.bwd)
            self.put(2, ME, hi, self.fwd)
            self.put(3, ME, lo, self.bwd)

        def forward(self):
            arrived(self.blk(PREV, lo), self.sem.at[0])
            self.put(4, PREV, lo, self.fwd)
            arrived(self.blk(NEXT, hi), self.sem.at[1])
            self.put(5, NEXT, hi, self.bwd)

        def got(self, d):
            for k, rows in {PREV: ((2, hi),), NEXT: ((3, lo),), FAR: ((4, lo), (5, hi))}[d]:
                arrived(self.blk(d, rows), self.sem.at[k])

    def all_gather(ps, buf, consume, hook):
        inner, outer = [], []
        for hf in BOTH:
            a, b, ap, am, bp, bm, _ = place[hf]

            def block(ia, ib, rows, hf=hf):
                cols = pl.ds(hf * HALF, HALF)
                return buf.at[ia, ib, rows, cols] if hf == 0 else buf.at[ib, ia, rows, cols]

            inner.append(Ring(ps, hf, TAIL, lambda d, rows, a=a, b=b, block=block: block(a, up1(b, d), rows), bp, bm))
            outer.append([Ring(ps, hf, j, lambda d, rows, a=a, b=b, j=j, block=block: block(up1(a, d), up1(b, j), rows), ap, am)
                          for j in range(4)])
        for hf in BOTH:
            inner[hf].start()
        for hf in BOTH:
            outer[hf][ME].start()
        for hf in BOTH:
            inner[hf].forward()
        for d in (PREV, NEXT):
            for hf in BOTH:
                inner[hf].got(d)
                outer[hf][d].start()
        hook(0)
        for hf in BOTH:
            outer[hf][ME].forward()
        for hf in BOTH:
            inner[hf].got(FAR)
            outer[hf][FAR].start()
        for d in (PREV, NEXT):
            for hf in BOTH:
                outer[hf][d].forward()
        hook(1)
        for hf in BOTH:
            consume(hf, place[hf][0])
        for hf in BOTH:
            outer[hf][FAR].forward()
        for d in (PREV, NEXT, FAR):
            for hf in BOTH:
                for r in outer[hf]:
                    r.got(d)
                consume(hf, up1(place[hf][0], d))
            if d == NEXT:
                hook(2)

    def out_chunk(hf, i):
        rows = (o_s[i] if hf == 0 else o_s[:, i]).reshape(128, 160)
        part = mm(rows, wof_s[:, hf * HALF:hf * HALF + HALF], NN)
        p_s[0, hf, i] = part.astype(BF).reshape(4, 32, HALF)

    def attn_between():
        g_u.forward()
        g_u.share()

    part = reduce_scatter(0, out_chunk, attn_between)
    mine = pl.ds(pl.multiple_of(tp * 32, 32), 32)
    for hf in BOTH:
        cols = slice(hf * HALF, hf * HALF + HALF)
        h_s[:, cols] = x_s[mine, cols].astype(F32) + part[hf]
    resid = h_s[...]
    inv = lax.rsqrt(jnp.sum(resid * resid, axis=1, keepdims=True) * (1.0 / DM) + NORM_EPS)
    gain = jnp.concatenate([wg_s[i, 1] for i in range(8)], axis=1)
    g_s[z, y] = (resid * inv * gain).astype(BF)

    def mlp_hook(step):
        if step == 0:
            g_u.last()
            g_d.forward()
        elif step == 1:
            g_d.share()
            g_u.siblings()
        else:
            g_d.last()

    def up_part(hf, i):
        w = wu_s[4 * hf:4 * hf + 4].reshape(HALF, FF)
        cols = slice(hf * HALF, hf * HALF + HALF)
        rows = (g_s[i, :, :, cols] if hf == 0 else g_s[:, i, :, cols]).reshape(128, HALF)
        prod = mm(rows, w, NN).reshape(4, 32, FF)
        if hf == 0:
            u_s[i] += prod
        else:
            u_s[:, i] += prod

    all_gather(0, g_s, up_part, mlp_hook)
    g_d.siblings()
    todo = [FAR], [NEXT, PREV, ME], [], [], [], [], [], []
    calls = iter(todo)

    def down_chunk(hf, i):
        for d in next(calls):
            k = up1(z, d)
            hid_s[k] = jax.nn.gelu(u_s[k], approximate=True).astype(BF)
        rows = (hid_s[i] if hf == 0 else hid_s[:, i]).reshape(128, FF)
        w = wd_s[4 * hf:4 * hf + 4].reshape(HALF, FF)
        p_s[1, hf, i] = mm(rows, w, NT).astype(BF).reshape(4, 32, HALF)

    part = reduce_scatter(1, down_chunk, lambda: None)
    y_v[z, y] = jnp.concatenate([h_s[:, 0:HALF] + part[0], h_s[:, HALF:DM] + part[1]], axis=1).astype(BF)
    all_gather(1, y_v, lambda hf, i: None, lambda step: None)
    for g in gathers:
        g.all_sent()
    for ps in BOTH:
        for kind in BOTH:
            sent(g_s.at[0, pl.ds(0, 3)], msem_s.at[ps, kind, 0], rsem.at[0, 0, 0])
            sent(g_s.at[pl.ds(0, 3)], msem_s.at[ps, kind, 1], rsem.at[0, 0, 0])


def result_kernel(y_v, k_v, v_v, y_h, k_h, v_h, sem):
    copies = [pltpu.make_async_copy(src, dst, sem.at[i]) for i, (src, dst) in enumerate(((y_v, y_h), (k_v, k_h), (v_v, v_h)))]
    for cp in copies:
        cp.start()
    for cp in copies:
        cp.wait()


def solution(mesh):
    tok_axes = ("dp", "wg")
    in_specs = (P(tok_axes, None), P("wg"), P("wg"), P("wg", None, "tp", None), P("wg", "tp", None), P("tp", None, "wg"), P("wg", "tp"), P("tp", "wg"), P("tp", None), P("tp", None), P(None, None), P(tok_axes, "tp", None, None), P(tok_axes, "tp", None, None), P(tok_axes))
    out_specs = (P(tok_axes, None), P(tok_axes, "tp", None), P(tok_axes, "tp", None))

    def vm(shape, dtype=BF):
        return pltpu.VMEM(shape, dtype)

    def dma(*shape):
        return pltpu.SemaphoreType.DMA(shape)

    blocks = (2, 2, 4, 2)
    scratch = [
        vm((SEQ, DM)), vm((1, SEQ), jnp.int32), vm((2, HD), F32), vm((2, HD), F32), vm((CL, DM)), vm((HW, SLICE)),
        vm((3 * HW, SLICE)), vm((HW, SLICE)), vm((8, 2, 1, SLICE), F32), vm((8, HW, FF)), vm((8, 80, FF)), vm((8, CL, HW), F32), vm((8, 80, FF)),
        vm((8, SLICE, FF)), vm((8, SLICE, FF)), vm((2, CL, HD, SEQ)), vm((2, CL, HD, SEQ)),
        vm((SEQ, 128), F32), vm((3 * HW, SEQ), F32), vm((HD, SEQ), F32), vm((2, CL, SEQ), F32), vm((2, 1, SEQ), F32),
        vm((HW, SEQ), F32), vm((4, 4, 32, HW)), vm((HW, DM)), vm((2, 2, 4, 4, 32, HALF)),
        vm(blocks + (16, HALF)), vm(blocks + (32, HALF)), vm(blocks + (16, HALF)), vm((2, 2, 4, 32, HALF)), vm((2, 2, 4, 32, HALF)),
        vm((32, DM), F32), vm((4, 4, 32, DM)), vm((4, 4, 32, FF), F32), vm((4, 4, 32, FF)), vm((4, SEQ, FF)),
        dma(14), dma(7), dma(7, 10), dma(2, 2, 2), dma(2, 5, 6), dma(2, 5, 6),
    ]
    call = pl.pallas_call(
        layer_kernel,
        out_shape=[vm((4, 4, 32, DM)), vm((HW, SEQ)), vm((HW, SEQ))],
        in_specs=[pl.BlockSpec(memory_space=ANY)] * 14,
        out_specs=[pl.BlockSpec(memory_space=pltpu.VMEM)] * 3,
        scratch_shapes=scratch,
        compiler_params=pltpu.CompilerParams(collective_id=0, has_side_effects=True, vmem_limit_bytes=56 * 1024 * 1024),
        name="layer",
    )

    shapes = ((4, 4, 32, DM), (HW, SEQ), (HW, SEQ))
    write = pl.pallas_call(
        result_kernel,
        out_shape=[jax.ShapeDtypeStruct(shape, BF) for shape in shapes],
        in_specs=[pl.BlockSpec(memory_space=pltpu.VMEM)] * 3,
        out_specs=[pl.BlockSpec(memory_space=ANY)] * 3,
        scratch_shapes=[dma(3)],
        compiler_params=pltpu.CompilerParams(vmem_limit_bytes=1 << 20),
        name="results",
    )

    def device_step(tokens, gain_attn, gain_mlp, w_qkv, w_rel, w_out, w_up, w_down, bias_u, bias_v, rel_table, k_cache, v_cache, positions):
        out, k_new, v_new = write(*call(
            tokens, positions.reshape(1, SEQ), bias_u, bias_v, gain_attn, gain_mlp,
            w_qkv.transpose(1, 2, 3, 0).reshape(480, 320), w_rel.transpose(1, 2, 0).reshape(160, 320),
            w_out.reshape(160, 320), w_up, w_down.T, rel_table,
            k_cache.transpose(1, 2, 3, 0), v_cache.transpose(1, 2, 3, 0)))
        return (out.reshape(SEQ, DM), k_new.reshape(2, HD, SEQ).transpose(2, 0, 1), v_new.reshape(2, HD, SEQ).transpose(2, 0, 1))

    return jax.shard_map(device_step, mesh=mesh, in_specs=in_specs, out_specs=out_specs, check_vma=False)
```

```python
import jax
import jax.numpy as jnp
from jax import lax
from jax.experimental import pallas as pl
from jax.experimental.pallas import tpu as pltpu
from jax.sharding import PartitionSpec as P

NORM_EPS = 1e-6
BF = jnp.bfloat16
F32 = jnp.float32
MESH = pl.DeviceIdType.MESH
ANY = pl.ANY
SEQ, DM, HALF, HD, CL, FF = 512, 2560, 1280, 80, 32, 640
SLICE, HW, QK = 320, 160, 320
ME, NEXT, FAR, PREV, TAIL = range(5)
LO, HI, WHOLE = 0, 1, None
BOTH = range(2)
ORDER = (FAR, NEXT, PREV, ME)
NT = (((1,), (1,)), ((), ()))
NN = (((1,), (0,)), ((), ()))
TN = (((0,), (0,)), ((), ()))


def mm(a, b, dims):
    return lax.dot_general(a, b, dims, preferred_element_type=F32)


def layer_kernel(x_h, pos_h, bu_h, bv_h, ga_h, gm_h, wq_h, wr_h, wo_h, wu_h, wd_h, rt_h, k_h, v_h,
                 y_v, kn_s, vn_s,
                 x_s, pos_s, bu_s, bv_s, rt_s, wr_s, wqt_s, wot_s, wg_s, wk_s, wv_s, qp_s, wo_s, wu_s, wd_s, k_s, v_s,
                 rs_s, acc, qu_s, sc_s, sp_s, ot_s, o_s, wof_s, p_s, rel_s, rcv_s, stg_s, s2_s, t_s, h_s, g_s, u_s, hid_s, n_s,
                 lsem, gsem_s, gsem_r, msem_s, rsem, asem):
    tp, wg = lax.axis_index("tp"), lax.axis_index("wg")
    z, y = tp // 4, tp % 4
    x, c = wg // 2, wg % 2

    def up1(i, d):
        return lax.rem(i + d, 4)

    def dev(dz=0, dy=0, dx=0, flip=False):
        cc = 1 - c if flip else c
        return (0, up1(z, dz) * 4 + up1(y, dy), up1(x, dx) * 2 + cc)

    xp, xm, sib = dev(dx=1), dev(dx=3), dev(flip=True)
    zp, zm, yp, ym = dev(dz=1), dev(dz=3), dev(dy=1), dev(dy=3)
    xf, zf, yf = dev(dx=2), dev(dz=2), dev(dy=2)

    def send(src, dst, ssem, rsem, device):
        pltpu.make_async_remote_copy(src, dst, ssem, rsem, device_id=device, device_id_type=MESH).start()

    def sent(ref, ssem, rsem):
        pltpu.make_async_remote_copy(ref, ref, ssem, rsem, device_id=sib, device_id_type=MESH).wait_send()

    def arrived(dst, rsem):
        pltpu.make_async_remote_copy(dst, dst, gsem_s.at[0], rsem, device_id=sib, device_id_type=MESH).wait_recv()

    n_local = [0]

    def local(src, dst):
        cp = pltpu.make_async_copy(src, dst, lsem.at[n_local[0]])
        n_local[0] += 1
        cp.start()
        return cp

    barrier = pltpu.get_barrier_semaphore()
    peers = (xp, xm, xf, sib, zp, zm, zf, yp, ym, yf)
    for d in peers:
        pl.semaphore_signal(barrier, inc=1, device_id=d, device_id_type=MESH)

    own = 2 * x + c
    l_g = [local(ga_h, wg_s.at[own, 0, 0]), local(gm_h, wg_s.at[own, 1, 0])]
    l_q = local(wq_h, wqt_s)
    l_x = local(x_h, x_s)
    l_rt = local(rt_h, rt_s)
    l_pos = local(pos_h, pos_s)
    l_bu = local(bu_h, bu_s)
    l_bv = local(bv_h, bv_s)
    l_wr = local(wr_h, wr_s)
    l_wo = local(wo_h, wot_s)
    l_wu = local(wu_h, wu_s.at[own])
    l_wd = local(wd_h, wd_s.at[own])
    l_k = local(k_h, k_s)
    l_v = local(v_h, v_s)

    def slot(dx, flip=False):
        return 2 * up1(x, dx) + (1 - c if flip else c)

    class Gather:
        def __init__(self, ar, buf, rows, low):
            self.ar, self.buf, self.rows, self.low, self.relay = ar, buf, rows, low, True

        def ref(self, s, part):
            if part is WHOLE:
                return self.buf.at[s]
            return self.buf.at[s, pl.ds(0, self.low) if part == LO else pl.ds(self.low, self.rows - self.low)]

        def put(self, k, s, part, device):
            r = self.ref(s, part)
            send(r, r, gsem_s.at[self.ar], gsem_r.at[self.ar, k], device)

        def got(self, k, s, part):
            arrived(self.ref(s, part), gsem_r.at[self.ar, k])

        def start(self):
            o = slot(ME)
            if not self.relay:
                self.put(4, o, LO, xf)
                self.put(5, o, HI, xf)
            self.put(0, o, LO, xp)
            self.put(1, o, HI, xm)
            self.put(2, o, HI, xp)
            self.put(3, o, LO, xm)
            self.put(6, o, WHOLE, sib)

        def forward(self):
            self.got(0, slot(PREV), LO)
            if self.relay:
                self.put(4, slot(PREV), LO, xp)
            self.got(1, slot(NEXT), HI)
            if self.relay:
                self.put(5, slot(NEXT), HI, xm)

        def share(self):
            self.got(2, slot(PREV), HI)
            self.put(7, slot(PREV), WHOLE, sib)
            self.got(3, slot(NEXT), LO)
            self.put(8, slot(NEXT), WHOLE, sib)

        def last(self):
            self.got(4, slot(FAR), LO)
            self.got(5, slot(FAR), HI)
            self.put(9, slot(FAR), WHOLE, sib)

        def sibling(self, dx):
            self.got({ME: 6, PREV: 7, NEXT: 8, FAR: 9}[dx], slot(dx, True), WHOLE)

        def siblings(self):
            for dx in (ME, PREV, NEXT, FAR):
                self.sibling(dx)

        def all_sent(self):
            sent(self.buf.at[pl.ds(0, 7)], gsem_s.at[self.ar], gsem_r.at[self.ar, 0])

    g_g, g_k, g_v, g_o, g_u, g_d, g_r = gathers = [Gather(i, *spec) for i, spec in enumerate((
        (wg_s, 2, 1), (wk_s, HW, 80), (wv_s, 80, 48), (wo_s, 80, 48), (wu_s, SLICE, HW), (wd_s, SLICE, HW), (qp_s, CL, 16)))]
    g_o.relay = False

    l_q.wait()
    wk_s[own] = jnp.concatenate([wqt_s[0:HW, :], wqt_s[HW:QK, :]], axis=1)
    wv_s[own] = jnp.concatenate([wqt_s[QK:400, :], wqt_s[400:480, :]], axis=1)
    l_wo.wait()
    wo_s[own] = jnp.concatenate([wot_s[0:80, :], wot_s[80:160, :]], axis=1)
    l_x.wait()

    def stat_rows(r, carry):
        rows = pl.ds(pl.multiple_of(r * 32, 32), 32)
        v = x_s[rows, :].astype(F32)
        ms = jnp.sum(v * v, axis=1, keepdims=True) * (1.0 / DM)
        rs_s[rows, :] = jnp.broadcast_to(lax.rsqrt(ms + NORM_EPS), (32, 128))
        return carry

    lax.fori_loop(0, 16, stat_rows, 0)
    l_rt.wait()
    l_wr.wait()
    base = pl.multiple_of(640 * x, 128)
    q_even = mm(rt_s[:, pl.ds(base, 384)][:, 0:320], wr_s[...], NT)
    q_odd = mm(rt_s[:, pl.ds(pl.multiple_of(base + 256, 128), 384)][:, 64:384], wr_s[...], NT)
    qp_s[own] = jnp.where(c == 1, q_odd, q_even)
    for cp in l_g:
        cp.wait()
    pl.semaphore_wait(barrier, len(peers))
    g_g.start()
    g_r.start()
    g_k.start()
    g_v.start()
    acc[...] = jnp.zeros_like(acc)
    u_s[...] = jnp.zeros_like(u_s)

    def unpack(even, odd):
        halves = [jnp.concatenate([even[:, cut], odd[:, cut]], axis=1) for cut in (slice(0, SLICE), slice(SLICE, FF))]
        return jnp.concatenate(halves, axis=0)

    def norm_cols(dx):
        xo = up1(x, dx)
        cols = pl.ds(pl.multiple_of(xo * 640, 128), 640)
        g_g.sibling(dx)
        gain = jnp.concatenate([wg_s[2 * xo, 0], wg_s[2 * xo + 1, 0]], axis=1)
        n_s[dx] = (x_s[:, cols].astype(F32) * rs_s[:, 0:1] * gain).astype(BF)

    def pair(g, buf, rows, dx):
        xo = up1(x, dx)
        g.sibling(dx)
        acc[rows, :] += mm(unpack(buf[2 * xo], buf[2 * xo + 1]), n_s[dx], NT)

    qk_rows, v_rows = slice(0, QK), slice(QK, None)
    norm_cols(ME)
    pair(g_k, wk_s, qk_rows, ME)
    g_g.forward()
    g_r.forward()
    g_k.forward()
    g_g.share()
    g_r.share()
    g_k.share()
    g_v.forward()
    g_o.start()
    g_v.share()
    l_wu.wait()
    g_u.start()
    l_wd.wait()
    g_d.start()
    g_g.last()
    g_r.last()
    for dx in (PREV, NEXT, FAR):
        norm_cols(dx)
    pair(g_k, wk_s, qk_rows, PREV)
    pair(g_k, wk_s, qk_rows, NEXT)
    g_k.last()
    for dx in (ME, PREV, NEXT):
        pair(g_v, wv_s, v_rows, dx)
    pair(g_k, wk_s, qk_rows, FAR)
    g_v.last()

    kn_s[...] = acc[HW:QK, :].astype(BF)
    l_pos.wait()
    l_bu.wait()
    l_bv.wait()
    g_r.siblings()

    flip_rows = (lax.broadcasted_iota(jnp.int32, (CL, CL), 0) + lax.broadcasted_iota(jnp.int32, (CL, CL), 1)) % CL == 0
    flip_mat = jnp.where(flip_rows, 1.0, 0.0).astype(BF)
    q_rel = qp_s[0]
    for i in range(1, 8):
        q_rel = q_rel + qp_s[i]
    rel_rev = mm(flip_mat, q_rel.astype(BF), NN).astype(BF)
    diag = lax.broadcasted_iota(jnp.int32, (HD, HD), 0) == lax.broadcasted_iota(jnp.int32, (HD, HD), 1)

    def column(row):
        return jnp.sum(jnp.where(diag, row, 0.0), axis=1, keepdims=True)

    lanes = [slice(first, first + 128) for first in range(0, SEQ, 128)]
    pos = pos_s[...]
    steps = lax.broadcasted_iota(jnp.int32, (CL, SEQ), 0)
    is_self = steps == pos
    l_k.wait()

    for h in BOTH:
        hr = slice(h * HD, h * HD + HD)
        q = acc[hr, :].astype(BF).astype(F32)
        q_u = (q + column(bu_s[h:h + 1, :])).astype(BF).astype(F32)
        q_v = (q + column(bv_s[h:h + 1, :])).astype(BF)
        qu_s[...] = q_u
        rel = mm(rel_rev[:, hr], q_v, NN)
        for b in range(5):
            rel = jnp.where((pos >> b) & 1 == 1, pltpu.roll(rel, 1 << b, 0), rel)
        self_score = jnp.sum(q_u * kn_s[hr, :].astype(F32), axis=0, keepdims=True)
        for ln in lanes:
            quc = qu_s[:, ln]

            def content(g, carry, h=h, ln=ln, quc=quc):
                rows = [jnp.sum(k_s[h, g * 8 + j, :, ln].astype(F32) * quc, axis=0, keepdims=True) for j in range(8)]
                sc_s[h, pl.ds(pl.multiple_of(g * 8, 8), 8), ln] = jnp.concatenate(rows, axis=0)
                return carry

            lax.fori_loop(0, CL // 8, content, 0)
        scores = jnp.where(is_self, self_score, sc_s[h])
        scores = jnp.where(steps <= pos, (scores + rel) * (HD ** -0.5), -1e30)
        e = jnp.exp(scores - jnp.max(scores, axis=0, keepdims=True))
        prob = (e / jnp.sum(e, axis=0, keepdims=True)).astype(BF).astype(F32)
        sp_s[h] = jnp.sum(jnp.where(is_self, prob, 0.0), axis=0, keepdims=True)
        sc_s[h] = jnp.where(is_self, 0.0, prob)

    pair(g_v, wv_s, v_rows, FAR)
    vn_s[...] = acc[v_rows, :].astype(BF)
    l_v.wait()
    for h in BOTH:
        hr = slice(h * HD, h * HD + HD)
        for ln in lanes:

            def mix(g, o, h=h, ln=ln):
                pr = sc_s[h, pl.ds(pl.multiple_of(g * 8, 8), 8), ln]
                for j in range(8):
                    o = o + pr[j:j + 1, :] * v_s[h, g * 8 + j, :, ln].astype(F32)
                return o

            start = sp_s[h, :, ln] * vn_s[hr, ln].astype(F32)
            ot_s[hr, ln] = lax.fori_loop(0, CL // 8, mix, start)
        if h == 0:
            g_o.forward()
            g_o.share()

    g_o.last()
    o_s[...] = jnp.transpose(ot_s[...]).astype(BF).reshape(4, 4, 32, 160)
    for dx in (ME, PREV, NEXT, FAR):
        xo = up1(x, dx)
        g_o.sibling(dx)
        wof_s[:, pl.ds(pl.multiple_of(640 * xo, 128), 640)] = unpack(wo_s[2 * xo], wo_s[2 * xo + 1])

    place = ((z, y, zp, zm, yp, ym, yf), (y, z, yp, ym, zp, zm, zf))

    lo, hi = pl.ds(0, 16), pl.ds(16, 16)

    class Exchange:
        def __init__(self, ps, hf, e, src, fwd, bwd):
            self.src, self.fwd, self.bwd, self.sem = src, fwd, bwd, rsem.at[hf, e]
            self.ssem = msem_s.at[ps, 0, 1]
            self.rel, self.rcv, self.stg = rel_s.at[ps, hf, e], rcv_s.at[ps, hf, e], stg_s.at[ps, hf, e]

        def relay(self):
            send(self.src(FAR).at[lo], self.rel.at[LO], self.ssem, self.sem.at[0], self.fwd)
            send(self.src(FAR).at[hi], self.rel.at[HI], self.ssem, self.sem.at[1], self.bwd)

        def direct(self, d):
            if d == NEXT:
                send(self.src(NEXT).at[hi], self.rcv.at[0, hi], self.ssem, self.sem.at[2], self.fwd)
            else:
                send(self.src(PREV).at[lo], self.rcv.at[1, lo], self.ssem, self.sem.at[3], self.bwd)

        def join(self):
            for part, rows, d, device in ((LO, lo, NEXT, self.fwd), (HI, hi, PREV, self.bwd)):
                arrived(self.rel.at[part], self.sem.at[part])
                both = self.src(d).at[rows][...].astype(F32) + self.rel.at[part][...].astype(F32)
                self.stg.at[part][...] = both.astype(BF)
                send(self.stg.at[part], self.rcv.at[part, rows], self.ssem, self.sem.at[4 + part], device)

        def received(self):
            for k, way, rows in ((2, 0, hi), (3, 1, lo), (4, 0, lo), (5, 1, hi)):
                arrived(self.rcv.at[way, rows], self.sem.at[k])
            return self.rcv.at[0][...].astype(F32) + self.rcv.at[1][...].astype(F32)

        def total(self):
            return self.received() + self.src(ME)[...].astype(F32)

    class Spread:
        def __init__(self, ps, hf, devices):
            self.src, self.rcv, self.devices = s2_s.at[ps, hf], t_s.at[ps, hf], devices
            self.sem, self.ssem = rsem.at[hf, TAIL], msem_s.at[ps, 0, 0]

        def put(self, j):
            send(self.src.at[j], self.rcv.at[j], self.ssem, self.sem.at[j], self.devices[j])

        def received(self):
            for j in ORDER[:3]:
                arrived(self.rcv.at[j], self.sem.at[j])
            return sum(self.rcv.at[j][...].astype(F32) for j in ORDER[:3])

    def reduce_scatter(ps, chunk, between):
        first, second = [], []
        for hf in BOTH:
            a, b, ap, am, bp, bm, bf = place[hf]
            first.append([Exchange(ps, hf, j, lambda d, hf=hf, a=a, b=b, j=j: p_s.at[ps, hf, up1(a, d), up1(b, j)], ap, am)
                          for j in range(4)])
            second.append(Spread(ps, hf, {NEXT: bp, FAR: bf, PREV: bm}))

        def directs(hf, j):
            first[hf][j].direct(NEXT)
            first[hf][j].direct(PREV)

        for hf in BOTH:
            chunk(hf, up1(place[hf][0], FAR))
            for j in ORDER:
                first[hf][j].relay()
        for hf in BOTH:
            chunk(hf, up1(place[hf][0], NEXT))
            chunk(hf, up1(place[hf][0], PREV))
            directs(hf, ORDER[0])
            directs(hf, ORDER[1])
        for hf in BOTH:
            chunk(hf, place[hf][0])
        for t, j in enumerate(ORDER):
            for hf in BOTH:
                first[hf][j].join()
                if t < 2:
                    directs(hf, ORDER[t + 2])
        for j in ORDER[:3]:
            for hf in BOTH:
                s2_s[ps, hf, j] = first[hf][j].total().astype(BF)
                second[hf].put(j)
            if j == FAR:
                between()
        own_sum = [first[hf][ME].total() for hf in BOTH]
        return [own_sum[hf] + second[hf].received() for hf in BOTH]

    class Ring:
        def __init__(self, ps, hf, e, blk, fwd, bwd):
            self.blk, self.fwd, self.bwd, self.sem = blk, fwd, bwd, asem.at[hf, e]
            self.ssem = msem_s.at[ps, 1, 0 if e == TAIL else 1]

        def put(self, k, d, rows, device):
            r = self.blk(d, rows)
            send(r, r, self.ssem, self.sem.at[k], device)

        def start(self):
            self.put(0, ME, lo, self.fwd)
            self.put(1, ME, hi, self.bwd)
            self.put(2, ME, hi, self.fwd)
            self.put(3, ME, lo, self.bwd)

        def forward(self):
            arrived(self.blk(PREV, lo), self.sem.at[0])
            self.put(4, PREV, lo, self.fwd)
            arrived(self.blk(NEXT, hi), self.sem.at[1])
            self.put(5, NEXT, hi, self.bwd)

        def got(self, d):
            for k, rows in {PREV: ((2, hi),), NEXT: ((3, lo),), FAR: ((4, lo), (5, hi))}[d]:
                arrived(self.blk(d, rows), self.sem.at[k])

    def all_gather(ps, buf, consume, hook):
        inner, outer = [], []
        for hf in BOTH:
            a, b, ap, am, bp, bm, _ = place[hf]

            def block(ia, ib, rows, hf=hf):
                cols = pl.ds(hf * HALF, HALF)
                return buf.at[ia, ib, rows, cols] if hf == 0 else buf.at[ib, ia, rows, cols]

            inner.append(Ring(ps, hf, TAIL, lambda d, rows, a=a, b=b, block=block: block(a, up1(b, d), rows), bp, bm))
            outer.append([Ring(ps, hf, j, lambda d, rows, a=a, b=b, j=j, block=block: block(up1(a, d), up1(b, j), rows), ap, am)
                          for j in range(4)])
        for hf in BOTH:
            inner[hf].start()
        for hf in BOTH:
            outer[hf][ME].start()
        for hf in BOTH:
            inner[hf].forward()
        for d in (PREV, NEXT):
            for hf in BOTH:
                inner[hf].got(d)
                outer[hf][d].start()
        hook(0)
        for hf in BOTH:
            outer[hf][ME].forward()
        for hf in BOTH:
            inner[hf].got(FAR)
            outer[hf][FAR].start()
        for d in (PREV, NEXT):
            for hf in BOTH:
                outer[hf][d].forward()
        hook(1)
        for hf in BOTH:
            consume(hf, place[hf][0])
        for hf in BOTH:
            outer[hf][FAR].forward()
        for d in (PREV, NEXT, FAR):
            for hf in BOTH:
                for r in outer[hf]:
                    r.got(d)
                consume(hf, up1(place[hf][0], d))
            if d == NEXT:
                hook(2)

    def out_chunk(hf, i):
        rows = (o_s[i] if hf == 0 else o_s[:, i]).reshape(128, 160)
        part = mm(rows, wof_s[:, hf * HALF:hf * HALF + HALF], NN)
        p_s[0, hf, i] = part.astype(BF).reshape(4, 32, HALF)

    def attn_between():
        g_u.forward()
        g_u.share()

    part = reduce_scatter(0, out_chunk, attn_between)
    mine = pl.ds(pl.multiple_of(tp * 32, 32), 32)
    for hf in BOTH:
        cols = slice(hf * HALF, hf * HALF + HALF)
        h_s[:, cols] = x_s[mine, cols].astype(F32) + part[hf]
    resid = h_s[...]
    inv = lax.rsqrt(jnp.sum(resid * resid, axis=1, keepdims=True) * (1.0 / DM) + NORM_EPS)
    gain = jnp.concatenate([wg_s[i, 1] for i in range(8)], axis=1)
    g_s[z, y] = (resid * inv * gain).astype(BF)

    def mlp_hook(step):
        if step == 0:
            g_u.last()
            g_d.forward()
        elif step == 1:
            g_d.share()
            g_u.siblings()
        else:
            g_d.last()

    def up_part(hf, i):
        w = wu_s[4 * hf:4 * hf + 4].reshape(HALF, FF)
        cols = slice(hf * HALF, hf * HALF + HALF)
        rows = (g_s[i, :, :, cols] if hf == 0 else g_s[:, i, :, cols]).reshape(128, HALF)
        prod = mm(rows, w, NN).reshape(4, 32, FF)
        if hf == 0:
            u_s[i] += prod
        else:
            u_s[:, i] += prod

    all_gather(0, g_s, up_part, mlp_hook)
    g_d.siblings()
    todo = [FAR], [NEXT, PREV, ME], [], [], [], [], [], []
    calls = iter(todo)

    def down_chunk(hf, i):
        for d in next(calls):
            k = up1(z, d)
            hid_s[k] = jax.nn.gelu(u_s[k], approximate=True).astype(BF)
        rows = (hid_s[i] if hf == 0 else hid_s[:, i]).reshape(128, FF)
        w = wd_s[4 * hf:4 * hf + 4].reshape(HALF, FF)
        p_s[1, hf, i] = mm(rows, w, NT).astype(BF).reshape(4, 32, HALF)

    part = reduce_scatter(1, down_chunk, lambda: None)
    y_v[z, y] = jnp.concatenate([h_s[:, 0:HALF] + part[0], h_s[:, HALF:DM] + part[1]], axis=1).astype(BF)
    all_gather(1, y_v, lambda hf, i: None, lambda step: None)
    for g in gathers:
        g.all_sent()
    for ps in BOTH:
        for kind in BOTH:
            sent(g_s.at[0, pl.ds(0, 3)], msem_s.at[ps, kind, 0], rsem.at[0, 0, 0])
            sent(g_s.at[pl.ds(0, 3)], msem_s.at[ps, kind, 1], rsem.at[0, 0, 0])


def result_kernel(y_v, k_v, v_v, y_h, k_h, v_h, sem):
    copies = [pltpu.make_async_copy(src, dst, sem.at[i]) for i, (src, dst) in enumerate(((y_v, y_h), (k_v, k_h), (v_v, v_h)))]
    for cp in copies:
        cp.start()
    for cp in copies:
        cp.wait()


def solution(mesh):
    tok_axes = ("dp", "wg")
    in_specs = (P(tok_axes, None), P("wg"), P("wg"), P("wg", None, "tp", None), P("wg", "tp", None), P("tp", None, "wg"), P("wg", "tp"), P("tp", "wg"), P("tp", None), P("tp", None), P(None, None), P(tok_axes, "tp", None, None), P(tok_axes, "tp", None, None), P(tok_axes))
    out_specs = (P(tok_axes, None), P(tok_axes, "tp", None), P(tok_axes, "tp", None))

    def vm(shape, dtype=BF):
        return pltpu.VMEM(shape, dtype)

    def dma(*shape):
        return pltpu.SemaphoreType.DMA(shape)

    blocks = (2, 2, 4, 2)
    scratch = [
        vm((SEQ, DM)), vm((1, SEQ), jnp.int32), vm((2, HD), F32), vm((2, HD), F32), vm((CL, DM)), vm((HW, SLICE)),
        vm((3 * HW, SLICE)), vm((HW, SLICE)), vm((8, 2, 1, SLICE), F32), vm((8, HW, FF)), vm((8, 80, FF)), vm((8, CL, HW), F32), vm((8, 80, FF)),
        vm((8, SLICE, FF)), vm((8, SLICE, FF)), vm((2, CL, HD, SEQ)), vm((2, CL, HD, SEQ)),
        vm((SEQ, 128), F32), vm((3 * HW, SEQ), F32), vm((HD, SEQ), F32), vm((2, CL, SEQ), F32), vm((2, 1, SEQ), F32),
        vm((HW, SEQ), F32), vm((4, 4, 32, HW)), vm((HW, DM)), vm((2, 2, 4, 4, 32, HALF)),
        vm(blocks + (16, HALF)), vm(blocks + (32, HALF)), vm(blocks + (16, HALF)), vm((2, 2, 4, 32, HALF)), vm((2, 2, 4, 32, HALF)),
        vm((32, DM), F32), vm((4, 4, 32, DM)), vm((4, 4, 32, FF), F32), vm((4, 4, 32, FF)), vm((4, SEQ, FF)),
        dma(14), dma(7), dma(7, 10), dma(2, 2, 2), dma(2, 5, 6), dma(2, 5, 6),
    ]
    call = pl.pallas_call(
        layer_kernel,
        out_shape=[vm((4, 4, 32, DM)), vm((HW, SEQ)), vm((HW, SEQ))],
        in_specs=[pl.BlockSpec(memory_space=ANY)] * 14,
        out_specs=[pl.BlockSpec(memory_space=pltpu.VMEM)] * 3,
        scratch_shapes=scratch,
        compiler_params=pltpu.CompilerParams(collective_id=0, has_side_effects=True, vmem_limit_bytes=56 * 1024 * 1024),
        name="layer",
    )

    shapes = ((4, 4, 32, DM), (HW, SEQ), (HW, SEQ))
    write = pl.pallas_call(
        result_kernel,
        out_shape=[jax.ShapeDtypeStruct(shape, BF) for shape in shapes],
        in_specs=[pl.BlockSpec(memory_space=pltpu.VMEM)] * 3,
        out_specs=[pl.BlockSpec(memory_space=ANY)] * 3,
        scratch_shapes=[dma(3)],
        compiler_params=pltpu.CompilerParams(vmem_limit_bytes=1 << 20),
        name="results",
    )

    def device_step(tokens, gain_attn, gain_mlp, w_qkv, w_rel, w_out, w_up, w_down, bias_u, bias_v, rel_table, k_cache, v_cache, positions):
        out, k_new, v_new = write(*call(
            tokens, positions.reshape(1, SEQ), bias_u, bias_v, gain_attn, gain_mlp,
            w_qkv.transpose(1, 2, 3, 0).reshape(480, 320), w_rel.transpose(1, 2, 0).reshape(160, 320),
            w_out.reshape(160, 320), w_up, w_down.T, rel_table,
            k_cache.transpose(1, 2, 3, 0), v_cache.transpose(1, 2, 3, 0)))
        return (out.reshape(SEQ, DM), k_new.reshape(2, HD, SEQ).transpose(2, 0, 1), v_new.reshape(2, HD, SEQ).transpose(2, 0, 1))

    return jax.shard_map(device_step, mesh=mesh, in_specs=in_specs, out_specs=out_specs, check_vma=False)
```

```python
import jax
import jax.numpy as jnp
from jax import lax
from jax.experimental import pallas as pl
from jax.experimental.pallas import tpu as pltpu
from jax.sharding import PartitionSpec as P

NORM_EPS = 1e-6
BF = jnp.bfloat16
F32 = jnp.float32
MESH = pl.DeviceIdType.MESH
ANY = pl.ANY
SEQ, DM, HALF, HD, CL, FF = 512, 2560, 1280, 80, 32, 640
SLICE, HW, QK = 320, 160, 320
ME, NEXT, FAR, PREV, TAIL = range(5)
LO, HI, WHOLE = 0, 1, None
BOTH = range(2)
ORDER = (FAR, NEXT, PREV, ME)
NT = (((1,), (1,)), ((), ()))
NN = (((1,), (0,)), ((), ()))
TN = (((0,), (0,)), ((), ()))


def mm(a, b, dims):
    return lax.dot_general(a, b, dims, preferred_element_type=F32)


def layer_kernel(x_h, pos_h, bu_h, bv_h, ga_h, gm_h, wq_h, wr_h, wo_h, wu_h, wd_h, rt_h, k_h, v_h,
                 y_v, kn_s, vn_s,
                 x_s, pos_s, bu_s, bv_s, rt_s, wr_s, wqt_s, wot_s, wg_s, wk_s, wv_s, qp_s, wo_s, wu_s, wd_s, k_s, v_s,
                 rs_s, acc, qu_s, sc_s, sp_s, ot_s, o_s, wof_s, p_s, rel_s, rcv_s, stg_s, s2_s, t_s, h_s, g_s, u_s, hid_s, n_s,
                 lsem, gsem_s, gsem_r, msem_s, rsem, asem):
    tp, wg = lax.axis_index("tp"), lax.axis_index("wg")
    z, y = tp // 4, tp % 4
    x, c = wg // 2, wg % 2

    def up1(i, d):
        return lax.rem(i + d, 4)

    def dev(dz=0, dy=0, dx=0, flip=False):
        cc = 1 - c if flip else c
        return (0, up1(z, dz) * 4 + up1(y, dy), up1(x, dx) * 2 + cc)

    xp, xm, sib = dev(dx=1), dev(dx=3), dev(flip=True)
    zp, zm, yp, ym = dev(dz=1), dev(dz=3), dev(dy=1), dev(dy=3)
    xf, zf, yf = dev(dx=2), dev(dz=2), dev(dy=2)

    def send(src, dst, ssem, rsem, device):
        pltpu.make_async_remote_copy(src, dst, ssem, rsem, device_id=device, device_id_type=MESH).start()

    def sent(ref, ssem, rsem):
        pltpu.make_async_remote_copy(ref, ref, ssem, rsem, device_id=sib, device_id_type=MESH).wait_send()

    def arrived(dst, rsem):
        pltpu.make_async_remote_copy(dst, dst, gsem_s.at[0], rsem, device_id=sib, device_id_type=MESH).wait_recv()

    n_local = [0]

    def local(src, dst):
        cp = pltpu.make_async_copy(src, dst, lsem.at[n_local[0]])
        n_local[0] += 1
        cp.start()
        return cp

    barrier = pltpu.get_barrier_semaphore()
    peers = (xp, xm, xf, sib, zp, zm, zf, yp, ym, yf)
    for d in peers:
        pl.semaphore_signal(barrier, inc=1, device_id=d, device_id_type=MESH)

    own = 2 * x + c
    l_g = [local(ga_h, wg_s.at[own, 0, 0]), local(gm_h, wg_s.at[own, 1, 0])]
    l_q = local(wq_h, wqt_s)
    l_x = local(x_h, x_s)
    l_rt = local(rt_h, rt_s)
    l_pos = local(pos_h, pos_s)
    l_bu = local(bu_h, bu_s)
    l_bv = local(bv_h, bv_s)
    l_wr = local(wr_h, wr_s)
    l_wo = local(wo_h, wot_s)
    l_wu = local(wu_h, wu_s.at[own])
    l_wd = local(wd_h, wd_s.at[own])
    l_k = local(k_h, k_s)
    l_v = local(v_h, v_s)

    def slot(dx, flip=False):
        return 2 * up1(x, dx) + (1 - c if flip else c)

    class Gather:
        def __init__(self, ar, buf, rows, low):
            self.ar, self.buf, self.rows, self.low, self.relay = ar, buf, rows, low, True

        def ref(self, s, part):
            if part is WHOLE:
                return self.buf.at[s]
            return self.buf.at[s, pl.ds(0, self.low) if part == LO else pl.ds(self.low, self.rows - self.low)]

        def put(self, k, s, part, device):
            r = self.ref(s, part)
            send(r, r, gsem_s.at[self.ar], gsem_r.at[self.ar, k], device)

        def got(self, k, s, part):
            arrived(self.ref(s, part), gsem_r.at[self.ar, k])

        def start(self):
            o = slot(ME)
            if not self.relay:
                self.put(4, o, LO, xf)
                self.put(5, o, HI, xf)
            self.put(0, o, LO, xp)
            self.put(1, o, HI, xm)
            self.put(2, o, HI, xp)
            self.put(3, o, LO, xm)
            self.put(6, o, WHOLE, sib)

        def forward(self):
            self.got(0, slot(PREV), LO)
            if self.relay:
                self.put(4, slot(PREV), LO, xp)
            self.got(1, slot(NEXT), HI)
            if self.relay:
                self.put(5, slot(NEXT), HI, xm)

        def share(self):
            self.got(2, slot(PREV), HI)
            self.put(7, slot(PREV), WHOLE, sib)
            self.got(3, slot(NEXT), LO)
            self.put(8, slot(NEXT), WHOLE, sib)

        def last(self):
            self.got(4, slot(FAR), LO)
            self.got(5, slot(FAR), HI)
            self.put(9, slot(FAR), WHOLE, sib)

        def sibling(self, dx):
            self.got({ME: 6, PREV: 7, NEXT: 8, FAR: 9}[dx], slot(dx, True), WHOLE)

        def siblings(self):
            for dx in (ME, PREV, NEXT, FAR):
                self.sibling(dx)

        def all_sent(self):
            sent(self.buf.at[pl.ds(0, 7)], gsem_s.at[self.ar], gsem_r.at[self.ar, 0])

    g_g, g_k, g_v, g_o, g_u, g_d, g_r = gathers = [Gather(i, *spec) for i, spec in enumerate((
        (wg_s, 2, 1), (wk_s, HW, 80), (wv_s, 80, 48), (wo_s, 80, 48), (wu_s, SLICE, HW), (wd_s, SLICE, HW), (qp_s, CL, 16)))]
    g_o.relay = False

    l_q.wait()
    wk_s[own] = jnp.concatenate([wqt_s[0:HW, :], wqt_s[HW:QK, :]], axis=1)
    wv_s[own] = jnp.concatenate([wqt_s[QK:400, :], wqt_s[400:480, :]], axis=1)
    l_wo.wait()
    wo_s[own] = jnp.concatenate([wot_s[0:80, :], wot_s[80:160, :]], axis=1)
    l_x.wait()

    def stat_rows(r, carry):
        rows = pl.ds(pl.multiple_of(r * 32, 32), 32)
        v = x_s[rows, :].astype(F32)
        ms = jnp.sum(v * v, axis=1, keepdims=True) * (1.0 / DM)
        rs_s[rows, :] = jnp.broadcast_to(lax.rsqrt(ms + NORM_EPS), (32, 128))
        return carry

    lax.fori_loop(0, 16, stat_rows, 0)
    l_rt.wait()
    l_wr.wait()
    base = pl.multiple_of(640 * x, 128)
    q_even = mm(rt_s[:, pl.ds(base, 384)][:, 0:320], wr_s[...], NT)
    q_odd = mm(rt_s[:, pl.ds(pl.multiple_of(base + 256, 128), 384)][:, 64:384], wr_s[...], NT)
    qp_s[own] = jnp.where(c == 1, q_odd, q_even)
    for cp in l_g:
        cp.wait()
    pl.semaphore_wait(barrier, len(peers))
    g_g.start()
    g_r.start()
    g_k.start()
    g_v.start()
    acc[...] = jnp.zeros_like(acc)
    u_s[...] = jnp.zeros_like(u_s)

    def unpack(even, odd):
        halves = [jnp.concatenate([even[:, cut], odd[:, cut]], axis=1) for cut in (slice(0, SLICE), slice(SLICE, FF))]
        return jnp.concatenate(halves, axis=0)

    def norm_cols(dx):
        xo = up1(x, dx)
        cols = pl.ds(pl.multiple_of(xo * 640, 128), 640)
        g_g.sibling(dx)
        gain = jnp.concatenate([wg_s[2 * xo, 0], wg_s[2 * xo + 1, 0]], axis=1)
        n_s[dx] = (x_s[:, cols].astype(F32) * rs_s[:, 0:1] * gain).astype(BF)

    def pair(g, buf, rows, dx):
        xo = up1(x, dx)
        g.sibling(dx)
        acc[rows, :] += mm(unpack(buf[2 * xo], buf[2 * xo + 1]), n_s[dx], NT)

    qk_rows, v_rows = slice(0, QK), slice(QK, None)
    norm_cols(ME)
    pair(g_k, wk_s, qk_rows, ME)
    g_g.forward()
    g_r.forward()
    g_k.forward()
    g_g.share()
    g_r.share()
    g_k.share()
    g_v.forward()
    g_o.start()
    g_v.share()
    g_g.last()
    g_r.last()
    for dx in (PREV, NEXT, FAR):
        norm_cols(dx)
    pair(g_k, wk_s, qk_rows, PREV)
    pair(g_k, wk_s, qk_rows, NEXT)
    g_k.last()
    for dx in (ME, PREV, NEXT):
        pair(g_v, wv_s, v_rows, dx)
    pair(g_k, wk_s, qk_rows, FAR)
    g_v.last()

    kn_s[...] = acc[HW:QK, :].astype(BF)
    l_pos.wait()
    l_bu.wait()
    l_bv.wait()
    g_r.siblings()

    flip_rows = (lax.broadcasted_iota(jnp.int32, (CL, CL), 0) + lax.broadcasted_iota(jnp.int32, (CL, CL), 1)) % CL == 0
    flip_mat = jnp.where(flip_rows, 1.0, 0.0).astype(BF)
    q_rel = qp_s[0]
    for i in range(1, 8):
        q_rel = q_rel + qp_s[i]
    rel_rev = mm(flip_mat, q_rel.astype(BF), NN).astype(BF)
    diag = lax.broadcasted_iota(jnp.int32, (HD, HD), 0) == lax.broadcasted_iota(jnp.int32, (HD, HD), 1)

    def column(row):
        return jnp.sum(jnp.where(diag, row, 0.0), axis=1, keepdims=True)

    lanes = [slice(first, first + 128) for first in range(0, SEQ, 128)]
    pos = pos_s[...]
    steps = lax.broadcasted_iota(jnp.int32, (CL, SEQ), 0)
    is_self = steps == pos
    l_k.wait()

    for h in BOTH:
        hr = slice(h * HD, h * HD + HD)
        q = acc[hr, :].astype(BF).astype(F32)
        q_u = (q + column(bu_s[h:h + 1, :])).astype(BF).astype(F32)
        q_v = (q + column(bv_s[h:h + 1, :])).astype(BF)
        qu_s[...] = q_u
        rel = mm(rel_rev[:, hr], q_v, NN)
        for b in range(5):
            rel = jnp.where((pos >> b) & 1 == 1, pltpu.roll(rel, 1 << b, 0), rel)
        self_score = jnp.sum(q_u * kn_s[hr, :].astype(F32), axis=0, keepdims=True)
        for ln in lanes:
            quc = qu_s[:, ln]

            def content(g, carry, h=h, ln=ln, quc=quc):
                rows = [jnp.sum(k_s[h, g * 8 + j, :, ln].astype(F32) * quc, axis=0, keepdims=True) for j in range(8)]
                sc_s[h, pl.ds(pl.multiple_of(g * 8, 8), 8), ln] = jnp.concatenate(rows, axis=0)
                return carry

            lax.fori_loop(0, CL // 8, content, 0)
        scores = jnp.where(is_self, self_score, sc_s[h])
        scores = jnp.where(steps <= pos, (scores + rel) * (HD ** -0.5), -1e30)
        e = jnp.exp(scores - jnp.max(scores, axis=0, keepdims=True))
        prob = (e / jnp.sum(e, axis=0, keepdims=True)).astype(BF).astype(F32)
        sp_s[h] = jnp.sum(jnp.where(is_self, prob, 0.0), axis=0, keepdims=True)
        sc_s[h] = jnp.where(is_self, 0.0, prob)

    pair(g_v, wv_s, v_rows, FAR)
    vn_s[...] = acc[v_rows, :].astype(BF)
    l_v.wait()
    for h in BOTH:
        hr = slice(h * HD, h * HD + HD)
        for ln in lanes:

            def mix(g, o, h=h, ln=ln):
                pr = sc_s[h, pl.ds(pl.multiple_of(g * 8, 8), 8), ln]
                for j in range(8):
                    o = o + pr[j:j + 1, :] * v_s[h, g * 8 + j, :, ln].astype(F32)
                return o

            start = sp_s[h, :, ln] * vn_s[hr, ln].astype(F32)
            ot_s[hr, ln] = lax.fori_loop(0, CL // 8, mix, start)
        if h == 0:
            g_o.forward()
            g_o.share()

    g_o.last()
    l_wu.wait()
    g_u.start()
    l_wd.wait()
    g_d.start()
    o_s[...] = jnp.transpose(ot_s[...]).astype(BF).reshape(4, 4, 32, 160)
    for dx in (ME, PREV, NEXT, FAR):
        xo = up1(x, dx)
        g_o.sibling(dx)
        wof_s[:, pl.ds(pl.multiple_of(640 * xo, 128), 640)] = unpack(wo_s[2 * xo], wo_s[2 * xo + 1])

    place = ((z, y, zp, zm, yp, ym, yf), (y, z, yp, ym, zp, zm, zf))

    lo, hi = pl.ds(0, 16), pl.ds(16, 16)

    class Exchange:
        def __init__(self, ps, hf, e, src, fwd, bwd):
            self.src, self.fwd, self.bwd, self.sem = src, fwd, bwd, rsem.at[hf, e]
            self.ssem = msem_s.at[ps, 0, 1]
            self.rel, self.rcv, self.stg = rel_s.at[ps, hf, e], rcv_s.at[ps, hf, e], stg_s.at[ps, hf, e]

        def relay(self):
            send(self.src(FAR).at[lo], self.rel.at[LO], self.ssem, self.sem.at[0], self.fwd)
            send(self.src(FAR).at[hi], self.rel.at[HI], self.ssem, self.sem.at[1], self.bwd)

        def direct(self, d):
            if d == NEXT:
                send(self.src(NEXT).at[hi], self.rcv.at[0, hi], self.ssem, self.sem.at[2], self.fwd)
            else:
                send(self.src(PREV).at[lo], self.rcv.at[1, lo], self.ssem, self.sem.at[3], self.bwd)

        def join(self):
            for part, rows, d, device in ((LO, lo, NEXT, self.fwd), (HI, hi, PREV, self.bwd)):
                arrived(self.rel.at[part], self.sem.at[part])
                both = self.src(d).at[rows][...].astype(F32) + self.rel.at[part][...].astype(F32)
                self.stg.at[part][...] = both.astype(BF)
                send(self.stg.at[part], self.rcv.at[part, rows], self.ssem, self.sem.at[4 + part], device)

        def received(self):
            for k, way, rows in ((2, 0, hi), (3, 1, lo), (4, 0, lo), (5, 1, hi)):
                arrived(self.rcv.at[way, rows], self.sem.at[k])
            return self.rcv.at[0][...].astype(F32) + self.rcv.at[1][...].astype(F32)

        def total(self):
            return self.received() + self.src(ME)[...].astype(F32)

    class Spread:
        def __init__(self, ps, hf, devices):
            self.src, self.rcv, self.devices = s2_s.at[ps, hf], t_s.at[ps, hf], devices
            self.sem, self.ssem = rsem.at[hf, TAIL], msem_s.at[ps, 0, 0]

        def put(self, j):
            send(self.src.at[j], self.rcv.at[j], self.ssem, self.sem.at[j], self.devices[j])

        def received(self):
            for j in ORDER[:3]:
                arrived(self.rcv.at[j], self.sem.at[j])
            return sum(self.rcv.at[j][...].astype(F32) for j in ORDER[:3])

    def reduce_scatter(ps, chunk, between):
        first, second = [], []
        for hf in BOTH:
            a, b, ap, am, bp, bm, bf = place[hf]
            first.append([Exchange(ps, hf, j, lambda d, hf=hf, a=a, b=b, j=j: p_s.at[ps, hf, up1(a, d), up1(b, j)], ap, am)
                          for j in range(4)])
            second.append(Spread(ps, hf, {NEXT: bp, FAR: bf, PREV: bm}))

        def directs(hf, j):
            first[hf][j].direct(NEXT)
            first[hf][j].direct(PREV)

        for hf in BOTH:
            chunk(hf, up1(place[hf][0], FAR))
            for j in ORDER:
                first[hf][j].relay()
        for hf in BOTH:
            chunk(hf, up1(place[hf][0], NEXT))
            chunk(hf, up1(place[hf][0], PREV))
            directs(hf, ORDER[0])
            directs(hf, ORDER[1])
        for hf in BOTH:
            chunk(hf, place[hf][0])
        for t, j in enumerate(ORDER):
            for hf in BOTH:
                first[hf][j].join()
                if t < 2:
                    directs(hf, ORDER[t + 2])
        for j in ORDER[:3]:
            for hf in BOTH:
                s2_s[ps, hf, j] = first[hf][j].total().astype(BF)
                second[hf].put(j)
            if j == NEXT:
                between()
        own_sum = [first[hf][ME].total() for hf in BOTH]
        return [own_sum[hf] + second[hf].received() for hf in BOTH]

    class Ring:
        def __init__(self, ps, hf, e, blk, fwd, bwd):
            self.blk, self.fwd, self.bwd, self.sem = blk, fwd, bwd, asem.at[hf, e]
            self.ssem = msem_s.at[ps, 1, 0 if e == TAIL else 1]

        def put(self, k, d, rows, device):
            r = self.blk(d, rows)
            send(r, r, self.ssem, self.sem.at[k], device)

        def start(self):
            self.put(0, ME, lo, self.fwd)
            self.put(1, ME, hi, self.bwd)
            self.put(2, ME, hi, self.fwd)
            self.put(3, ME, lo, self.bwd)

        def forward(self):
            arrived(self.blk(PREV, lo), self.sem.at[0])
            self.put(4, PREV, lo, self.fwd)
            arrived(self.blk(NEXT, hi), self.sem.at[1])
            self.put(5, NEXT, hi, self.bwd)

        def got(self, d):
            for k, rows in {PREV: ((2, hi),), NEXT: ((3, lo),), FAR: ((4, lo), (5, hi))}[d]:
                arrived(self.blk(d, rows), self.sem.at[k])

    def all_gather(ps, buf, consume, hook):
        inner, outer = [], []
        for hf in BOTH:
            a, b, ap, am, bp, bm, _ = place[hf]

            def block(ia, ib, rows, hf=hf):
                cols = pl.ds(hf * HALF, HALF)
                return buf.at[ia, ib, rows, cols] if hf == 0 else buf.at[ib, ia, rows, cols]

            inner.append(Ring(ps, hf, TAIL, lambda d, rows, a=a, b=b, block=block: block(a, up1(b, d), rows), bp, bm))
            outer.append([Ring(ps, hf, j, lambda d, rows, a=a, b=b, j=j, block=block: block(up1(a, d), up1(b, j), rows), ap, am)
                          for j in range(4)])
        for hf in BOTH:
            inner[hf].start()
        for hf in BOTH:
            outer[hf][ME].start()
        for hf in BOTH:
            inner[hf].forward()
        for d in (PREV, NEXT):
            for hf in BOTH:
                inner[hf].got(d)
                outer[hf][d].start()
        hook(0)
        for hf in BOTH:
            outer[hf][ME].forward()
        for hf in BOTH:
            inner[hf].got(FAR)
            outer[hf][FAR].start()
        for d in (PREV, NEXT):
            for hf in BOTH:
                outer[hf][d].forward()
        hook(1)
        for hf in BOTH:
            consume(hf, place[hf][0])
        for hf in BOTH:
            outer[hf][FAR].forward()
        for d in (PREV, NEXT, FAR):
            for hf in BOTH:
                for r in outer[hf]:
                    r.got(d)
                consume(hf, up1(place[hf][0], d))
            if d == NEXT:
                hook(2)

    def out_chunk(hf, i):
        rows = (o_s[i] if hf == 0 else o_s[:, i]).reshape(128, 160)
        part = mm(rows, wof_s[:, hf * HALF:hf * HALF + HALF], NN)
        p_s[0, hf, i] = part.astype(BF).reshape(4, 32, HALF)

    def attn_between():
        g_u.forward()
        g_u.share()

    part = reduce_scatter(0, out_chunk, attn_between)
    mine = pl.ds(pl.multiple_of(tp * 32, 32), 32)
    for hf in BOTH:
        cols = slice(hf * HALF, hf * HALF + HALF)
        h_s[:, cols] = x_s[mine, cols].astype(F32) + part[hf]
    resid = h_s[...]
    inv = lax.rsqrt(jnp.sum(resid * resid, axis=1, keepdims=True) * (1.0 / DM) + NORM_EPS)
    gain = jnp.concatenate([wg_s[i, 1] for i in range(8)], axis=1)
    g_s[z, y] = (resid * inv * gain).astype(BF)

    def mlp_hook(step):
        if step == 0:
            g_u.last()
            g_d.forward()
        elif step == 1:
            g_d.share()
            g_u.siblings()
        else:
            g_d.last()

    def up_part(hf, i):
        w = wu_s[4 * hf:4 * hf + 4].reshape(HALF, FF)
        cols = slice(hf * HALF, hf * HALF + HALF)
        rows = (g_s[i, :, :, cols] if hf == 0 else g_s[:, i, :, cols]).reshape(128, HALF)
        prod = mm(rows, w, NN).reshape(4, 32, FF)
        if hf == 0:
            u_s[i] += prod
        else:
            u_s[:, i] += prod

    all_gather(0, g_s, up_part, mlp_hook)
    g_d.siblings()
    todo = [FAR], [NEXT, PREV, ME], [], [], [], [], [], []
    calls = iter(todo)

    def down_chunk(hf, i):
        for d in next(calls):
            k = up1(z, d)
            hid_s[k] = jax.nn.gelu(u_s[k], approximate=True).astype(BF)
        rows = (hid_s[i] if hf == 0 else hid_s[:, i]).reshape(128, FF)
        w = wd_s[4 * hf:4 * hf + 4].reshape(HALF, FF)
        p_s[1, hf, i] = mm(rows, w, NT).astype(BF).reshape(4, 32, HALF)

    part = reduce_scatter(1, down_chunk, lambda: None)
    y_v[z, y] = jnp.concatenate([h_s[:, 0:HALF] + part[0], h_s[:, HALF:DM] + part[1]], axis=1).astype(BF)
    all_gather(1, y_v, lambda hf, i: None, lambda step: None)
    for g in gathers:
        g.all_sent()
    for ps in BOTH:
        for kind in BOTH:
            sent(g_s.at[0, pl.ds(0, 3)], msem_s.at[ps, kind, 0], rsem.at[0, 0, 0])
            sent(g_s.at[pl.ds(0, 3)], msem_s.at[ps, kind, 1], rsem.at[0, 0, 0])


def result_kernel(y_v, k_v, v_v, y_h, k_h, v_h, sem):
    copies = [pltpu.make_async_copy(src, dst, sem.at[i]) for i, (src, dst) in enumerate(((y_v, y_h), (k_v, k_h), (v_v, v_h)))]
    for cp in copies:
        cp.start()
    for cp in copies:
        cp.wait()


def solution(mesh):
    tok_axes = ("dp", "wg")
    in_specs = (P(tok_axes, None), P("wg"), P("wg"), P("wg", None, "tp", None), P("wg", "tp", None), P("tp", None, "wg"), P("wg", "tp"), P("tp", "wg"), P("tp", None), P("tp", None), P(None, None), P(tok_axes, "tp", None, None), P(tok_axes, "tp", None, None), P(tok_axes))
    out_specs = (P(tok_axes, None), P(tok_axes, "tp", None), P(tok_axes, "tp", None))

    def vm(shape, dtype=BF):
        return pltpu.VMEM(shape, dtype)

    def dma(*shape):
        return pltpu.SemaphoreType.DMA(shape)

    blocks = (2, 2, 4, 2)
    scratch = [
        vm((SEQ, DM)), vm((1, SEQ), jnp.int32), vm((2, HD), F32), vm((2, HD), F32), vm((CL, DM)), vm((HW, SLICE)),
        vm((3 * HW, SLICE)), vm((HW, SLICE)), vm((8, 2, 1, SLICE), F32), vm((8, HW, FF)), vm((8, 80, FF)), vm((8, CL, HW), F32), vm((8, 80, FF)),
        vm((8, SLICE, FF)), vm((8, SLICE, FF)), vm((2, CL, HD, SEQ)), vm((2, CL, HD, SEQ)),
        vm((SEQ, 128), F32), vm((3 * HW, SEQ), F32), vm((HD, SEQ), F32), vm((2, CL, SEQ), F32), vm((2, 1, SEQ), F32),
        vm((HW, SEQ), F32), vm((4, 4, 32, HW)), vm((HW, DM)), vm((2, 2, 4, 4, 32, HALF)),
        vm(blocks + (16, HALF)), vm(blocks + (32, HALF)), vm(blocks + (16, HALF)), vm((2, 2, 4, 32, HALF)), vm((2, 2, 4, 32, HALF)),
        vm((32, DM), F32), vm((4, 4, 32, DM)), vm((4, 4, 32, FF), F32), vm((4, 4, 32, FF)), vm((4, SEQ, FF)),
        dma(14), dma(7), dma(7, 10), dma(2, 2, 2), dma(2, 5, 6), dma(2, 5, 6),
    ]
    call = pl.pallas_call(
        layer_kernel,
        out_shape=[vm((4, 4, 32, DM)), vm((HW, SEQ)), vm((HW, SEQ))],
        in_specs=[pl.BlockSpec(memory_space=ANY)] * 14,
        out_specs=[pl.BlockSpec(memory_space=pltpu.VMEM)] * 3,
        scratch_shapes=scratch,
        compiler_params=pltpu.CompilerParams(collective_id=0, has_side_effects=True, vmem_limit_bytes=56 * 1024 * 1024),
        name="layer",
    )

    shapes = ((4, 4, 32, DM), (HW, SEQ), (HW, SEQ))
    write = pl.pallas_call(
        result_kernel,
        out_shape=[jax.ShapeDtypeStruct(shape, BF) for shape in shapes],
        in_specs=[pl.BlockSpec(memory_space=pltpu.VMEM)] * 3,
        out_specs=[pl.BlockSpec(memory_space=ANY)] * 3,
        scratch_shapes=[dma(3)],
        compiler_params=pltpu.CompilerParams(vmem_limit_bytes=1 << 20),
        name="results",
    )

    def device_step(tokens, gain_attn, gain_mlp, w_qkv, w_rel, w_out, w_up, w_down, bias_u, bias_v, rel_table, k_cache, v_cache, positions):
        out, k_new, v_new = write(*call(
            tokens, positions.reshape(1, SEQ), bias_u, bias_v, gain_attn, gain_mlp,
            w_qkv.transpose(1, 2, 3, 0).reshape(480, 320), w_rel.transpose(1, 2, 0).reshape(160, 320),
            w_out.reshape(160, 320), w_up, w_down.T, rel_table,
            k_cache.transpose(1, 2, 3, 0), v_cache.transpose(1, 2, 3, 0)))
        return (out.reshape(SEQ, DM), k_new.reshape(2, HD, SEQ).transpose(2, 0, 1), v_new.reshape(2, HD, SEQ).transpose(2, 0, 1))

    return jax.shard_map(device_step, mesh=mesh, in_specs=in_specs, out_specs=out_specs, check_vma=False)
```
